32 devices in a mesh: mem: 4 (over z), hor: 2 (over x), grp: 4 (over y, core).
Axes of the slice: x: 2, y: 2, z: 4, core: 2. Of those that a mesh axis runs over, the one named last changes fastest.
Arguments:
- ensemble: float32 [128, 2, 32, 1024], P(('mem', 'grp'), None, None, 'hor'), may hold values from -1 to 1
- coupling: float32 [32, 32], replicated, may hold values from -1 to 1
- obs_column: int32 [2, 16, 2, 512], P(None, ('mem', 'grp'), 'hor'), may hold values from 0 to 511
- obs_level: int32 [2, 16, 2, 512], P(None, ('mem', 'grp'), 'hor'), may hold values from 0 to 1
- obs_value: float32 [2, 16, 2, 512], P(None, ('mem', 'grp'), 'hor'), may hold values from -6 to 6
- obs_error: float32 [2, 16, 2, 512], P(None, ('mem', 'grp'), 'hor'), may hold values from 0.25 to 4
- obs_live: int32 [2, 16, 2, 512], P(None, ('mem', 'grp'), 'hor'), may hold values 0 or 1
- partners: int32 [16, 2, 2], P(('mem', 'grp'), 'hor'), may hold values from 0 to 15, as said below
Outputs:
- analysed: float32 [128, 2, 32, 1024], P(('mem', 'grp'), None, None, 'hor')
The draws below stay inside these ranges and needn't reach their ends.
Inputs may be any that keep to these rules, and one draw needn't show every extreme that they name: `partners`: each row holds 2 different slab numbers, none of them the row's own slab.
All inputs are finite; a program needn't handle non-finite values. No bound on the sum of `obs_live` on one device may be relied on, other than what follows from the above.
Results may differ from the reference program's by a relative error of at most 0.0003.
Values sent between devices are 32-bit elements; how exact they have to be, the bound alone decides.
A program may use at most 64 MiB of HBM per device.

```python
import math
import jax
import jax.numpy as jnp
from jax import lax

MEMBERS = 128
LEVELS = 32
COL_DEV = 512
OBS_SLOTS = 512
SUBSTEPS = 4
CYCLES = 2
ROOT_STEPS = 8
PARTNER_COUNT = 2
SLABS = 16
TILES = 2
SLAB_LEVELS = 2
COLUMNS = 1024


def draw_partners(key, part):
    first_key, second_key = jax.random.split(jax.random.fold_in(key, 7))
    first = jax.random.randint(first_key, (SLABS, TILES), 1, SLABS)
    second = jax.random.randint(second_key, (SLABS, TILES), 1, SLABS - 1)
    second = second + (second >= first).astype(jnp.int32)
    own_slab = jnp.arange(SLABS, dtype=jnp.int32)[:, None]
    chosen = jnp.stack([(own_slab + first) % SLABS, (own_slab + second) % SLABS], axis=-1)
    return chosen.astype(jnp.int32)


def place_ends(drawn, own_key, smallest, top_value):
    spot = [jax.random.randint(jax.random.fold_in(own_key, axis), (), 0, length) for axis, length in enumerate(drawn.shape)]
    main_axis = drawn.shape.index(max(drawn.shape))
    neighbour = spot[:main_axis] + [(spot[main_axis] + 1) % drawn.shape[main_axis]] + spot[main_axis + 1:]
    return drawn.at[tuple(spot)].set(smallest).at[tuple(neighbour)].set(top_value)


def block_levels(key, extent, cuts, least, top_value):
    gain = 1.0
    for axis_at, shards_of in cuts:
        draws = jax.random.uniform(jax.random.fold_in(jax.random.fold_in(key, 6), axis_at), (shards_of,), jnp.float32, least / len(cuts), top_value / len(cuts))
        gain = gain * jnp.repeat(jnp.exp(draws), extent[axis_at] // shards_of).reshape((-1,) + (1,) * (len(extent) - 1 - axis_at))
    return gain


def gaussian(stream_key, dims, scale, bound, pieces=(), held_as=jnp.bfloat16):
    array = jax.random.normal(stream_key, dims, jnp.float32) * scale
    if len(pieces) > 0:
        array = block_levels(stream_key, dims, pieces, -0.22, 0.18) * array
    return jnp.clip(array, min=-bound, max=bound).astype(held_as)


def setup_inputs(seed: int = 0) -> dict:
    streams_of = jax.random.split(jax.random.key(seed), 9)
    ensemble = gaussian(streams_of[0], (MEMBERS, 2, LEVELS, COLUMNS), 0.25, 1.0, ((0, 16), (3, 2)), jnp.float32)
    coupling = gaussian(streams_of[1], (LEVELS, LEVELS), LEVELS ** -0.5, 1.0, (), jnp.float32)
    obs_column = place_ends(jax.random.randint(streams_of[2], (CYCLES, SLABS, TILES, OBS_SLOTS), 0, COL_DEV), jax.random.fold_in(streams_of[2], 1), 0, COL_DEV - 1).astype(jnp.int32)
    obs_level = place_ends(jax.random.randint(streams_of[3], (CYCLES, SLABS, TILES, OBS_SLOTS), 0, SLAB_LEVELS), jax.random.fold_in(streams_of[3], 1), 0, SLAB_LEVELS - 1).astype(jnp.int32)
    obs_value = gaussian(streams_of[4], (CYCLES, SLABS, TILES, OBS_SLOTS), 1.0, 6.0, ((1, 16), (2, 2)), jnp.float32)
    obs_error = jnp.clip(jnp.exp(math.log(4.0) - 2.7725887 * jax.random.uniform(streams_of[5], (CYCLES, SLABS, TILES, OBS_SLOTS), jnp.float32) ** block_levels(streams_of[5], (CYCLES, SLABS, TILES, OBS_SLOTS), ((1, 16), (2, 2)), -0.2, 0.2)), 0.25, 4.0)
    obs_live = place_ends((jax.random.randint(streams_of[6], (CYCLES, SLABS, TILES, OBS_SLOTS), 0, 4) < 3).astype(jnp.int32), jax.random.fold_in(streams_of[6], 1), 0, 1)
    partners = draw_partners(jax.random.fold_in(streams_of[8], 71), 0)
    return {"ensemble": ensemble, "coupling": coupling, "obs_column": obs_column, "obs_level": obs_level, "obs_value": obs_value, "obs_error": obs_error, "obs_live": obs_live, "partners": partners}


time_step = 0.2

def centred(field):
    return (jnp.roll(field, -1, axis=-1) - jnp.roll(field, 1, axis=-1)) * 0.5

def substep(velocity, height, coupling):
    pressure = jnp.einsum('lk,mkc->mlc', coupling, height, precision=lax.Precision.HIGHEST)
    moved = velocity - time_step * (velocity * centred(velocity) + centred(pressure))
    fluxes = moved * height
    height_new = height - time_step * centred(fluxes)
    return (moved, height_new)

def observe(patch, column, level, value, error, live):
    width = patch.shape[0]
    cells = patch.shape[-1]
    heights = patch[:, 1].reshape(width, -1)
    position = (level * cells + column).astype(jnp.int32)
    observed = jnp.take(heights, position, axis=1)
    average = lax.optimization_barrier(jnp.mean(observed, axis=0))
    anomalies = observed - average
    weight = live.astype(jnp.float32) / error
    gram_matrix = jnp.dot(anomalies * weight, anomalies.T, precision=lax.Precision.HIGHEST)
    innovation = jnp.dot(anomalies, weight * (value - average), precision=lax.Precision.HIGHEST)
    return (gram_matrix, innovation)

def analyse(patch, gram_sum, vector_sum, count):
    width = patch.shape[0]
    identity = jnp.eye(width, dtype=jnp.float32)
    blended = (width - 1.0) * identity + gram_sum / (count + 1.0)
    bvector = vector_sum / (count + 1.0)
    frobenius = jnp.sqrt(jnp.sum(blended * blended))
    iterate = blended / frobenius
    inverse_root = identity
    for step_index in range(ROOT_STEPS):
        newton = 1.5 * identity - 0.5 * jnp.dot(inverse_root, iterate, precision=lax.Precision.HIGHEST)
        iterate = jnp.dot(iterate, newton, precision=lax.Precision.HIGHEST)
        inverse_root = jnp.dot(newton, inverse_root, precision=lax.Precision.HIGHEST)
    spread = inverse_root * (jnp.sqrt(width - 1.0) / jnp.sqrt(frobenius))
    inner = jnp.dot(inverse_root, bvector, precision=lax.Precision.HIGHEST)
    mean_weight = jnp.dot(inverse_root, inner, precision=lax.Precision.HIGHEST) / frobenius
    transform = mean_weight[:, None] + spread
    flat = patch.reshape(width, -1)
    average = lax.optimization_barrier(jnp.mean(flat, axis=0))
    anomalies = flat - average
    result = average + jnp.dot(transform.T, anomalies, precision=lax.Precision.HIGHEST)
    return result.reshape(patch.shape)

def reference(ensemble, coupling, obs_column, obs_level, obs_value, obs_error, obs_live, partners):
    members = ensemble
    tile_index = jnp.arange(TILES, dtype=jnp.int32)[None, :]
    for cycle_index in range(CYCLES):
        velocity, height = (members[:, 0], members[:, 1])
        for step_index in range(SUBSTEPS):
            velocity, height = substep(velocity, height, coupling)
        members = jnp.stack([velocity, height], axis=1)
        patches = members.reshape(MEMBERS, 2, SLABS, SLAB_LEVELS, TILES, COL_DEV).transpose(2, 4, 0, 1, 3, 5)
        flat_patches = patches.reshape(SLABS * TILES, MEMBERS, 2, SLAB_LEVELS, COL_DEV)

        def observe_one(items):
            return observe(items[0], items[1], items[2], items[3], items[4], items[5])
        grams, vectors = lax.map(observe_one, (flat_patches, obs_column[cycle_index].reshape(-1, OBS_SLOTS), obs_level[cycle_index].reshape(-1, OBS_SLOTS), obs_value[cycle_index].reshape(-1, OBS_SLOTS), obs_error[cycle_index].reshape(-1, OBS_SLOTS), obs_live[cycle_index].reshape(-1, OBS_SLOTS)))
        grams = grams.reshape(SLABS, TILES, MEMBERS, MEMBERS)
        vectors = vectors.reshape(SLABS, TILES, MEMBERS)
        gram_sum = grams
        vector_sum = vectors
        for which in range(PARTNER_COUNT):
            gram_sum = gram_sum + grams[partners[:, :, which], tile_index]
            vector_sum = vector_sum + vectors[partners[:, :, which], tile_index]

        def analyse_one(items):
            return analyse(items[0], items[1], items[2], PARTNER_COUNT)
        updated = lax.map(analyse_one, (flat_patches, gram_sum.reshape(-1, MEMBERS, MEMBERS), vector_sum.reshape(-1, MEMBERS)))
        members = updated.reshape(SLABS, TILES, MEMBERS, 2, SLAB_LEVELS, COL_DEV).transpose(2, 3, 0, 4, 1, 5).reshape(MEMBERS, 2, LEVELS, COLUMNS)
    return members
```

```python
import functools

import jax
import jax.numpy as jnp
from jax import lax
from jax.experimental import pallas as pl
from jax.experimental.pallas import tpu as pltpu
from jax.sharding import PartitionSpec as P

SUBSTEPS = 4
ROOT_STEPS = 8
MESH = pl.DeviceIdType.MESH
LANES = 128
HALO = 2 * SUBSTEPS

time_step = 0.2


def split(value):
    high = value.astype(jnp.bfloat16)
    return high, (value - high.astype(jnp.float32)).astype(jnp.bfloat16)


def split3(value):
    high, rest = value.astype(jnp.bfloat16), None
    rest = value - high.astype(jnp.float32)
    middle = rest.astype(jnp.bfloat16)
    low = (rest - middle.astype(jnp.float32)).astype(jnp.bfloat16)
    return high, middle, low


def one(a, b, across=0):
    dims = (((1,), (across,)), ((), ()))
    return lax.dot_general(a, b, dims, preferred_element_type=jnp.float32)


def product(left, right, across=0):
    left_high, left_low = split(left)
    right_high, right_low = split(right)
    return one(left_high, right_high, across) + (
        one(left_high, right_low, across) + one(left_low, right_high, across)
    )


def iota(shape, axis):
    return lax.broadcasted_iota(jnp.int32, shape, axis)


def program(
    sizes, count, cycles,
    x_ref, coupling_ref, column_ref, level_ref, value_ref, error_ref, live_ref, blend_ref,
    out_ref,
    kron, u_ref, h_ref, p_ref, edge_u, edge_h, edge_p, packed, halo,
    heights, speeds, updated, returned, cells,
    own, column, partial, arrived, peers_blend,
    send_n, recv_n, send_a, recv_a, send_b, recv_b, send_c, recv_c,
    send_h, recv_h, send_u, recv_u, send_e, recv_e,
):
    mem_count, grp_count, hor_count = sizes
    mem = lax.axis_index("mem")
    grp = lax.axis_index("grp")
    hor = lax.axis_index("hor")
    slab_count = mem_count * grp_count
    slab = mem * grp_count + grp
    slab_levels, block, width = x_ref.shape[2:]
    levels = slab_count * slab_levels
    rows = levels * block
    members = slab_count * block

    def grp_peer(step):
        return lax.rem(grp + step, grp_count)

    upper = mem // (mem_count // 2)

    def far_mem(at):
        low = mem_count - 1 - at - (mem + 1 + at) // mem_count
        high = at + (at + mem_count - mem) // mem_count
        return (1 - upper) * low + upper * high

    peers = []
    for at in range(mem_count - 1):
        for step in range(grp_count):
            peers.append((far_mem(at), grp_peer(step)))
    near = [(mem, grp_peer(step)) for step in range(1, grp_count)]

    barrier = pltpu.get_barrier_semaphore()
    right = lax.rem(hor + 1, hor_count)
    left = lax.rem(hor + hor_count - 1, hor_count)
    for one_mem, one_grp in peers + near:
        pl.semaphore_signal(
            barrier, inc=1, device_id={"mem": one_mem, "grp": one_grp}, device_id_type=MESH
        )
    for side in (left, right):
        pl.semaphore_signal(barrier, inc=1, device_id={"hor": side}, device_id_type=MESH)

    def pack(source):
        lane = iota((block, LANES), 1)
        per = LANES // HALO
        for group in range(2 * levels // per):
            low = jnp.zeros((block, LANES), jnp.float32)
            high = jnp.zeros((block, LANES), jnp.float32)
            for at in range(per):
                index = group * per + at
                field, level = index // levels, index % levels
                place = (field, level // slab_levels, level % slab_levels)
                inside = (lane >= at * HALO) & (lane < (at + 1) * HALO)
                first = source[place + (slice(None), slice(0, LANES))]
                last = source[place + (slice(None), slice(width - LANES, width))]
                if at:
                    first = pltpu.roll(first, at * HALO, 1)
                turn = (at * HALO + HALO) % LANES
                if turn:
                    last = pltpu.roll(last, turn, 1)
                low = jnp.where(inside, first, low)
                high = jnp.where(inside, last, high)
            packed[0, group] = low
            packed[1, group] = high

    def send_halo(cycle):
        copies = []
        for side, target in ((0, left), (1, right)):
            copy = pltpu.make_async_remote_copy(
                src_ref=packed.at[side], dst_ref=halo.at[cycle, side],
                send_sem=send_n.at[cycle, side], recv_sem=recv_n.at[cycle, side],
                device_id={"hor": target}, device_id_type=MESH,
            )
            copy.start()
            copies.append(copy)
        return copies

    def unpack(source, cycle):
        lane = iota((block, LANES), 1)
        per = LANES // HALO
        for field, target in ((0, edge_u), (1, edge_h)):
            for level in range(levels):
                index = field * levels + level
                group, at = index // per, index % per
                place = (level // slab_levels, level % slab_levels)
                before = halo[cycle, 1, group]
                after = halo[cycle, 0, group]
                if at:
                    before = pltpu.roll(before, LANES - at * HALO, 1)
                turn = (2 * LANES - HALO - at * HALO) % LANES
                if turn:
                    after = pltpu.roll(after, turn, 1)
                first = source[(field,) + place + (slice(None), slice(0, LANES))]
                last = source[(field,) + place + (slice(None), slice(width - LANES, width))]
                mixed = jnp.where(
                    lane < LANES // 2,
                    pltpu.roll(first, HALO, 1), pltpu.roll(last, LANES - HALO, 1),
                )
                mixed = jnp.where(lane < HALO, before, mixed)
                target[place] = jnp.where(lane >= LANES - HALO, after, mixed)

    def centred(field):
        return (pltpu.roll(field, field.shape[-1] - 1, 1) - pltpu.roll(field, 1, 1)) * 0.5

    def substep(read_u, read_h, write_u, write_h, press):
        span = press.shape[-1]
        for at in range(span // LANES):
            lanes = slice(at * LANES, (at + 1) * LANES)
            high, low = split(read_h(slice(0, slab_count), lanes).reshape(rows, LANES))
            result = one(kron[0], high) + (one(kron[0], low) + one(kron[1], high))
            press[:, :, :, lanes] = result.reshape(slab_count, slab_levels, block, LANES)
        everything = slice(0, span)

        for at in range(slab_count):
            part = slice(at, at + 1)
            size = (slab_levels * block, span)
            velocity = read_u(part, everything).reshape(size)
            height = read_h(part, everything).reshape(size)
            pressure = press[part].reshape(size)
            moved = velocity - time_step * (velocity * centred(velocity) + centred(pressure))
            risen = height - time_step * centred(moved * height)
            write_u[part] = moved.reshape(1, slab_levels, block, span)
            write_h[part] = risen.reshape(1, slab_levels, block, span)

    def reader(ref):
        return lambda part, lanes: ref[part, :, :, lanes]

    def field_reader(ref, field):
        return lambda part, lanes: ref[field, part, :, :, lanes]

    def advance(source, cycle, copies):
        substep(field_reader(source, 0), field_reader(source, 1), u_ref, h_ref, p_ref)

        def again(step, carry):
            substep(reader(u_ref), reader(h_ref), u_ref, h_ref, p_ref)
            return carry

        lax.fori_loop(1, SUBSTEPS, again, 0)
        for copy in copies:
            copy.wait()
        unpack(source, cycle)

        def edge(step, carry):
            substep(reader(edge_u), reader(edge_h), edge_u, edge_h, edge_p)
            return carry

        lax.fori_loop(0, SUBSTEPS, edge, 0)
        lane = iota((block, LANES), 1)
        for strip, whole in ((edge_h, h_ref), (edge_u, u_ref)):
            for at in range(slab_count):
                for level in range(slab_levels):
                    fresh = strip[at, level]
                    first = whole[at, level, :, 0:LANES]
                    last = whole[at, level, :, width - LANES : width]
                    whole[at, level, :, 0:LANES] = jnp.where(
                        lane < HALO, pltpu.roll(fresh, LANES - HALO, 1), first
                    )
                    whole[at, level, :, width - LANES : width] = jnp.where(
                        lane >= LANES - HALO, pltpu.roll(fresh, HALO, 1), last
                    )

    def remote(source, target, send_sem, recv_sem, one_mem, one_grp):
        other = one_mem * grp_count + one_grp
        return pltpu.make_async_remote_copy(
            src_ref=source.at[other], dst_ref=target.at[slab],
            send_sem=send_sem.at[other], recv_sem=recv_sem.at[slab],
            device_id={"mem": one_mem, "grp": one_grp}, device_id_type=MESH,
        )

    def send_all(source, target, send_sem, recv_sem, listed):
        copies = []
        for one_mem, one_grp in listed:
            copy = remote(source, target, send_sem, recv_sem, one_mem, one_grp)
            copy.start()
            copies.append(copy)
        return copies

    def take_all(target, recv_sem):
        for one_mem, one_grp in near + peers:
            other = one_mem * grp_count + one_grp
            pltpu.make_async_remote_copy(
                src_ref=target.at[other], dst_ref=target.at[other],
                send_sem=recv_sem.at[other], recv_sem=recv_sem.at[other],
                device_id={"mem": one_mem, "grp": one_grp}, device_id_type=MESH,
            ).wait_recv()

    def sum_cells(cycle):
        place = level_ref[cycle] * width + column_ref[cycle]
        weight = live_ref[cycle].astype(jnp.float32) / error_ref[cycle]
        pulled = weight * value_ref[cycle]
        parts = split3(weight) + split3(pulled)
        spare = jnp.zeros((16 - len(parts), weight.shape[1]), jnp.bfloat16)
        lhs = jnp.concatenate(parts + (spare,), axis=0)
        total = slab_levels * width

        def chunk(at, carry):
            numbers = iota((LANES, weight.shape[1]), 0) + at * LANES
            hits = jnp.where(numbers == place, 1.0, 0.0).astype(jnp.bfloat16)
            sums = one(lhs, hits, 1)
            cells[0, at] = sums[0:1] + (sums[1:2] + sums[2:3])
            cells[1, at] = sums[3:4] + (sums[4:5] + sums[5:6])
            return carry

        lax.fori_loop(0, total // LANES, chunk, 0)

    def gram():
        per = width // LANES
        total = None
        for level in range(slab_levels):
            flat = heights[:, level].reshape(members, width)
            average = jnp.mean(flat, axis=0, keepdims=True)
            anomalies = flat - average
            weight = jnp.concatenate(
                [cells[0, level * per + at] for at in range(per)], axis=1
            )
            pulled = jnp.concatenate(
                [cells[1, level * per + at] for at in range(per)], axis=1
            )
            pull = pulled - weight * average
            lhs = jnp.concatenate(
                [anomalies * weight, jnp.broadcast_to(pull, (8, width))], axis=0
            )
            here = product(lhs, anomalies, 1)
            total = here if total is None else total + here
        own[...] = total

    lanes = iota((1, blend_ref.shape[1]), 1)

    def share(row, step):
        place = lax.rem(mem + mem_count - step, mem_count) * grp_count + grp
        return jnp.sum(jnp.where(lanes == place, row[0:1], 0.0), axis=1, keepdims=True)

    def blended_for(row):
        total = share(row, 0) * own[...]
        for step in range(1, mem_count):
            total = total + share(row, step) * column[step - 1]
        return total

    def root(total):
        total = total / (count + 1.0)
        square = (members, members)
        identity = (iota(square, 0) == iota(square, 1)).astype(jnp.float32)
        blended = (members - 1.0) * identity + total[:members]
        bvector = total[members:]
        squares = jnp.sum(
            jnp.sum(blended * blended, axis=1, keepdims=True), axis=0, keepdims=True
        )
        frobenius = jnp.sqrt(squares)
        iterate = blended / frobenius
        newton = 1.5 * identity - 0.5 * iterate
        inverse_root = newton
        for step in range(1, ROOT_STEPS):
            iterate = product(newton, iterate)
            newton = 1.5 * identity - 0.5 * product(inverse_root, iterate)
            inverse_root = product(newton, inverse_root)
        spread = inverse_root * (jnp.sqrt(members - 1.0) / jnp.sqrt(frobenius))
        inner = product(bvector, inverse_root)
        mean_weight = product(inner, inverse_root) / frobenius
        return spread + mean_weight[0:1]

    def update(transposed, source, field):
        high, low = split(transposed)
        for level in range(slab_levels):
            flat = source[:, level].reshape(members, width)
            average = jnp.mean(flat, axis=0, keepdims=True)
            flat_high, flat_low = split(flat - average)
            result = average + (
                one(high, flat_high) + (one(high, flat_low) + one(low, flat_high))
            )
            updated[field, :, level] = result.reshape(slab_count, block, width)

    pack(x_ref)
    pl.semaphore_wait(barrier, slab_count - 1 + 2)
    copies = send_halo(0)
    blends = []
    for step in range(1, grp_count):
        copy = pltpu.make_async_remote_copy(
            src_ref=blend_ref, dst_ref=peers_blend.at[step - 1],
            send_sem=send_b.at[step - 1], recv_sem=recv_b.at[step - 1],
            device_id={"grp": grp_peer(step)}, device_id_type=MESH,
        )
        copy.start()
        blends.append(copy)
    spread_rows = jnp.where(
        iota((rows, levels), 0) // block == iota((rows, levels), 1), 1.0, 0.0
    ).astype(jnp.bfloat16)
    same = lax.rem(iota((rows, rows), 0), block) == lax.rem(iota((rows, rows), 1), block)
    for at, part in enumerate(split(coupling_ref[...])):
        tall = one(spread_rows, part).astype(jnp.bfloat16)
        kron[at] = jnp.where(same, one(tall, spread_rows, 1), 0.0).astype(jnp.bfloat16)

    for cycle in range(cycles):
        source = x_ref if cycle == 0 else returned
        if cycle:
            pack(source)
            copies = send_halo(cycle)
        advance(source, cycle, copies)
        outward = send_all(h_ref, heights, send_h.at[cycle], recv_h.at[cycle], peers + near)
        heights[slab] = h_ref[slab]
        speeds[slab] = u_ref[slab]
        sum_cells(cycle)
        take_all(heights, recv_h.at[cycle])
        gram()

        gathers = []
        for step in range(1, mem_count):
            copy = pltpu.make_async_remote_copy(
                src_ref=own, dst_ref=column.at[step - 1],
                send_sem=send_a.at[cycle, step - 1], recv_sem=recv_a.at[cycle, step - 1],
                device_id={"mem": lax.rem(mem + step, mem_count)}, device_id_type=MESH,
            )
            copy.start()
            gathers.append(copy)
        outward = outward + send_all(
            u_ref, speeds, send_u.at[cycle], recv_u.at[cycle], peers
        )
        if cycle == 0:
            for copy in blends:
                copy.wait()
        for copy in gathers:
            copy.wait()
        returns = []
        for step in range(1, grp_count):
            partial[step - 1] = blended_for(peers_blend[step - 1])
            copy = pltpu.make_async_remote_copy(
                src_ref=partial.at[step - 1], dst_ref=arrived.at[step - 1],
                send_sem=send_c.at[cycle, step - 1], recv_sem=recv_c.at[cycle, step - 1],
                device_id={"grp": grp_peer(grp_count - step)}, device_id_type=MESH,
            )
            copy.start()
            returns.append(copy)
        outward = outward + send_all(
            u_ref, speeds, send_u.at[cycle], recv_u.at[cycle], near
        )
        total = blended_for(blend_ref[...])
        for copy in returns:
            copy.wait()
        for step in range(1, grp_count):
            total = total + arrived[step - 1]
        transposed = root(total)
        update(transposed, heights, 1)
        back = send_all(
            updated.at[1], returned.at[1], send_e.at[cycle, 1], recv_e.at[cycle, 1],
            peers + near,
        )
        returned[1, slab] = updated[1, slab]
        take_all(speeds, recv_u.at[cycle])
        update(transposed, speeds, 0)
        back = back + send_all(
            updated.at[0], returned.at[0], send_e.at[cycle, 0], recv_e.at[cycle, 0],
            peers + near,
        )
        returned[0, slab] = updated[0, slab]
        for copy in outward:
            copy.wait_send()
        take_all(returned.at[1], recv_e.at[cycle, 1])
        take_all(returned.at[0], recv_e.at[cycle, 0])
        for copy in back:
            copy.wait_send()
    out_ref[...] = returned[...]


def shards(ensemble, coupling, obs_column, obs_level, obs_value, obs_error, obs_live, partners):
    mem_count = lax.axis_size("mem")
    grp_count = lax.axis_size("grp")
    hor_count = lax.axis_size("hor")
    slab_count = mem_count * grp_count
    own_slab = lax.axis_index("mem") * grp_count + lax.axis_index("grp")
    lanes = max(128, -(-slab_count // 128) * 128)
    slab_numbers = jnp.arange(lanes, dtype=jnp.int32)
    chosen = partners[0, 0]
    count = chosen.shape[0]
    blend_weights = (slab_numbers == own_slab).astype(jnp.float32)
    blend_weights = blend_weights + jnp.sum(
        (slab_numbers[:, None] == chosen[None, :]).astype(jnp.float32), axis=1
    )
    blend = jnp.broadcast_to(blend_weights, (8, lanes))
    block, fields, levels, width = ensemble.shape
    cycles = obs_column.shape[0]
    members = block * slab_count
    slab_levels = levels // slab_count
    x = ensemble.reshape(block, fields, slab_count, slab_levels, width).transpose(1, 2, 3, 0, 4)
    state = (slab_count, slab_levels, block, width)
    strip = (slab_count, slab_levels, block, LANES)
    tall = (members + 8, members)
    rows = levels * block
    groups = 2 * levels * HALO // LANES
    vmem = pl.BlockSpec(memory_space=pltpu.VMEM)
    dma = pltpu.SemaphoreType.DMA
    f32 = jnp.float32
    result = pl.pallas_call(
        functools.partial(program, (mem_count, grp_count, hor_count), count, cycles),
        out_shape=jax.ShapeDtypeStruct((2,) + state, f32),
        in_specs=[vmem] * 8,
        out_specs=vmem,
        scratch_shapes=[
            pltpu.VMEM((2, rows, rows), jnp.bfloat16),
            pltpu.VMEM(state, f32), pltpu.VMEM(state, f32), pltpu.VMEM(state, f32),
            pltpu.VMEM(strip, f32), pltpu.VMEM(strip, f32), pltpu.VMEM(strip, f32),
            pltpu.VMEM((2, groups, block, LANES), f32),
            pltpu.VMEM((cycles, 2, groups, block, LANES), f32),
            pltpu.VMEM(state, f32), pltpu.VMEM(state, f32),
            pltpu.VMEM((2,) + state, f32), pltpu.VMEM((2,) + state, f32),
            pltpu.VMEM((2, slab_levels * width // LANES, 1, LANES), f32),
            pltpu.VMEM(tall, f32),
            pltpu.VMEM((mem_count - 1,) + tall, f32),
            pltpu.VMEM((grp_count - 1,) + tall, f32),
            pltpu.VMEM((grp_count - 1,) + tall, f32),
            pltpu.VMEM((grp_count - 1,) + blend.shape, f32),
            dma((cycles, 2)), dma((cycles, 2)),
            dma((cycles, mem_count - 1)), dma((cycles, mem_count - 1)),
            dma((grp_count - 1,)), dma((grp_count - 1,)),
            dma((cycles, grp_count - 1)), dma((cycles, grp_count - 1)),
            dma((cycles, slab_count)), dma((cycles, slab_count)),
            dma((cycles, slab_count)), dma((cycles, slab_count)),
            dma((cycles, 2, slab_count)), dma((cycles, 2, slab_count)),
        ],
        compiler_params=pltpu.CompilerParams(collective_id=0, has_side_effects=True),
    )(
        x, coupling, obs_column[:, 0], obs_level[:, 0], obs_value[:, 0], obs_error[:, 0],
        obs_live[:, 0], blend,
    )
    return result.transpose(3, 0, 1, 2, 4).reshape(ensemble.shape)


def solution(mesh):
    in_specs = (
        P(("mem", "grp"), None, None, "hor"),
        P(),
        P(None, ("mem", "grp"), "hor", None),
        P(None, ("mem", "grp"), "hor", None),
        P(None, ("mem", "grp"), "hor", None),
        P(None, ("mem", "grp"), "hor", None),
        P(None, ("mem", "grp"), "hor", None),
        P(("mem", "grp"), "hor", None),
    )
    out_specs = P(("mem", "grp"), None, None, "hor")
    return jax.shard_map(shards, mesh=mesh, in_specs=in_specs, out_specs=out_specs, check_vma=False)
```

```python
import functools

import jax
import jax.numpy as jnp
from jax import lax
from jax.experimental import pallas as pl
from jax.experimental.pallas import tpu as pltpu
from jax.sharding import PartitionSpec as P

SUBSTEPS = 4
ROOT_STEPS = 8
MESH = pl.DeviceIdType.MESH
LANES = 128
HALO = 2 * SUBSTEPS

time_step = 0.2


def split(value):
    high = value.astype(jnp.bfloat16)
    return high, (value - high.astype(jnp.float32)).astype(jnp.bfloat16)


def split3(value):
    high, rest = value.astype(jnp.bfloat16), None
    rest = value - high.astype(jnp.float32)
    middle = rest.astype(jnp.bfloat16)
    low = (rest - middle.astype(jnp.float32)).astype(jnp.bfloat16)
    return high, middle, low


def one(a, b, across=0):
    dims = (((1,), (across,)), ((), ()))
    return lax.dot_general(a, b, dims, preferred_element_type=jnp.float32)


def product(left, right, across=0):
    left_high, left_low = split(left)
    right_high, right_low = split(right)
    return one(left_high, right_high, across) + (
        one(left_high, right_low, across) + one(left_low, right_high, across)
    )


def iota(shape, axis):
    return lax.broadcasted_iota(jnp.int32, shape, axis)


def program(
    sizes, count, cycles,
    x_ref, coupling_ref, column_ref, level_ref, value_ref, error_ref, live_ref, blend_ref,
    out_ref,
    kron, u_ref, h_ref, p_ref, edge_u, edge_h, edge_p, packed, halo,
    heights, speeds, updated, returned, final, relayed, cells, bundle, notes,
    own, column, partial, arrived, blends,
    send_n, recv_n, send_o, recv_o, send_a, recv_a, send_b, recv_b, send_c, recv_c,
    send_h, recv_h, send_u, recv_u, send_e, recv_e, send_f, recv_f,
    send_r, recv_r, send_g,
):
    mem_count, grp_count, hor_count = sizes
    mem = lax.axis_index("mem")
    grp = lax.axis_index("grp")
    hor = lax.axis_index("hor")
    slab_count = mem_count * grp_count
    slab_levels, block, width = x_ref.shape[2:]
    levels = slab_count * slab_levels
    rows = levels * block
    members = slab_count * block

    depth = mem_count // 2
    pairs = hor_count // 2
    pair = hor // 2
    side = lax.rem(hor, 2)
    half = mem // depth
    deep = lax.rem(mem, depth)
    away = half + side - 2 * half * side
    line = side * depth + deep
    slab = line * grp_count + grp
    first_block = mem * grp_count + grp

    def turned(at, step, size):
        return lax.rem(at + step, size)

    def spot(in_half, step_side, step_deep, step_grp):
        to_side = turned(side, step_side, 2)
        to_deep = turned(deep, step_deep, depth)
        to_grp = turned(grp, step_grp, grp_count)
        device = {"mem": in_half * depth + to_deep, "hor": 2 * pair + to_side, "grp": to_grp}
        return device, (to_side * depth + to_deep) * grp_count + to_grp

    steps = [
        (one_side, one_deep, one_grp)
        for one_side in range(2) for one_deep in range(depth) for one_grp in range(grp_count)
    ]
    cube = [spot(half, *step) for step in steps[:0:-1]]
    across = [(at, spot(1 - half, 0, *step[1:])) for at, step in enumerate(steps[: len(steps) // 2])]

    right = ({"hor": turned(hor, 1, hor_count)},
             {"mem": turned(mem, depth, mem_count),
              "hor": 2 * turned(pair, half, pairs) + side})
    left = ({"hor": turned(hor, hor_count - 1, hor_count)},
            {"mem": turned(mem, depth, mem_count),
             "hor": 2 * turned(pair, half + pairs - 1, pairs) + side})

    barrier = pltpu.get_barrier_semaphore()
    for device, _ in cube + [spot(1 - half, *step) for step in steps]:
        pl.semaphore_signal(barrier, inc=1, device_id=device, device_id_type=MESH)
    for device in left + right:
        pl.semaphore_signal(barrier, inc=1, device_id=device, device_id_type=MESH)

    def remote(source, target, send_sem, recv_sem, device):
        return pltpu.make_async_remote_copy(
            src_ref=source, dst_ref=target, send_sem=send_sem, recv_sem=recv_sem,
            device_id=device, device_id_type=MESH,
        )

    def pack(source):
        lane = iota((block, LANES), 1)
        per = LANES // HALO
        for group in range(2 * levels // per):
            low = jnp.zeros((block, LANES), jnp.float32)
            high = jnp.zeros((block, LANES), jnp.float32)
            for at in range(per):
                index = group * per + at
                field, level = index // levels, index % levels
                place = (field, level // slab_levels, level % slab_levels)
                inside = (lane >= at * HALO) & (lane < (at + 1) * HALO)
                first = source[place + (slice(None), slice(0, LANES))]
                last = source[place + (slice(None), slice(width - LANES, width))]
                if at:
                    first = pltpu.roll(first, at * HALO, 1)
                turn = (at * HALO + HALO) % LANES
                if turn:
                    last = pltpu.roll(last, turn, 1)
                low = jnp.where(inside, first, low)
                high = jnp.where(inside, last, high)
            packed[0, group] = low
            packed[1, group] = high

    def send_halo(cycle):
        copies = []
        for at, target in ((0, left[cycle > 0]), (1, right[cycle > 0])):
            copy = remote(
                packed.at[at], halo.at[cycle, at],
                send_n.at[cycle, at], recv_n.at[cycle, at], target,
            )
            copy.start()
            copies.append(copy)
        return copies

    def unpack(source, cycle):
        lane = iota((block, LANES), 1)
        per = LANES // HALO
        for field, target in ((0, edge_u), (1, edge_h)):
            for level in range(levels):
                index = field * levels + level
                group, at = index // per, index % per
                place = (level // slab_levels, level % slab_levels)
                before = halo[cycle, 1, group]
                after = halo[cycle, 0, group]
                if at:
                    before = pltpu.roll(before, LANES - at * HALO, 1)
                turn = (2 * LANES - HALO - at * HALO) % LANES
                if turn:
                    after = pltpu.roll(after, turn, 1)
                first = source[(field,) + place + (slice(None), slice(0, LANES))]
                last = source[(field,) + place + (slice(None), slice(width - LANES, width))]
                mixed = jnp.where(
                    lane < LANES // 2,
                    pltpu.roll(first, HALO, 1), pltpu.roll(last, LANES - HALO, 1),
                )
                mixed = jnp.where(lane < HALO, before, mixed)
                target[place] = jnp.where(lane >= LANES - HALO, after, mixed)

    def centred(field):
        return (pltpu.roll(field, field.shape[-1] - 1, 1) - pltpu.roll(field, 1, 1)) * 0.5

    def substep(read_u, read_h, write_u, write_h, press):
        span = press.shape[-1]
        for at in range(span // LANES):
            lanes = slice(at * LANES, (at + 1) * LANES)
            high, low = split(read_h(slice(0, slab_count), lanes).reshape(rows, LANES))
            result = one(kron[0], high) + (one(kron[0], low) + one(kron[1], high))
            press[:, :, :, lanes] = result.reshape(slab_count, slab_levels, block, LANES)
        everything = slice(0, span)

        for at in range(slab_count):
            part = slice(at, at + 1)
            size = (slab_levels * block, span)
            velocity = read_u(part, everything).reshape(size)
            height = read_h(part, everything).reshape(size)
            pressure = press[part].reshape(size)
            moved = velocity - time_step * (velocity * centred(velocity) + centred(pressure))
            risen = height - time_step * centred(moved * height)
            write_u[part] = moved.reshape(1, slab_levels, block, span)
            write_h[part] = risen.reshape(1, slab_levels, block, span)

    def reader(ref):
        return lambda part, lanes: ref[part, :, :, lanes]

    def field_reader(ref, field):
        return lambda part, lanes: ref[field, part, :, :, lanes]

    def advance(source, cycle, copies):
        substep(field_reader(source, 0), field_reader(source, 1), u_ref, h_ref, p_ref)

        def again(step, carry):
            substep(reader(u_ref), reader(h_ref), u_ref, h_ref, p_ref)
            return carry

        lax.fori_loop(1, SUBSTEPS, again, 0)
        for copy in copies:
            copy.wait()
        unpack(source, cycle)

        def edge(step, carry):
            substep(reader(edge_u), reader(edge_h), edge_u, edge_h, edge_p)
            return carry

        lax.fori_loop(0, SUBSTEPS, edge, 0)
        lane = iota((block, LANES), 1)
        for strip, whole in ((edge_h, h_ref), (edge_u, u_ref)):
            for at in range(slab_count):
                for level in range(slab_levels):
                    fresh = strip[at, level]
                    first = whole[at, level, :, 0:LANES]
                    last = whole[at, level, :, width - LANES : width]
                    whole[at, level, :, 0:LANES] = jnp.where(
                        lane < HALO, pltpu.roll(fresh, LANES - HALO, 1), first
                    )
                    whole[at, level, :, width - LANES : width] = jnp.where(
                        lane >= LANES - HALO, pltpu.roll(fresh, HALO, 1), last
                    )

    def arrive(target, recv_sem, other):
        remote(
            target.at[other], target.at[other], recv_sem.at[other], recv_sem.at[other], {"hor": hor}
        ).wait_recv()

    def cube_send(source, target, send_sem, recv_sem):
        copies = []
        for device, other in cube:
            copy = remote(
                source.at[other], target.at[slab], send_sem.at[other], recv_sem.at[slab], device
            )
            copy.start()
            copies.append(copy)
        return copies

    def cube_take(target, recv_sem):
        for _, other in cube:
            arrive(target, recv_sem, other)

    def relay_copy(field, source, at, other):
        return remote(
            source.at[other], relayed.at[field, at], send_r.at[field, at], recv_r.at[field, at],
            {"hor": 2 * pair + 1 - side},
        )

    def inward_relay(field, source):
        @pl.when(away == 1)
        def _():
            for at, step in enumerate(steps[: len(steps) // 2]):
                relay_copy(field, source, at, spot(half, 1, *step[1:])[1]).start()

    def inward_copies(spots, source, target, send_sem, recv_sem):
        return [
            remote(
                source.at[other], target.at[first_block],
                send_sem.at[other], recv_sem.at[first_block], device,
            )
            for device, other in spots
        ]

    straight = [there for _, there in across]

    def forward_copy(field, target, recv_sem, at, device):
        return remote(
            relayed.at[field, at], target.at[first_block],
            send_g.at[field, at], recv_sem.at[first_block], device,
        )

    def inward_send(field, source, target, send_sem, recv_sem):
        @pl.when(away == 1)
        def _():
            for copy in inward_copies(straight, source, target, send_sem, recv_sem):
                copy.start()

        @pl.when(away == 0)
        def _():
            for copy in inward_copies(cube, source, target, send_sem, recv_sem):
                copy.start()
            for at, (device, other) in across:
                relay_copy(field, source, at, other).wait_recv()
                forward_copy(field, target, recv_sem, at, device).start()

    def inward_drain(field, source, target, send_sem, recv_sem):
        @pl.when(away == 1)
        def _():
            for copy in inward_copies(straight, source, target, send_sem, recv_sem):
                copy.wait_send()
            for at, step in enumerate(steps[: len(steps) // 2]):
                relay_copy(field, source, at, spot(half, 1, *step[1:])[1]).wait_send()

        @pl.when(away == 0)
        def _():
            for copy in inward_copies(cube, source, target, send_sem, recv_sem):
                copy.wait_send()
            for at, (device, other) in across:
                forward_copy(field, target, recv_sem, at, device).wait_send()

    def inward_take(target, recv_sem):
        for step_mem in range(mem_count):
            for step_grp in range(grp_count):
                other = turned(mem, step_mem, mem_count) * grp_count + turned(grp, step_grp, grp_count)
                if step_mem + step_grp:
                    arrive(target, recv_sem, other)
                else:
                    @pl.when(away == 1)
                    def _():
                        arrive(target, recv_sem, other)

    def outward_copies(field):
        copies = []
        for step_mem in range(mem_count):
            for step_grp in range(grp_count):
                to_mem = turned(mem, step_mem, mem_count)
                to_grp = turned(grp, step_grp, grp_count)
                other = to_mem * grp_count + to_grp
                copies.append(remote(
                    updated.at[field, other], final.at[field, slab],
                    send_f.at[field, other], recv_f.at[field, slab],
                    {"mem": to_mem, "hor": 2 * pair + half, "grp": to_grp},
                ))
        return copies

    def outward_send(field):
        copies = outward_copies(field)

        @pl.when(away == 1)
        def _():
            copies[0].start()

        for copy in copies[1:]:
            copy.start()

        @pl.when(away == 0)
        def _():
            final[field, slab] = updated[field, slab]

    def outward_finish(field):
        for at in range(slab_count):
            other = turned(slab, at, slab_count)
            if at:
                arrive(final.at[field], recv_f.at[field], other)
            else:
                @pl.when(away == 1)
                def _():
                    arrive(final.at[field], recv_f.at[field], other)
        copies = outward_copies(field)

        @pl.when(away == 1)
        def _():
            copies[0].wait_send()

        for copy in copies[1:]:
            copy.wait_send()

    def bundle_copy():
        return remote(
            bundle, notes, send_o.at[0], recv_o.at[0],
            {"mem": turned(mem, depth, mem_count), "hor": 2 * pair + 1 - side},
        )

    def sum_cells(cycle):
        place = notes[cycle, 0:1].astype(jnp.int32)
        weight = notes[cycle, 1:2]
        pulled = notes[cycle, 2:3]
        parts = split3(weight) + split3(pulled)
        spare = jnp.zeros((16 - len(parts), weight.shape[1]), jnp.bfloat16)
        lhs = jnp.concatenate(parts + (spare,), axis=0)
        total = slab_levels * width

        def chunk(at, carry):
            numbers = iota((LANES, weight.shape[1]), 0) + at * LANES
            hits = jnp.where(numbers == place, 1.0, 0.0).astype(jnp.bfloat16)
            sums = one(lhs, hits, 1)
            cells[0, at] = sums[0:1] + (sums[1:2] + sums[2:3])
            cells[1, at] = sums[3:4] + (sums[4:5] + sums[5:6])
            return carry

        lax.fori_loop(0, total // LANES, chunk, 0)

    def gram():
        per = width // LANES
        total = None
        for level in range(slab_levels):
            flat = heights[:, level].reshape(members, width)
            average = jnp.mean(flat, axis=0, keepdims=True)
            anomalies = flat - average
            weight = jnp.concatenate(
                [cells[0, level * per + at] for at in range(per)], axis=1
            )
            pulled = jnp.concatenate(
                [cells[1, level * per + at] for at in range(per)], axis=1
            )
            pull = pulled - weight * average
            lhs = jnp.concatenate(
                [anomalies * weight, jnp.broadcast_to(pull, (8, width))], axis=0
            )
            here = product(lhs, anomalies, 1)
            total = here if total is None else total + here
        own[...] = total

    lanes = iota((1, blend_ref.shape[1]), 1)

    def share(row, step):
        place = turned(line, mem_count - step, mem_count) * grp_count + grp
        return jnp.sum(jnp.where(lanes == place, row[0:1], 0.0), axis=1, keepdims=True)

    def blended_for(row):
        total = share(row, 0) * own[...]
        for step in range(1, mem_count):
            total = total + share(row, step) * column[step - 1]
        return total

    def root(total):
        total = total / (count + 1.0)
        square = (members, members)
        identity = (iota(square, 0) == iota(square, 1)).astype(jnp.float32)
        blended = (members - 1.0) * identity + total[:members]
        bvector = total[members:]
        squares = jnp.sum(
            jnp.sum(blended * blended, axis=1, keepdims=True), axis=0, keepdims=True
        )
        frobenius = jnp.sqrt(squares)
        iterate = blended / frobenius
        newton = 1.5 * identity - 0.5 * iterate
        inverse_root = newton
        for step in range(1, ROOT_STEPS):
            iterate = product(newton, iterate)
            newton = 1.5 * identity - 0.5 * product(inverse_root, iterate)
            inverse_root = product(newton, inverse_root)
        spread = inverse_root * (jnp.sqrt(members - 1.0) / jnp.sqrt(frobenius))
        inner = product(bvector, inverse_root)
        mean_weight = product(inner, inverse_root) / frobenius
        return spread + mean_weight[0:1]

    def update(transposed, source, field):
        high, low = split(transposed)
        for level in range(slab_levels):
            flat = source[:, level].reshape(members, width)
            average = jnp.mean(flat, axis=0, keepdims=True)
            flat_high, flat_low = split(flat - average)
            result = average + (
                one(high, flat_high) + (one(high, flat_low) + one(low, flat_high))
            )
            updated[field, :, level] = result.reshape(slab_count, block, width)

    pack(x_ref)
    for cycle in range(cycles):
        weight = live_ref[cycle].astype(jnp.float32) / error_ref[cycle]
        place = level_ref[cycle] * width + column_ref[cycle]
        bundle[cycle, 0:1] = place.astype(jnp.float32)
        bundle[cycle, 1:2] = weight
        bundle[cycle, 2:3] = weight * value_ref[cycle]
    bundle[cycles, :, 0 : blend_ref.shape[1]] = blend_ref[...]
    pl.semaphore_wait(barrier, 2 * slab_count - 1 + 4)
    copies = send_halo(0)

    @pl.when(away == 1)
    def _():
        bundle_copy().start()

    @pl.when(away == 0)
    def _():
        notes[...] = bundle[...]

    spread_rows = jnp.where(
        iota((rows, levels), 0) // block == iota((rows, levels), 1), 1.0, 0.0
    ).astype(jnp.bfloat16)
    same = lax.rem(iota((rows, rows), 0), block) == lax.rem(iota((rows, rows), 1), block)
    for at, part in enumerate(split(coupling_ref[...])):
        tall = one(spread_rows, part).astype(jnp.bfloat16)
        kron[at] = jnp.where(same, one(tall, spread_rows, 1), 0.0).astype(jnp.bfloat16)

    blend_copies = []
    for cycle in range(cycles):
        source = x_ref if cycle == 0 else returned
        if cycle:
            pack(source)
            copies = send_halo(cycle)
        advance(source, cycle, copies)
        heights_now = (h_ref, heights, send_h.at[cycle], recv_h.at[cycle])
        speeds_now = (u_ref, speeds, send_u.at[cycle], recv_u.at[cycle])
        drains = []
        if cycle == 0:
            inward_relay(1, h_ref)
            inward_send(1, *heights_now)
            inward_relay(0, u_ref)

            @pl.when(away == 1)
            def _():
                bundle_copy().wait()

            @pl.when(away == 0)
            def _():
                heights[slab] = h_ref[slab]
                speeds[slab] = u_ref[slab]

            blends[0] = notes[cycles, 0:8, 0 : blend_ref.shape[1]]
            for step in range(1, grp_count):
                copy = remote(
                    blends.at[0], blends.at[step], send_b.at[step], recv_b.at[step],
                    {"grp": turned(grp, step, grp_count)},
                )
                copy.start()
                blend_copies.append(copy)
        else:
            drains = cube_send(*heights_now)
            heights[slab] = h_ref[slab]
            speeds[slab] = u_ref[slab]
        sum_cells(cycle)
        if cycle == 0:
            inward_take(heights, recv_h.at[cycle])
        else:
            cube_take(heights, recv_h.at[cycle])
        gram()

        gathers = []
        for step in range(1, mem_count):
            to_line = turned(line, step, mem_count)
            copy = remote(
                own, column.at[step - 1], send_a.at[cycle, step - 1], recv_a.at[cycle, step - 1],
                {"mem": half * depth + lax.rem(to_line, depth), "hor": 2 * pair + to_line // depth},
            )
            copy.start()
            gathers.append(copy)
        if cycle == 0:
            inward_send(0, *speeds_now)
        else:
            drains = drains + cube_send(*speeds_now)
        for copy in blend_copies:
            copy.wait()
        blend_copies = []
        for copy in gathers:
            copy.wait()
        returns = []
        for step in range(1, grp_count):
            partial[step - 1] = blended_for(blends[step])
            copy = remote(
                partial.at[step - 1], arrived.at[step - 1],
                send_c.at[cycle, step - 1], recv_c.at[cycle, step - 1],
                {"grp": turned(grp, grp_count - step, grp_count)},
            )
            copy.start()
            returns.append(copy)
        total = blended_for(blends[0])
        for copy in returns:
            copy.wait()
        for step in range(1, grp_count):
            total = total + arrived[step - 1]
        transposed = root(total)
        last = cycle == cycles - 1
        for field, patch in ((1, heights), (0, speeds)):
            if field == 0:
                if cycle == 0:
                    inward_take(speeds, recv_u.at[cycle])
                else:
                    cube_take(speeds, recv_u.at[cycle])
            update(transposed, patch, field)
            if last:
                outward_send(field)
            else:
                drains = drains + cube_send(
                    updated.at[field], returned.at[field],
                    send_e.at[cycle, field], recv_e.at[cycle, field],
                )
                returned[field, slab] = updated[field, slab]
        if not last:
            for field in (1, 0):
                cube_take(returned.at[field], recv_e.at[cycle, field])
        for copy in drains:
            copy.wait_send()
        if cycle == 0:
            inward_drain(1, *heights_now)
            inward_drain(0, *speeds_now)
    for field in (1, 0):
        outward_finish(field)
    out_ref[...] = final[...]


def shards(ensemble, coupling, obs_column, obs_level, obs_value, obs_error, obs_live, partners):
    mem_count = lax.axis_size("mem")
    grp_count = lax.axis_size("grp")
    hor_count = lax.axis_size("hor")
    slab_count = mem_count * grp_count
    own_slab = lax.axis_index("mem") * grp_count + lax.axis_index("grp")
    lanes = max(128, -(-slab_count // 128) * 128)
    slab_numbers = jnp.arange(lanes, dtype=jnp.int32)
    chosen = partners[0, 0]
    count = chosen.shape[0]
    blend_weights = (slab_numbers == own_slab).astype(jnp.float32)
    blend_weights = blend_weights + jnp.sum(
        (slab_numbers[:, None] == chosen[None, :]).astype(jnp.float32), axis=1
    )
    blend = jnp.broadcast_to(blend_weights, (8, lanes))
    block, fields, levels, width = ensemble.shape
    cycles = obs_column.shape[0]
    members = block * slab_count
    slab_levels = levels // slab_count
    x = ensemble.reshape(block, fields, slab_count, slab_levels, width).transpose(1, 2, 3, 0, 4)
    state = (slab_count, slab_levels, block, width)
    strip = (slab_count, slab_levels, block, LANES)
    tall = (members + 8, members)
    rows = levels * block
    groups = 2 * levels * HALO // LANES
    slots = max(obs_column.shape[-1], lanes)
    vmem = pl.BlockSpec(memory_space=pltpu.VMEM)
    dma = pltpu.SemaphoreType.DMA
    f32 = jnp.float32
    result = pl.pallas_call(
        functools.partial(program, (mem_count, grp_count, hor_count), count, cycles),
        out_shape=jax.ShapeDtypeStruct((2,) + state, f32),
        in_specs=[vmem] * 8,
        out_specs=vmem,
        scratch_shapes=[
            pltpu.VMEM((2, rows, rows), jnp.bfloat16),
            pltpu.VMEM(state, f32), pltpu.VMEM(state, f32), pltpu.VMEM(state, f32),
            pltpu.VMEM(strip, f32), pltpu.VMEM(strip, f32), pltpu.VMEM(strip, f32),
            pltpu.VMEM((2, groups, block, LANES), f32),
            pltpu.VMEM((cycles, 2, groups, block, LANES), f32),
            pltpu.VMEM(state, f32), pltpu.VMEM(state, f32),
            pltpu.VMEM((2,) + state, f32), pltpu.VMEM((2,) + state, f32),
            pltpu.VMEM((2,) + state, f32),
            pltpu.VMEM((2, slab_count // 2) + state[1:], f32),
            pltpu.VMEM((2, slab_levels * width // LANES, 1, LANES), f32),
            pltpu.VMEM((cycles + 1, 8, slots), f32), pltpu.VMEM((cycles + 1, 8, slots), f32),
            pltpu.VMEM(tall, f32),
            pltpu.VMEM((mem_count - 1,) + tall, f32),
            pltpu.VMEM((grp_count - 1,) + tall, f32),
            pltpu.VMEM((grp_count - 1,) + tall, f32),
            pltpu.VMEM((grp_count,) + blend.shape, f32),
            dma((cycles, 2)), dma((cycles, 2)),
            dma((1,)), dma((1,)),
            dma((cycles, mem_count - 1)), dma((cycles, mem_count - 1)),
            dma((grp_count,)), dma((grp_count,)),
            dma((cycles, grp_count - 1)), dma((cycles, grp_count - 1)),
            dma((cycles, slab_count)), dma((cycles, slab_count)),
            dma((cycles, slab_count)), dma((cycles, slab_count)),
            dma((cycles, 2, slab_count)), dma((cycles, 2, slab_count)),
            dma((2, slab_count)), dma((2, slab_count)),
            dma((2, slab_count // 2)), dma((2, slab_count // 2)), dma((2, slab_count // 2)),
        ],
        compiler_params=pltpu.CompilerParams(collective_id=0, has_side_effects=True),
    )(
        x, coupling, obs_column[:, 0], obs_level[:, 0], obs_value[:, 0], obs_error[:, 0],
        obs_live[:, 0], blend,
    )
    return result.transpose(3, 0, 1, 2, 4).reshape(ensemble.shape)


def solution(mesh):
    in_specs = (
        P(("mem", "grp"), None, None, "hor"),
        P(),
        P(None, ("mem", "grp"), "hor", None),
        P(None, ("mem", "grp"), "hor", None),
        P(None, ("mem", "grp"), "hor", None),
        P(None, ("mem", "grp"), "hor", None),
        P(None, ("mem", "grp"), "hor", None),
        P(("mem", "grp"), "hor", None),
    )
    out_specs = P(("mem", "grp"), None, None, "hor")
    return jax.shard_map(shards, mesh=mesh, in_specs=in_specs, out_specs=out_specs, check_vma=False)
```

```python
import functools

import jax
import jax.numpy as jnp
from jax import lax
from jax.experimental import pallas as pl
from jax.experimental.pallas import tpu as pltpu
from jax.sharding import PartitionSpec as P

SUBSTEPS = 4
ROOT_STEPS = 8
MESH = pl.DeviceIdType.MESH
LANES = 128
HALO = 2 * SUBSTEPS

time_step = 0.2


def split(value):
    high = value.astype(jnp.bfloat16)
    return high, (value - high.astype(jnp.float32)).astype(jnp.bfloat16)


def split3(value):
    high, rest = value.astype(jnp.bfloat16), None
    rest = value - high.astype(jnp.float32)
    middle = rest.astype(jnp.bfloat16)
    low = (rest - middle.astype(jnp.float32)).astype(jnp.bfloat16)
    return high, middle, low


def one(a, b, across=0):
    dims = (((1,), (across,)), ((), ()))
    return lax.dot_general(a, b, dims, preferred_element_type=jnp.float32)


def product(left, right, across=0):
    left_high, left_low = split(left)
    right_high, right_low = split(right)
    return one(left_high, right_high, across) + (
        one(left_high, right_low, across) + one(left_low, right_high, across)
    )


def iota(shape, axis):
    return lax.broadcasted_iota(jnp.int32, shape, axis)


def program(
    sizes, count, cycles,
    given_ref, coupling_ref, column_ref, level_ref, value_ref, error_ref, live_ref, chosen_ref,
    out_ref,
    x_ref, kron, u_ref, h_ref, p_ref, edge_u, edge_h, edge_p, packed, halo,
    heights, speeds, updated, returned, final, relayed, cells, bundle, notes,
    own, column, partial, arrived, blends,
    send_n, recv_n, send_o, recv_o, send_a, recv_a, send_b, recv_b, send_c, recv_c,
    send_h, recv_h, send_u, recv_u, send_e, recv_e, send_f, recv_f,
    send_r, recv_r, send_g,
):
    mem_count, grp_count, hor_count = sizes
    mem = lax.axis_index("mem")
    grp = lax.axis_index("grp")
    hor = lax.axis_index("hor")
    slab_count = mem_count * grp_count
    slab_levels, block, width = x_ref.shape[2:]
    lane_count = blends.shape[2]
    levels = slab_count * slab_levels
    rows = levels * block
    members = slab_count * block

    depth = mem_count // 2
    pairs = hor_count // 2
    pair = hor // 2
    side = lax.rem(hor, 2)
    half = mem // depth
    deep = lax.rem(mem, depth)
    away = half + side - 2 * half * side
    line = side * depth + deep
    slab = line * grp_count + grp
    first_block = mem * grp_count + grp

    def turned(at, step, size):
        return lax.rem(at + step, size)

    def spot(in_half, step_side, step_deep, step_grp):
        to_side = turned(side, step_side, 2)
        to_deep = turned(deep, step_deep, depth)
        to_grp = turned(grp, step_grp, grp_count)
        device = {"mem": in_half * depth + to_deep, "hor": 2 * pair + to_side, "grp": to_grp}
        return device, (to_side * depth + to_deep) * grp_count + to_grp

    steps = [
        (one_side, one_deep, one_grp)
        for one_side in range(2) for one_deep in range(depth) for one_grp in range(grp_count)
    ]
    cube = [spot(half, *step) for step in steps[:0:-1]]
    across = [(at, spot(1 - half, 0, *step[1:])) for at, step in enumerate(steps[: len(steps) // 2])]

    right = ({"hor": turned(hor, 1, hor_count)},
             {"mem": turned(mem, depth, mem_count),
              "hor": 2 * turned(pair, half, pairs) + side})
    left = ({"hor": turned(hor, hor_count - 1, hor_count)},
            {"mem": turned(mem, depth, mem_count),
             "hor": 2 * turned(pair, half + pairs - 1, pairs) + side})

    barrier = pltpu.get_barrier_semaphore()
    for device, _ in cube + [spot(1 - half, *step) for step in steps]:
        pl.semaphore_signal(barrier, inc=1, device_id=device, device_id_type=MESH)
    for device in left + right:
        pl.semaphore_signal(barrier, inc=1, device_id=device, device_id_type=MESH)

    def remote(source, target, send_sem, recv_sem, device):
        return pltpu.make_async_remote_copy(
            src_ref=source, dst_ref=target, send_sem=send_sem, recv_sem=recv_sem,
            device_id=device, device_id_type=MESH,
        )

    def pack(source):
        lane = iota((block, LANES), 1)
        per = LANES // HALO
        for group in range(2 * levels // per):
            low = jnp.zeros((block, LANES), jnp.float32)
            high = jnp.zeros((block, LANES), jnp.float32)
            for at in range(per):
                index = group * per + at
                field, level = index // levels, index % levels
                place = (field, level // slab_levels, level % slab_levels)
                inside = (lane >= at * HALO) & (lane < (at + 1) * HALO)
                first = source[place + (slice(None), slice(0, LANES))]
                last = source[place + (slice(None), slice(width - LANES, width))]
                if at:
                    first = pltpu.roll(first, at * HALO, 1)
                turn = (at * HALO + HALO) % LANES
                if turn:
                    last = pltpu.roll(last, turn, 1)
                low = jnp.where(inside, first, low)
                high = jnp.where(inside, last, high)
            packed[0, group] = low
            packed[1, group] = high

    def send_halo(cycle):
        copies = []
        for at, target in ((0, left[cycle > 0]), (1, right[cycle > 0])):
            copy = remote(
                packed.at[at], halo.at[cycle, at],
                send_n.at[cycle, at], recv_n.at[cycle, at], target,
            )
            copy.start()
            copies.append(copy)
        return copies

    def unpack(source, cycle):
        lane = iota((block, LANES), 1)
        per = LANES // HALO
        for field, target in ((0, edge_u), (1, edge_h)):
            for level in range(levels):
                index = field * levels + level
                group, at = index // per, index % per
                place = (level // slab_levels, level % slab_levels)
                before = halo[cycle, 1, group]
                after = halo[cycle, 0, group]
                if at:
                    before = pltpu.roll(before, LANES - at * HALO, 1)
                turn = (2 * LANES - HALO - at * HALO) % LANES
                if turn:
                    after = pltpu.roll(after, turn, 1)
                first = source[(field,) + place + (slice(None), slice(0, LANES))]
                last = source[(field,) + place + (slice(None), slice(width - LANES, width))]
                mixed = jnp.where(
                    lane < LANES // 2,
                    pltpu.roll(first, HALO, 1), pltpu.roll(last, LANES - HALO, 1),
                )
                mixed = jnp.where(lane < HALO, before, mixed)
                target[place] = jnp.where(lane >= LANES - HALO, after, mixed)

    def centred(field):
        return (pltpu.roll(field, field.shape[-1] - 1, 1) - pltpu.roll(field, 1, 1)) * 0.5

    def substep(read_u, read_h, write_u, write_h, press):
        span = press.shape[-1]
        for at in range(span // LANES):
            lanes = slice(at * LANES, (at + 1) * LANES)
            high, low = split(read_h(slice(0, slab_count), lanes).reshape(rows, LANES))
            result = one(kron[0], high) + (one(kron[0], low) + one(kron[1], high))
            press[:, :, :, lanes] = result.reshape(slab_count, slab_levels, block, LANES)
        everything = slice(0, span)

        for at in range(slab_count):
            part = slice(at, at + 1)
            size = (slab_levels * block, span)
            velocity = read_u(part, everything).reshape(size)
            height = read_h(part, everything).reshape(size)
            pressure = press[part].reshape(size)
            moved = velocity - time_step * (velocity * centred(velocity) + centred(pressure))
            risen = height - time_step * centred(moved * height)
            write_u[part] = moved.reshape(1, slab_levels, block, span)
            write_h[part] = risen.reshape(1, slab_levels, block, span)

    def reader(ref):
        return lambda part, lanes: ref[part, :, :, lanes]

    def field_reader(ref, field):
        return lambda part, lanes: ref[field, part, :, :, lanes]

    def advance(source, cycle, greet):
        substep(field_reader(source, 0), field_reader(source, 1), u_ref, h_ref, p_ref)

        def again(step, carry):
            substep(reader(u_ref), reader(h_ref), u_ref, h_ref, p_ref)
            return carry

        ahead = SUBSTEPS // 2 if cycle == 0 else 1
        if ahead > 1:
            lax.fori_loop(1, ahead, again, 0)
        copies = greet()
        lax.fori_loop(ahead, SUBSTEPS, again, 0)
        for copy in copies:
            copy.wait()
        unpack(source, cycle)

        def edge(step, carry):
            substep(reader(edge_u), reader(edge_h), edge_u, edge_h, edge_p)
            return carry

        lax.fori_loop(0, SUBSTEPS, edge, 0)
        lane = iota((block, LANES), 1)
        for strip, whole in ((edge_h, h_ref), (edge_u, u_ref)):
            for at in range(slab_count):
                for level in range(slab_levels):
                    fresh = strip[at, level]
                    first = whole[at, level, :, 0:LANES]
                    last = whole[at, level, :, width - LANES : width]
                    whole[at, level, :, 0:LANES] = jnp.where(
                        lane < HALO, pltpu.roll(fresh, LANES - HALO, 1), first
                    )
                    whole[at, level, :, width - LANES : width] = jnp.where(
                        lane >= LANES - HALO, pltpu.roll(fresh, HALO, 1), last
                    )

    def arrive(target, recv_sem, other):
        remote(
            target.at[other], target.at[other], recv_sem.at[other], recv_sem.at[other], {"hor": hor}
        ).wait_recv()

    def cube_send(source, target, send_sem, recv_sem):
        copies = []
        for device, other in cube:
            copy = remote(
                source.at[other], target.at[slab], send_sem.at[other], recv_sem.at[slab], device
            )
            copy.start()
            copies.append(copy)
        return copies

    def cube_take(target, recv_sem):
        for _, other in cube:
            arrive(target, recv_sem, other)

    def relay_copy(field, source, at, other):
        return remote(
            source.at[other], relayed.at[field, at], send_r.at[field, at], recv_r.at[field, at],
            {"hor": 2 * pair + 1 - side},
        )

    def inward_relay(field, source):
        @pl.when(away == 1)
        def _():
            for at, step in enumerate(steps[: len(steps) // 2]):
                relay_copy(field, source, at, spot(half, 1, *step[1:])[1]).start()

    def inward_copies(spots, source, target, send_sem, recv_sem):
        return [
            remote(
                source.at[other], target.at[first_block],
                send_sem.at[other], recv_sem.at[first_block], device,
            )
            for device, other in spots
        ]

    straight = [there for _, there in across]

    def forward_copy(field, target, recv_sem, at, device):
        return remote(
            relayed.at[field, at], target.at[first_block],
            send_g.at[field, at], recv_sem.at[first_block], device,
        )

    def inward_send(field, source, target, send_sem, recv_sem):
        @pl.when(away == 1)
        def _():
            for copy in inward_copies(straight, source, target, send_sem, recv_sem):
                copy.start()

        @pl.when(away == 0)
        def _():
            for copy in inward_copies(cube, source, target, send_sem, recv_sem):
                copy.start()
            for at, (device, other) in across:
                relay_copy(field, source, at, other).wait_recv()
                forward_copy(field, target, recv_sem, at, device).start()

    def inward_drain(field, source, target, send_sem, recv_sem):
        @pl.when(away == 1)
        def _():
            for copy in inward_copies(straight, source, target, send_sem, recv_sem):
                copy.wait_send()
            for at, step in enumerate(steps[: len(steps) // 2]):
                relay_copy(field, source, at, spot(half, 1, *step[1:])[1]).wait_send()

        @pl.when(away == 0)
        def _():
            for copy in inward_copies(cube, source, target, send_sem, recv_sem):
                copy.wait_send()
            for at, (device, other) in across:
                forward_copy(field, target, recv_sem, at, device).wait_send()

    def inward_take(target, recv_sem):
        for step_mem in range(mem_count):
            for step_grp in range(grp_count):
                other = turned(mem, step_mem, mem_count) * grp_count + turned(grp, step_grp, grp_count)
                if step_mem + step_grp:
                    arrive(target, recv_sem, other)
                else:
                    @pl.when(away == 1)
                    def _():
                        arrive(target, recv_sem, other)

    def outward_copies(field):
        copies = []
        for step_mem in range(mem_count):
            for step_grp in range(grp_count):
                to_mem = turned(mem, step_mem, mem_count)
                to_grp = turned(grp, step_grp, grp_count)
                other = to_mem * grp_count + to_grp
                copies.append(remote(
                    updated.at[field, other], final.at[field, slab],
                    send_f.at[field, other], recv_f.at[field, slab],
                    {"mem": to_mem, "hor": 2 * pair + half, "grp": to_grp},
                ))
        return copies

    def outward_send(field):
        copies = outward_copies(field)

        @pl.when(away == 1)
        def _():
            copies[0].start()

        for copy in copies[1:]:
            copy.start()

        @pl.when(away == 0)
        def _():
            final[field, slab] = updated[field, slab]

    def outward_finish(field):
        for at in range(slab_count):
            other = turned(slab, at, slab_count)
            if at:
                arrive(final.at[field], recv_f.at[field], other)
            else:
                @pl.when(away == 1)
                def _():
                    arrive(final.at[field], recv_f.at[field], other)
        copies = outward_copies(field)

        @pl.when(away == 1)
        def _():
            copies[0].wait_send()

        for copy in copies[1:]:
            copy.wait_send()

    def bundle_copy():
        return remote(
            bundle, notes, send_o.at[0], recv_o.at[0],
            {"mem": turned(mem, depth, mem_count), "hor": 2 * pair + 1 - side},
        )

    def sum_cells(cycle):
        place = notes[cycle, 0:1].astype(jnp.int32)
        weight = notes[cycle, 1:2]
        pulled = notes[cycle, 2:3]
        parts = split3(weight) + split3(pulled)
        spare = jnp.zeros((16 - len(parts), weight.shape[1]), jnp.bfloat16)
        lhs = jnp.concatenate(parts + (spare,), axis=0)
        total = slab_levels * width

        def chunk(at, carry):
            numbers = iota((LANES, weight.shape[1]), 0) + at * LANES
            hits = jnp.where(numbers == place, 1.0, 0.0).astype(jnp.bfloat16)
            sums = one(lhs, hits, 1)
            cells[0, at] = sums[0:1] + (sums[1:2] + sums[2:3])
            cells[1, at] = sums[3:4] + (sums[4:5] + sums[5:6])
            return carry

        lax.fori_loop(0, total // LANES, chunk, 0)

    def gram():
        per = width // LANES
        total = None
        for level in range(slab_levels):
            flat = heights[:, level].reshape(members, width)
            average = jnp.mean(flat, axis=0, keepdims=True)
            anomalies = flat - average
            weight = jnp.concatenate(
                [cells[0, level * per + at] for at in range(per)], axis=1
            )
            pulled = jnp.concatenate(
                [cells[1, level * per + at] for at in range(per)], axis=1
            )
            pull = pulled - weight * average
            lhs = jnp.concatenate(
                [anomalies * weight, jnp.broadcast_to(pull, (8, width))], axis=0
            )
            here = product(lhs, anomalies, 1)
            total = here if total is None else total + here
        short = members // 2
        row, lane = iota((short, members), 0), iota((short, members), 1)
        upper = total[:short]
        own[:short] = jnp.where(
            lane - short > row, pltpu.roll(upper, short, 1), total[short:members]
        )
        diagonal = jnp.sum(jnp.where(lane == row, upper, 0.0), axis=0, keepdims=True)
        own[short:] = jnp.where(
            iota((8, members), 0) == 0, total[members:], jnp.broadcast_to(diagonal, (8, members))
        )

    def unfold(total):
        short = members // 2
        row, lane = iota((short, members), 0), iota((short, members), 1)
        lower = total[:short]
        turned_over = jnp.transpose(jnp.concatenate([lower, lower], axis=0))
        first, second = turned_over[:short], turned_over[short:]
        inside = jnp.where(lane < row, second, total[short + 1 : short + 2])
        inside = jnp.where(lane > row, pltpu.roll(lower, short, 1), inside)
        top = jnp.where(lane >= short, first, inside)
        bottom = jnp.where(lane - short > row, second, lower)
        return jnp.concatenate([top, bottom], axis=0), total[short : short + 1]

    lanes = iota((1, lane_count), 1)

    def share(row, step):
        place = turned(line, mem_count - step, mem_count) * grp_count + grp
        return jnp.sum(jnp.where(lanes == place, row[0:1], 0.0), axis=1, keepdims=True)

    def blended_for(row):
        total = share(row, 0) * own[...]
        for step in range(1, mem_count):
            total = total + share(row, step) * column[step - 1]
        return total

    def root(total):
        total = total / (count + 1.0)
        square = (members, members)
        identity = (iota(square, 0) == iota(square, 1)).astype(jnp.float32)
        whole, bvector = unfold(total)
        blended = (members - 1.0) * identity + whole
        bvector = jnp.broadcast_to(bvector, (8, members))
        squares = jnp.sum(
            jnp.sum(blended * blended, axis=1, keepdims=True), axis=0, keepdims=True
        )
        frobenius = jnp.sqrt(squares)
        iterate = blended / frobenius
        newton = 1.5 * identity - 0.5 * iterate
        inverse_root = newton
        for step in range(1, ROOT_STEPS):
            iterate = product(newton, iterate)
            newton = 1.5 * identity - 0.5 * product(inverse_root, iterate)
            inverse_root = product(newton, inverse_root)
        spread = inverse_root * (jnp.sqrt(members - 1.0) / jnp.sqrt(frobenius))
        inner = product(bvector, inverse_root)
        mean_weight = product(inner, inverse_root) / frobenius
        return spread + mean_weight[0:1]

    def update(transposed, source, field):
        high, low = split(transposed)
        for level in range(slab_levels):
            flat = source[:, level].reshape(members, width)
            average = jnp.mean(flat, axis=0, keepdims=True)
            flat_high, flat_low = split(flat - average)
            result = average + (
                one(high, flat_high) + (one(high, flat_low) + one(low, flat_high))
            )
            updated[field, :, level] = result.reshape(slab_count, block, width)

    for field in range(2):
        for at in range(0, levels, 8):
            part = given_ref[:, field, at : at + 8]
            part = jnp.swapaxes(part, 0, 1)
            x_ref[field, at // slab_levels : (at + 8) // slab_levels] = part.reshape(
                8 // slab_levels, slab_levels, block, width
            )
    pack(x_ref)
    for cycle in range(cycles):
        weight = live_ref[cycle].astype(jnp.float32) / error_ref[cycle]
        place = level_ref[cycle] * width + column_ref[cycle]
        bundle[cycle, 0:1] = place.astype(jnp.float32)
        bundle[cycle, 1:2] = weight
        bundle[cycle, 2:3] = weight * value_ref[cycle]
    numbers = iota((8, lane_count), 1)
    blend = jnp.where(numbers == first_block, 1.0, 0.0)
    for at in range(count):
        blend = blend + jnp.where(numbers == chosen_ref[0, at], 1.0, 0.0)
    bundle[cycles, :, 0:lane_count] = blend
    spread_rows = jnp.where(
        iota((rows, levels), 0) // block == iota((rows, levels), 1), 1.0, 0.0
    ).astype(jnp.bfloat16)
    same = lax.rem(iota((rows, rows), 0), block) == lax.rem(iota((rows, rows), 1), block)
    for at, part in enumerate(split(coupling_ref[...])):
        tall = one(spread_rows, part).astype(jnp.bfloat16)
        kron[at] = jnp.where(same, one(tall, spread_rows, 1), 0.0).astype(jnp.bfloat16)

    def meet():
        pl.semaphore_wait(barrier, 2 * slab_count - 1 + 4)
        copies = send_halo(0)

        @pl.when(away == 1)
        def _():
            bundle_copy().start()

        @pl.when(away == 0)
        def _():
            notes[...] = bundle[...]

        return copies

    blend_copies = []
    for cycle in range(cycles):
        source = x_ref if cycle == 0 else returned
        if cycle:
            pack(source)
            copies = send_halo(cycle)
            advance(source, cycle, lambda: copies)
        else:
            advance(source, cycle, meet)
        heights_now = (h_ref, heights, send_h.at[cycle], recv_h.at[cycle])
        speeds_now = (u_ref, speeds, send_u.at[cycle], recv_u.at[cycle])
        drains = []
        if cycle == 0:
            inward_relay(1, h_ref)
            inward_send(1, *heights_now)
            inward_relay(0, u_ref)

            @pl.when(away == 1)
            def _():
                bundle_copy().wait()

            @pl.when(away == 0)
            def _():
                heights[slab] = h_ref[slab]
                speeds[slab] = u_ref[slab]

            blends[0] = notes[cycles, 0:8, 0:lane_count]
            for step in range(1, grp_count):
                copy = remote(
                    blends.at[0], blends.at[step], send_b.at[step], recv_b.at[step],
                    {"grp": turned(grp, step, grp_count)},
                )
                copy.start()
                blend_copies.append(copy)
        else:
            drains = cube_send(*heights_now)
            heights[slab] = h_ref[slab]
            speeds[slab] = u_ref[slab]
        sum_cells(cycle)
        if cycle == 0:
            inward_take(heights, recv_h.at[cycle])
        else:
            cube_take(heights, recv_h.at[cycle])
        gram()

        gathers = []
        for step in range(1, mem_count):
            to_line = turned(line, step, mem_count)
            copy = remote(
                own, column.at[step - 1], send_a.at[cycle, step - 1], recv_a.at[cycle, step - 1],
                {"mem": half * depth + lax.rem(to_line, depth), "hor": 2 * pair + to_line // depth},
            )
            copy.start()
            gathers.append(copy)
        if cycle == 0:
            inward_send(0, *speeds_now)
        else:
            drains = drains + cube_send(*speeds_now)
        for copy in blend_copies:
            copy.wait()
        blend_copies = []
        for copy in gathers:
            copy.wait()
        returns = []
        for step in range(1, grp_count):
            partial[step - 1] = blended_for(blends[step])
            copy = remote(
                partial.at[step - 1], arrived.at[step - 1],
                send_c.at[cycle, step - 1], recv_c.at[cycle, step - 1],
                {"grp": turned(grp, grp_count - step, grp_count)},
            )
            copy.start()
            returns.append(copy)
        total = blended_for(blends[0])
        for copy in returns:
            copy.wait()
        for step in range(1, grp_count):
            total = total + arrived[step - 1]
        transposed = root(total)
        last = cycle == cycles - 1
        for field, patch in ((1, heights), (0, speeds)):
            if field == 0:
                if cycle == 0:
                    inward_take(speeds, recv_u.at[cycle])
                else:
                    cube_take(speeds, recv_u.at[cycle])
            update(transposed, patch, field)
            if last:
                outward_send(field)
            else:
                drains = drains + cube_send(
                    updated.at[field], returned.at[field],
                    send_e.at[cycle, field], recv_e.at[cycle, field],
                )
                returned[field, slab] = updated[field, slab]
        if not last:
            for field in (1, 0):
                cube_take(returned.at[field], recv_e.at[cycle, field])
        for copy in drains:
            copy.wait_send()
        if cycle == 0:
            inward_drain(1, *heights_now)
            inward_drain(0, *speeds_now)
    for field in (1, 0):
        outward_finish(field)
        for at in range(0, levels, 8):
            part = final[field, at // slab_levels : (at + 8) // slab_levels]
            part = part.reshape(8, block, width)
            out_ref[:, field, at : at + 8] = jnp.swapaxes(part, 0, 1)


def shards(ensemble, coupling, obs_column, obs_level, obs_value, obs_error, obs_live, partners):
    mem_count = lax.axis_size("mem")
    grp_count = lax.axis_size("grp")
    hor_count = lax.axis_size("hor")
    slab_count = mem_count * grp_count
    lanes = max(LANES, -(-slab_count // LANES) * LANES)
    count = partners.shape[-1]
    block, fields, levels, width = ensemble.shape
    cycles = obs_column.shape[0]
    members = block * slab_count
    slab_levels = levels // slab_count
    state = (slab_count, slab_levels, block, width)
    strip = (slab_count, slab_levels, block, LANES)
    tall = (members // 2 + 8, members)
    rows = levels * block
    groups = 2 * levels * HALO // LANES
    slots = max(obs_column.shape[-1], lanes)
    vmem = pl.BlockSpec(memory_space=pltpu.VMEM)
    dma = pltpu.SemaphoreType.DMA
    f32 = jnp.float32
    return pl.pallas_call(
        functools.partial(program, (mem_count, grp_count, hor_count), count, cycles),
        out_shape=jax.ShapeDtypeStruct(ensemble.shape, f32),
        in_specs=[vmem] * 7 + [pl.BlockSpec(memory_space=pltpu.SMEM)],
        out_specs=vmem,
        scratch_shapes=[
            pltpu.VMEM((2,) + state, f32),
            pltpu.VMEM((2, rows, rows), jnp.bfloat16),
            pltpu.VMEM(state, f32), pltpu.VMEM(state, f32), pltpu.VMEM(state, f32),
            pltpu.VMEM(strip, f32), pltpu.VMEM(strip, f32), pltpu.VMEM(strip, f32),
            pltpu.VMEM((2, groups, block, LANES), f32),
            pltpu.VMEM((cycles, 2, groups, block, LANES), f32),
            pltpu.VMEM(state, f32), pltpu.VMEM(state, f32),
            pltpu.VMEM((2,) + state, f32), pltpu.VMEM((2,) + state, f32),
            pltpu.VMEM((2,) + state, f32),
            pltpu.VMEM((2, slab_count // 2) + state[1:], f32),
            pltpu.VMEM((2, slab_levels * width // LANES, 1, LANES), f32),
            pltpu.VMEM((cycles + 1, 8, slots), f32), pltpu.VMEM((cycles + 1, 8, slots), f32),
            pltpu.VMEM(tall, f32),
            pltpu.VMEM((mem_count - 1,) + tall, f32),
            pltpu.VMEM((grp_count - 1,) + tall, f32),
            pltpu.VMEM((grp_count - 1,) + tall, f32),
            pltpu.VMEM((grp_count, 8, lanes), f32),
            dma((cycles, 2)), dma((cycles, 2)),
            dma((1,)), dma((1,)),
            dma((cycles, mem_count - 1)), dma((cycles, mem_count - 1)),
            dma((grp_count,)), dma((grp_count,)),
            dma((cycles, grp_count - 1)), dma((cycles, grp_count - 1)),
            dma((cycles, slab_count)), dma((cycles, slab_count)),
            dma((cycles, slab_count)), dma((cycles, slab_count)),
            dma((cycles, 2, slab_count)), dma((cycles, 2, slab_count)),
            dma((2, slab_count)), dma((2, slab_count)),
            dma((2, slab_count // 2)), dma((2, slab_count // 2)), dma((2, slab_count // 2)),
        ],
        compiler_params=pltpu.CompilerParams(collective_id=0, has_side_effects=True),
    )(
        ensemble, coupling, obs_column[:, 0], obs_level[:, 0], obs_value[:, 0], obs_error[:, 0],
        obs_live[:, 0], partners[0],
    )


def solution(mesh):
    in_specs = (
        P(("mem", "grp"), None, None, "hor"),
        P(),
        P(None, ("mem", "grp"), "hor", None),
        P(None, ("mem", "grp"), "hor", None),
        P(None, ("mem", "grp"), "hor", None),
        P(None, ("mem", "grp"), "hor", None),
        P(None, ("mem", "grp"), "hor", None),
        P(("mem", "grp"), "hor", None),
    )
    out_specs = P(("mem", "grp"), None, None, "hor")
    return jax.shard_map(shards, mesh=mesh, in_specs=in_specs, out_specs=out_specs, check_vma=False)
```

```python
import functools

import jax
import jax.numpy as jnp
from jax import lax
from jax.experimental import pallas as pl
from jax.experimental.pallas import tpu as pltpu
from jax.sharding import PartitionSpec as P

SUBSTEPS = 4
ROOT_STEPS = 8
MESH = pl.DeviceIdType.MESH
LANES = 128
HALO = 2 * SUBSTEPS
EARLY = 1

time_step = 0.2


def split(value):
    high = value.astype(jnp.bfloat16)
    return high, (value - high.astype(jnp.float32)).astype(jnp.bfloat16)


def split3(value):
    high, rest = value.astype(jnp.bfloat16), None
    rest = value - high.astype(jnp.float32)
    middle = rest.astype(jnp.bfloat16)
    low = (rest - middle.astype(jnp.float32)).astype(jnp.bfloat16)
    return high, middle, low


def one(a, b, across=0):
    dims = (((1,), (across,)), ((), ()))
    return lax.dot_general(a, b, dims, preferred_element_type=jnp.float32)


def product(left, right, across=0):
    left_high, left_low = split(left)
    right_high, right_low = split(right)
    return one(left_high, right_high, across) + (
        one(left_high, right_low, across) + one(left_low, right_high, across)
    )


def iota(shape, axis):
    return lax.broadcasted_iota(jnp.int32, shape, axis)


def program(
    sizes, count, cycles,
    given_hbm, coupling_hbm, column_hbm, level_hbm, value_hbm, error_hbm, live_hbm, chosen_ref,
    out_ref,
    given_ref, coupling_ref, column_ref, level_ref, value_ref, error_ref, live_ref, fetch_sem,
    x_ref, kron, u_ref, h_ref, p_ref, edge_u, edge_h, edge_p, packed, halo,
    heights, speeds, updated, returned, final, relayed, cells, bundle, notes,
    own, column, partial, arrived, blends,
    send_n, recv_n, send_o, recv_o, send_a, recv_a, send_b, recv_b, send_c, recv_c,
    send_h, recv_h, send_u, recv_u, send_e, recv_e, send_f, recv_f,
    send_r, recv_r, send_g,
):
    fetches = []
    for at, (source, target) in enumerate((
        (given_hbm, given_ref), (coupling_hbm, coupling_ref), (column_hbm, column_ref),
        (level_hbm, level_ref), (value_hbm, value_ref), (error_hbm, error_ref),
        (live_hbm, live_ref),
    )):
        copy = pltpu.make_async_copy(source, target, fetch_sem.at[at])
        copy.start()
        fetches.append(copy)
    mem_count, grp_count, hor_count = sizes
    mem = lax.axis_index("mem")
    grp = lax.axis_index("grp")
    hor = lax.axis_index("hor")
    slab_count = mem_count * grp_count
    slab_levels, block, width = x_ref.shape[2:]
    lane_count = blends.shape[2]
    levels = slab_count * slab_levels
    rows = levels * block
    members = slab_count * block

    depth = mem_count // 2
    pairs = hor_count // 2
    pair = hor // 2
    side = lax.rem(hor, 2)
    half = mem // depth
    deep = lax.rem(mem, depth)
    away = half + side - 2 * half * side
    line = side * depth + deep
    slab = line * grp_count + grp
    first_block = mem * grp_count + grp

    def turned(at, step, size):
        return lax.rem(at + step, size)

    def spot(in_half, step_side, step_deep, step_grp):
        to_side = turned(side, step_side, 2)
        to_deep = turned(deep, step_deep, depth)
        to_grp = turned(grp, step_grp, grp_count)
        device = {"mem": in_half * depth + to_deep, "hor": 2 * pair + to_side, "grp": to_grp}
        return device, (to_side * depth + to_deep) * grp_count + to_grp

    steps = [
        (one_side, one_deep, one_grp)
        for one_side in range(2) for one_deep in range(depth) for one_grp in range(grp_count)
    ]
    cube = [spot(half, *step) for step in steps[:0:-1]]
    level_first = [spot(half, *step) for step in steps[1:] if step[1] == 0]
    level_later = [spot(half, *step) for step in steps[1:] if step[1]]
    across = [(at, spot(1 - half, 0, *step[1:])) for at, step in enumerate(steps[: len(steps) // 2])]

    right = ({"hor": turned(hor, 1, hor_count)},
             {"mem": turned(mem, depth, mem_count),
              "hor": 2 * turned(pair, half, pairs) + side})
    left = ({"hor": turned(hor, hor_count - 1, hor_count)},
            {"mem": turned(mem, depth, mem_count),
             "hor": 2 * turned(pair, half + pairs - 1, pairs) + side})

    barrier = pltpu.get_barrier_semaphore()
    for device, _ in cube + [spot(1 - half, *step) for step in steps]:
        pl.semaphore_signal(barrier, inc=1, device_id=device, device_id_type=MESH)
    for device in left + right:
        pl.semaphore_signal(barrier, inc=1, device_id=device, device_id_type=MESH)

    def remote(source, target, send_sem, recv_sem, device):
        return pltpu.make_async_remote_copy(
            src_ref=source, dst_ref=target, send_sem=send_sem, recv_sem=recv_sem,
            device_id=device, device_id_type=MESH,
        )

    def pack(source):
        lane = iota((block, LANES), 1)
        per = LANES // HALO
        for group in range(2 * levels // per):
            low = jnp.zeros((block, LANES), jnp.float32)
            high = jnp.zeros((block, LANES), jnp.float32)
            for at in range(per):
                index = group * per + at
                field, level = index // levels, index % levels
                place = (field, level // slab_levels, level % slab_levels)
                inside = (lane >= at * HALO) & (lane < (at + 1) * HALO)
                first = source[place + (slice(None), slice(0, LANES))]
                last = source[place + (slice(None), slice(width - LANES, width))]
                if at:
                    first = pltpu.roll(first, at * HALO, 1)
                turn = (at * HALO + HALO) % LANES
                if turn:
                    last = pltpu.roll(last, turn, 1)
                low = jnp.where(inside, first, low)
                high = jnp.where(inside, last, high)
            packed[0, group] = low
            packed[1, group] = high

    def send_halo(cycle):
        copies = []
        for at, target in ((0, left[cycle > 0]), (1, right[cycle > 0])):
            copy = remote(
                packed.at[at], halo.at[cycle, at],
                send_n.at[cycle, at], recv_n.at[cycle, at], target,
            )
            copy.start()
            copies.append(copy)
        return copies

    def unpack(source, cycle):
        lane = iota((block, LANES), 1)
        per = LANES // HALO
        for field, target in ((0, edge_u), (1, edge_h)):
            for level in range(levels):
                index = field * levels + level
                group, at = index // per, index % per
                place = (level // slab_levels, level % slab_levels)
                before = halo[cycle, 1, group]
                after = halo[cycle, 0, group]
                if at:
                    before = pltpu.roll(before, LANES - at * HALO, 1)
                turn = (2 * LANES - HALO - at * HALO) % LANES
                if turn:
                    after = pltpu.roll(after, turn, 1)
                first = source[(field,) + place + (slice(None), slice(0, LANES))]
                last = source[(field,) + place + (slice(None), slice(width - LANES, width))]
                mixed = jnp.where(
                    lane < LANES // 2,
                    pltpu.roll(first, HALO, 1), pltpu.roll(last, LANES - HALO, 1),
                )
                mixed = jnp.where(lane < HALO, before, mixed)
                target[place] = jnp.where(lane >= LANES - HALO, after, mixed)

    def rise(field):
        return pltpu.roll(field, field.shape[-1] - 1, 1) - pltpu.roll(field, 1, 1)

    def substep(read_u, read_h, write_u, write_h, press):
        span = press.shape[-1]
        for at in range(span // LANES):
            lanes = slice(at * LANES, (at + 1) * LANES)
            high, low = split(read_h(slice(0, slab_count), lanes).reshape(rows, LANES))
            result = one(kron[0], high) + (one(kron[0], low) + one(kron[1], high))
            press[:, :, :, lanes] = result.reshape(slab_count, slab_levels, block, LANES)
        everything = slice(0, span)

        for at in range(slab_count):
            part = slice(at, at + 1)
            size = (slab_levels * block, span)
            velocity = read_u(part, everything).reshape(size)
            height = read_h(part, everything).reshape(size)
            pressure = press[part].reshape(size)
            moved = velocity - 0.5 * time_step * (velocity * rise(velocity) + rise(pressure))
            risen = height - 0.5 * time_step * rise(moved * height)
            write_u[part] = moved.reshape(1, slab_levels, block, span)
            write_h[part] = risen.reshape(1, slab_levels, block, span)

    def reader(ref):
        return lambda part, lanes: ref[part, :, :, lanes]

    def field_reader(ref, field):
        return lambda part, lanes: ref[field, part, :, :, lanes]

    def advance(source, cycle, greet):
        substep(field_reader(source, 0), field_reader(source, 1), u_ref, h_ref, p_ref)

        def again(step, carry):
            substep(reader(u_ref), reader(h_ref), u_ref, h_ref, p_ref)
            return carry

        def edge(step, carry):
            substep(reader(edge_u), reader(edge_h), edge_u, edge_h, edge_p)
            return carry

        def both(step, carry):
            return edge(step, again(step, carry))

        ahead = SUBSTEPS // 2 if cycle == 0 else 1
        if ahead > 1:
            lax.fori_loop(1, ahead, again, 0)
        copies = greet()
        lax.fori_loop(ahead, SUBSTEPS, again, 0)
        for copy in copies:
            copy.wait()
        unpack(source, cycle)
        lax.fori_loop(0, SUBSTEPS, edge, 0)
        lane = iota((block, LANES), 1)
        for strip, whole in ((edge_h, h_ref), (edge_u, u_ref)):
            for at in range(slab_count):
                for level in range(slab_levels):
                    fresh = strip[at, level]
                    first = whole[at, level, :, 0:LANES]
                    last = whole[at, level, :, width - LANES : width]
                    whole[at, level, :, 0:LANES] = jnp.where(
                        lane < HALO, pltpu.roll(fresh, LANES - HALO, 1), first
                    )
                    whole[at, level, :, width - LANES : width] = jnp.where(
                        lane >= LANES - HALO, pltpu.roll(fresh, HALO, 1), last
                    )

    def arrive(target, recv_sem, other):
        remote(
            target.at[other], target.at[other], recv_sem.at[other], recv_sem.at[other], {"hor": hor}
        ).wait_recv()

    def cube_send(source, target, send_sem, recv_sem, some=slice(None)):
        copies = []
        for device, other in cube[some]:
            copy = remote(
                source.at[other], target.at[slab], send_sem.at[other], recv_sem.at[slab], device
            )
            copy.start()
            copies.append(copy)
        return copies

    def cube_take(target, recv_sem):
        for _, other in cube:
            arrive(target, recv_sem, other)

    def relay_copy(field, source, at, other):
        return remote(
            source.at[other], relayed.at[field, at], send_r.at[field, at], recv_r.at[field, at],
            {"hor": 2 * pair + 1 - side},
        )

    def inward_relay(field, source):
        @pl.when(away == 1)
        def _():
            for at, step in enumerate(steps[: len(steps) // 2]):
                relay_copy(field, source, at, spot(half, 1, *step[1:])[1]).start()

    def inward_copies(spots, source, target, send_sem, recv_sem):
        return [
            remote(
                source.at[other], target.at[first_block],
                send_sem.at[other], recv_sem.at[first_block], device,
            )
            for device, other in spots
        ]

    straight = [there for _, there in across]

    def forward_copy(field, target, recv_sem, at, device):
        return remote(
            relayed.at[field, at], target.at[first_block],
            send_g.at[field, at], recv_sem.at[first_block], device,
        )

    def inward_send(field, source, target, send_sem, recv_sem, early=True, late=True):
        some = slice(0 if early else EARLY, None if late else EARLY)

        @pl.when(away == 1)
        def _():
            for copy in inward_copies(straight[some], source, target, send_sem, recv_sem):
                copy.start()

        @pl.when(away == 0)
        def _():
            if early:
                for copy in inward_copies(level_first, source, target, send_sem, recv_sem):
                    copy.start()
            own_copies = inward_copies(level_later[some], source, target, send_sem, recv_sem)
            for copy, (at, (device, other)) in zip(own_copies, across[some]):
                copy.start()
                relay_copy(field, source, at, other).wait_recv()
                forward_copy(field, target, recv_sem, at, device).start()

    def inward_drain(field, source, target, send_sem, recv_sem):
        @pl.when(away == 1)
        def _():
            for copy in inward_copies(straight, source, target, send_sem, recv_sem):
                copy.wait_send()
            for at, step in enumerate(steps[: len(steps) // 2]):
                relay_copy(field, source, at, spot(half, 1, *step[1:])[1]).wait_send()

        @pl.when(away == 0)
        def _():
            for copy in inward_copies(cube, source, target, send_sem, recv_sem):
                copy.wait_send()
            for at, (device, other) in across:
                forward_copy(field, target, recv_sem, at, device).wait_send()

    def inward_take(target, recv_sem):
        for step_mem in range(mem_count):
            for step_grp in range(grp_count):
                other = turned(mem, step_mem, mem_count) * grp_count + turned(grp, step_grp, grp_count)
                if step_mem + step_grp:
                    arrive(target, recv_sem, other)
                else:
                    @pl.when(away == 1)
                    def _():
                        arrive(target, recv_sem, other)

    def outward_copies(field):
        copies = []
        for step_mem in range(mem_count):
            for step_grp in range(grp_count):
                to_mem = turned(mem, step_mem, mem_count)
                to_grp = turned(grp, step_grp, grp_count)
                other = to_mem * grp_count + to_grp
                copies.append(remote(
                    updated.at[field, other], final.at[field, slab],
                    send_f.at[field, other], recv_f.at[field, slab],
                    {"mem": to_mem, "hor": 2 * pair + half, "grp": to_grp},
                ))
        return copies

    def outward_send(field):
        copies = outward_copies(field)

        @pl.when(away == 1)
        def _():
            copies[0].start()

        for copy in copies[1:]:
            copy.start()

        @pl.when(away == 0)
        def _():
            final[field, slab] = updated[field, slab]

    def outward_finish(field):
        for at in range(slab_count):
            other = turned(slab, at, slab_count)
            if at:
                arrive(final.at[field], recv_f.at[field], other)
            else:
                @pl.when(away == 1)
                def _():
                    arrive(final.at[field], recv_f.at[field], other)
        copies = outward_copies(field)

        @pl.when(away == 1)
        def _():
            copies[0].wait_send()

        for copy in copies[1:]:
            copy.wait_send()

    def bundle_copy():
        return remote(
            bundle, notes, send_o.at[0], recv_o.at[0],
            {"mem": turned(mem, depth, mem_count), "hor": 2 * pair + 1 - side},
        )

    def sum_cells(cycle):
        place = notes[cycle, 0:1].astype(jnp.int32)
        weight = notes[cycle, 1:2]
        pulled = notes[cycle, 2:3]
        parts = split3(weight) + split3(pulled)
        spare = jnp.zeros((16 - len(parts), weight.shape[1]), jnp.bfloat16)
        lhs = jnp.concatenate(parts + (spare,), axis=0)
        total = slab_levels * width

        def chunk(at, carry):
            numbers = iota((LANES, weight.shape[1]), 0) + at * LANES
            hits = jnp.where(numbers == place, 1.0, 0.0).astype(jnp.bfloat16)
            sums = one(lhs, hits, 1)
            cells[0, at] = sums[0:1] + (sums[1:2] + sums[2:3])
            cells[1, at] = sums[3:4] + (sums[4:5] + sums[5:6])
            return carry

        lax.fori_loop(0, total // LANES, chunk, 0)

    def gram():
        per = width // LANES
        total = None
        for level in range(slab_levels):
            flat = heights[:, level].reshape(members, width)
            average = jnp.mean(flat, axis=0, keepdims=True)
            anomalies = flat - average
            weight = jnp.concatenate(
                [cells[0, level * per + at] for at in range(per)], axis=1
            )
            pulled = jnp.concatenate(
                [cells[1, level * per + at] for at in range(per)], axis=1
            )
            pull = pulled - weight * average
            lhs = jnp.concatenate(
                [anomalies * weight, jnp.broadcast_to(pull, (8, width))], axis=0
            )
            here = product(lhs, anomalies, 1)
            total = here if total is None else total + here
        short = members // 2
        row, lane = iota((short, members), 0), iota((short, members), 1)
        upper = total[:short]
        own[:short] = jnp.where(
            lane - short > row, pltpu.roll(upper, short, 1), total[short:members]
        )
        diagonal = jnp.sum(jnp.where(lane == row, upper, 0.0), axis=0, keepdims=True)
        own[short:] = jnp.where(
            iota((8, members), 0) == 0, total[members:], jnp.broadcast_to(diagonal, (8, members))
        )

    def unfold(total):
        short = members // 2
        row, lane = iota((short, members), 0), iota((short, members), 1)
        lower = total[:short]
        turned_over = jnp.transpose(jnp.concatenate([lower, lower], axis=0))
        first, second = turned_over[:short], turned_over[short:]
        inside = jnp.where(lane < row, second, total[short + 1 : short + 2])
        inside = jnp.where(lane > row, pltpu.roll(lower, short, 1), inside)
        top = jnp.where(lane >= short, first, inside)
        bottom = jnp.where(lane - short > row, second, lower)
        return jnp.concatenate([top, bottom], axis=0), total[short : short + 1]

    lanes = iota((1, lane_count), 1)

    def share(row, step):
        place = turned(line, mem_count - step, mem_count) * grp_count + grp
        return jnp.sum(jnp.where(lanes == place, row[0:1], 0.0), axis=1, keepdims=True)

    def blended_for(row):
        total = share(row, 0) * own[...]
        for step in range(1, mem_count):
            total = total + share(row, step) * column[step - 1]
        return total

    def root(total):
        total = total / (count + 1.0)
        square = (members, members)
        identity = (iota(square, 0) == iota(square, 1)).astype(jnp.float32)
        whole, bvector = unfold(total)
        blended = (members - 1.0) * identity + whole
        bvector = jnp.broadcast_to(bvector, (8, members))
        squares = jnp.sum(
            jnp.sum(blended * blended, axis=1, keepdims=True), axis=0, keepdims=True
        )
        frobenius = jnp.sqrt(squares)
        iterate = blended / frobenius
        newton = 1.5 * identity - 0.5 * iterate
        inverse_root = newton
        for step in range(1, ROOT_STEPS):
            iterate = product(newton, iterate)
            newton = 1.5 * identity - 0.5 * product(inverse_root, iterate)
            inverse_root = product(newton, inverse_root)
        spread = inverse_root * (jnp.sqrt(members - 1.0) / jnp.sqrt(frobenius))
        inner = product(bvector, inverse_root)
        mean_weight = product(inner, inverse_root) / frobenius
        return spread + mean_weight[0:1]

    def update(transposed, source, field):
        high, low = split(transposed)
        for level in range(slab_levels):
            flat = source[:, level].reshape(members, width)
            average = jnp.mean(flat, axis=0, keepdims=True)
            flat_high, flat_low = split(flat - average)
            result = average + (
                one(high, flat_high) + (one(high, flat_low) + one(low, flat_high))
            )
            updated[field, :, level] = result.reshape(slab_count, block, width)

    for copy in fetches:
        copy.wait()
    for field in range(2):
        for at in range(0, levels, 8):
            part = given_ref[:, field, at : at + 8]
            part = jnp.swapaxes(part, 0, 1)
            x_ref[field, at // slab_levels : (at + 8) // slab_levels] = part.reshape(
                8 // slab_levels, slab_levels, block, width
            )
    pack(x_ref)
    for cycle in range(cycles):
        weight = live_ref[cycle].astype(jnp.float32) / error_ref[cycle]
        place = level_ref[cycle] * width + column_ref[cycle]
        bundle[cycle, 0:1] = place.astype(jnp.float32)
        bundle[cycle, 1:2] = weight
        bundle[cycle, 2:3] = weight * value_ref[cycle]
    numbers = iota((8, lane_count), 1)
    blend = jnp.where(numbers == first_block, 1.0, 0.0)
    for at in range(count):
        blend = blend + jnp.where(numbers == chosen_ref[0, at], 1.0, 0.0)
    bundle[cycles, :, 0:lane_count] = blend
    spread_rows = jnp.where(
        iota((rows, levels), 0) // block == iota((rows, levels), 1), 1.0, 0.0
    ).astype(jnp.bfloat16)
    same = lax.rem(iota((rows, rows), 0), block) == lax.rem(iota((rows, rows), 1), block)
    for at, part in enumerate(split(coupling_ref[...])):
        tall = one(spread_rows, part).astype(jnp.bfloat16)
        kron[at] = jnp.where(same, one(tall, spread_rows, 1), 0.0).astype(jnp.bfloat16)

    def meet():
        pl.semaphore_wait(barrier, 2 * slab_count - 1 + 4)
        copies = send_halo(0)

        @pl.when(away == 1)
        def _():
            bundle_copy().start()

        @pl.when(away == 0)
        def _():
            notes[...] = bundle[...]

        return copies

    blend_copies = []
    for cycle in range(cycles):
        source = x_ref if cycle == 0 else returned
        if cycle:
            pack(source)
            copies = send_halo(cycle)
            advance(source, cycle, lambda: copies)
        else:
            advance(source, cycle, meet)
        heights_now = (h_ref, heights, send_h.at[cycle], recv_h.at[cycle])
        speeds_now = (u_ref, speeds, send_u.at[cycle], recv_u.at[cycle])
        drains = []
        if cycle == 0:
            inward_relay(1, h_ref)
            inward_send(1, *heights_now)
            inward_relay(0, u_ref)
            inward_send(0, *speeds_now, late=False)

            @pl.when(away == 1)
            def _():
                bundle_copy().wait()

            @pl.when(away == 0)
            def _():
                heights[slab] = h_ref[slab]
                speeds[slab] = u_ref[slab]

            blends[0] = notes[cycles, 0:8, 0:lane_count]
            for step in range(1, grp_count):
                copy = remote(
                    blends.at[0], blends.at[step], send_b.at[step], recv_b.at[step],
                    {"grp": turned(grp, step, grp_count)},
                )
                copy.start()
                blend_copies.append(copy)
        else:
            drains = cube_send(*heights_now) + cube_send(*speeds_now, slice(0, 2 * EARLY))
            heights[slab] = h_ref[slab]
            speeds[slab] = u_ref[slab]
        sum_cells(cycle)
        if cycle == 0:
            inward_take(heights, recv_h.at[cycle])
        else:
            cube_take(heights, recv_h.at[cycle])
        gram()

        gathers = []
        for step in range(1, mem_count):
            to_line = turned(line, step, mem_count)
            copy = remote(
                own, column.at[step - 1], send_a.at[cycle, step - 1], recv_a.at[cycle, step - 1],
                {"mem": half * depth + lax.rem(to_line, depth), "hor": 2 * pair + to_line // depth},
            )
            copy.start()
            gathers.append(copy)
        if cycle == 0:
            inward_send(0, *speeds_now, early=False)
        else:
            drains = drains + cube_send(*speeds_now, slice(2 * EARLY, None))
        for copy in blend_copies:
            copy.wait()
        blend_copies = []
        for copy in gathers:
            copy.wait()
        returns = []
        for step in range(1, grp_count):
            partial[step - 1] = blended_for(blends[step])
            copy = remote(
                partial.at[step - 1], arrived.at[step - 1],
                send_c.at[cycle, step - 1], recv_c.at[cycle, step - 1],
                {"grp": turned(grp, grp_count - step, grp_count)},
            )
            copy.start()
            returns.append(copy)
        total = blended_for(blends[0])
        for copy in returns:
            copy.wait()
        for step in range(1, grp_count):
            total = total + arrived[step - 1]
        transposed = root(total)
        last = cycle == cycles - 1
        for field, patch in ((1, heights), (0, speeds)):
            if field == 0:
                if cycle == 0:
                    inward_take(speeds, recv_u.at[cycle])
                else:
                    cube_take(speeds, recv_u.at[cycle])
            update(transposed, patch, field)
            if last:
                outward_send(field)
            else:
                drains = drains + cube_send(
                    updated.at[field], returned.at[field],
                    send_e.at[cycle, field], recv_e.at[cycle, field],
                )
                returned[field, slab] = updated[field, slab]
        if not last:
            for field in (1, 0):
                cube_take(returned.at[field], recv_e.at[cycle, field])
        for copy in drains:
            copy.wait_send()
        if cycle == 0:
            inward_drain(1, *heights_now)
            inward_drain(0, *speeds_now)
    for field in (1, 0):
        outward_finish(field)
        for at in range(0, levels, 8):
            part = final[field, at // slab_levels : (at + 8) // slab_levels]
            part = part.reshape(8, block, width)
            out_ref[:, field, at : at + 8] = jnp.swapaxes(part, 0, 1)


def shards(ensemble, coupling, obs_column, obs_level, obs_value, obs_error, obs_live, partners):
    mem_count = lax.axis_size("mem")
    grp_count = lax.axis_size("grp")
    hor_count = lax.axis_size("hor")
    slab_count = mem_count * grp_count
    lanes = max(LANES, -(-slab_count // LANES) * LANES)
    count = partners.shape[-1]
    block, fields, levels, width = ensemble.shape
    cycles = obs_column.shape[0]
    members = block * slab_count
    slab_levels = levels // slab_count
    state = (slab_count, slab_levels, block, width)
    strip = (slab_count, slab_levels, block, LANES)
    tall = (members // 2 + 8, members)
    rows = levels * block
    groups = 2 * levels * HALO // LANES
    noted = (cycles, 1, obs_column.shape[-1])
    slots = max(obs_column.shape[-1], lanes)
    vmem = pl.BlockSpec(memory_space=pltpu.VMEM)
    dma = pltpu.SemaphoreType.DMA
    f32 = jnp.float32
    return pl.pallas_call(
        functools.partial(program, (mem_count, grp_count, hor_count), count, cycles),
        out_shape=jax.ShapeDtypeStruct(ensemble.shape, f32),
        in_specs=[pl.BlockSpec(memory_space=pltpu.HBM)] * 7 + [pl.BlockSpec(memory_space=pltpu.SMEM)],
        out_specs=vmem,
        scratch_shapes=[
            pltpu.VMEM(ensemble.shape, f32), pltpu.VMEM(coupling.shape, f32),
            pltpu.VMEM(noted, jnp.int32), pltpu.VMEM(noted, jnp.int32),
            pltpu.VMEM(noted, f32), pltpu.VMEM(noted, f32), pltpu.VMEM(noted, jnp.int32),
            dma((7,)),
            pltpu.VMEM((2,) + state, f32),
            pltpu.VMEM((2, rows, rows), jnp.bfloat16),
            pltpu.VMEM(state, f32), pltpu.VMEM(state, f32), pltpu.VMEM(state, f32),
            pltpu.VMEM(strip, f32), pltpu.VMEM(strip, f32), pltpu.VMEM(strip, f32),
            pltpu.VMEM((2, groups, block, LANES), f32),
            pltpu.VMEM((cycles, 2, groups, block, LANES), f32),
            pltpu.VMEM(state, f32), pltpu.VMEM(state, f32),
            pltpu.VMEM((2,) + state, f32), pltpu.VMEM((2,) + state, f32),
            pltpu.VMEM((2,) + state, f32),
            pltpu.VMEM((2, slab_count // 2) + state[1:], f32),
            pltpu.VMEM((2, slab_levels * width // LANES, 1, LANES), f32),
            pltpu.VMEM((cycles + 1, 8, slots), f32), pltpu.VMEM((cycles + 1, 8, slots), f32),
            pltpu.VMEM(tall, f32),
            pltpu.VMEM((mem_count - 1,) + tall, f32),
            pltpu.VMEM((grp_count - 1,) + tall, f32),
            pltpu.VMEM((grp_count - 1,) + tall, f32),
            pltpu.VMEM((grp_count, 8, lanes), f32),
            dma((cycles, 2)), dma((cycles, 2)),
            dma((1,)), dma((1,)),
            dma((cycles, mem_count - 1)), dma((cycles, mem_count - 1)),
            dma((grp_count,)), dma((grp_count,)),
            dma((cycles, grp_count - 1)), dma((cycles, grp_count - 1)),
            dma((cycles, slab_count)), dma((cycles, slab_count)),
            dma((cycles, slab_count)), dma((cycles, slab_count)),
            dma((cycles, 2, slab_count)), dma((cycles, 2, slab_count)),
            dma((2, slab_count)), dma((2, slab_count)),
            dma((2, slab_count // 2)), dma((2, slab_count // 2)), dma((2, slab_count // 2)),
        ],
        compiler_params=pltpu.CompilerParams(collective_id=0, has_side_effects=True),
    )(
        ensemble, coupling, obs_column[:, 0], obs_level[:, 0], obs_value[:, 0], obs_error[:, 0],
        obs_live[:, 0], partners[0],
    )


def solution(mesh):
    in_specs = (
        P(("mem", "grp"), None, None, "hor"),
        P(),
        P(None, ("mem", "grp"), "hor", None),
        P(None, ("mem", "grp"), "hor", None),
        P(None, ("mem", "grp"), "hor", None),
        P(None, ("mem", "grp"), "hor", None),
        P(None, ("mem", "grp"), "hor", None),
        P(("mem", "grp"), "hor", None),
    )
    out_specs = P(("mem", "grp"), None, None, "hor")
    return jax.shard_map(shards, mesh=mesh, in_specs=in_specs, out_specs=out_specs, check_vma=False)
```

```python
import functools

import jax
import jax.numpy as jnp
from jax import lax
from jax.experimental import pallas as pl
from jax.experimental.pallas import tpu as pltpu
from jax.sharding import PartitionSpec as P

SUBSTEPS = 4
ROOT_STEPS = 8
MESH = pl.DeviceIdType.MESH
LANES = 128
HALO = 2 * SUBSTEPS
EARLY = 1

time_step = 0.2


def split(value):
    high = value.astype(jnp.bfloat16)
    return high, (value - high.astype(jnp.float32)).astype(jnp.bfloat16)


def split3(value):
    high, rest = value.astype(jnp.bfloat16), None
    rest = value - high.astype(jnp.float32)
    middle = rest.astype(jnp.bfloat16)
    low = (rest - middle.astype(jnp.float32)).astype(jnp.bfloat16)
    return high, middle, low


def one(a, b, across=0):
    dims = (((1,), (across,)), ((), ()))
    return lax.dot_general(a, b, dims, preferred_element_type=jnp.float32)


def product(left, right, across=0):
    left_high, left_low = split(left)
    right_high, right_low = split(right)
    return one(left_high, right_high, across) + (
        one(left_high, right_low, across) + one(left_low, right_high, across)
    )


def iota(shape, axis):
    return lax.broadcasted_iota(jnp.int32, shape, axis)


def program(
    sizes, count, cycles,
    given_hbm, coupling_hbm, column_hbm, level_hbm, value_hbm, error_hbm, live_hbm, chosen_ref,
    final_hbm,
    given_ref, coupling_ref, column_ref, level_ref, value_ref, error_ref, live_ref, fetch_sem,
    x_ref, kron, u_ref, h_ref, p_ref, edge_u, edge_h, edge_p, packed, halo,
    heights, speeds, updated, returned, relayed, cells, bundle, notes,
    own, column, partial, arrived, blends,
    send_n, recv_n, send_o, recv_o, send_a, recv_a, send_b, recv_b, send_c, recv_c,
    send_h, recv_h, send_u, recv_u, send_e, recv_e, send_f, recv_f,
    send_r, recv_r, send_g,
):
    fetches = []
    for at, (source, target) in enumerate((
        (given_hbm, given_ref), (coupling_hbm, coupling_ref), (column_hbm, column_ref),
        (level_hbm, level_ref), (value_hbm, value_ref), (error_hbm, error_ref),
        (live_hbm, live_ref),
    )):
        copy = pltpu.make_async_copy(source, target, fetch_sem.at[at])
        copy.start()
        fetches.append(copy)
    mem_count, grp_count, hor_count = sizes
    mem = lax.axis_index("mem")
    grp = lax.axis_index("grp")
    hor = lax.axis_index("hor")
    slab_count = mem_count * grp_count
    slab_levels, block, width = x_ref.shape[2:]
    lane_count = blends.shape[2]
    levels = slab_count * slab_levels
    rows = levels * block
    members = slab_count * block

    depth = mem_count // 2
    pairs = hor_count // 2
    pair = hor // 2
    side = lax.rem(hor, 2)
    half = mem // depth
    deep = lax.rem(mem, depth)
    away = half + side - 2 * half * side
    line = side * depth + deep
    slab = line * grp_count + grp
    first_block = mem * grp_count + grp

    def turned(at, step, size):
        return lax.rem(at + step, size)

    def spot(in_half, step_side, step_deep, step_grp):
        to_side = turned(side, step_side, 2)
        to_deep = turned(deep, step_deep, depth)
        to_grp = turned(grp, step_grp, grp_count)
        device = {"mem": in_half * depth + to_deep, "hor": 2 * pair + to_side, "grp": to_grp}
        return device, (to_side * depth + to_deep) * grp_count + to_grp

    steps = [
        (one_side, one_deep, one_grp)
        for one_side in range(2) for one_deep in range(depth) for one_grp in range(grp_count)
    ]
    cube = [spot(half, *step) for step in steps[:0:-1]]
    level_first = [spot(half, *step) for step in steps[1:] if step[1] == 0]
    level_later = [spot(half, *step) for step in steps[1:] if step[1]]
    across = [(at, spot(1 - half, 0, *step[1:])) for at, step in enumerate(steps[: len(steps) // 2])]

    right = ({"hor": turned(hor, 1, hor_count)},
             {"mem": turned(mem, depth, mem_count),
              "hor": 2 * turned(pair, half, pairs) + side})
    left = ({"hor": turned(hor, hor_count - 1, hor_count)},
            {"mem": turned(mem, depth, mem_count),
             "hor": 2 * turned(pair, half + pairs - 1, pairs) + side})

    barrier = pltpu.get_barrier_semaphore()
    for device, _ in cube + [spot(1 - half, *step) for step in steps]:
        pl.semaphore_signal(barrier, inc=1, device_id=device, device_id_type=MESH)
    for device in left + right:
        pl.semaphore_signal(barrier, inc=1, device_id=device, device_id_type=MESH)

    def remote(source, target, send_sem, recv_sem, device):
        return pltpu.make_async_remote_copy(
            src_ref=source, dst_ref=target, send_sem=send_sem, recv_sem=recv_sem,
            device_id=device, device_id_type=MESH,
        )

    def pack(source):
        lane = iota((block, LANES), 1)
        per = LANES // HALO
        for group in range(2 * levels // per):
            low = jnp.zeros((block, LANES), jnp.float32)
            high = jnp.zeros((block, LANES), jnp.float32)
            for at in range(per):
                index = group * per + at
                field, level = index // levels, index % levels
                place = (field, level // slab_levels, level % slab_levels)
                inside = (lane >= at * HALO) & (lane < (at + 1) * HALO)
                first = source[place + (slice(None), slice(0, LANES))]
                last = source[place + (slice(None), slice(width - LANES, width))]
                if at:
                    first = pltpu.roll(first, at * HALO, 1)
                turn = (at * HALO + HALO) % LANES
                if turn:
                    last = pltpu.roll(last, turn, 1)
                low = jnp.where(inside, first, low)
                high = jnp.where(inside, last, high)
            packed[0, group] = low
            packed[1, group] = high

    def send_halo(cycle):
        copies = []
        for at, target in ((0, left[cycle > 0]), (1, right[cycle > 0])):
            copy = remote(
                packed.at[at], halo.at[cycle, at],
                send_n.at[cycle, at], recv_n.at[cycle, at], target,
            )
            copy.start()
            copies.append(copy)
        return copies

    def unpack(source, cycle):
        lane = iota((block, LANES), 1)
        per = LANES // HALO
        for field, target in ((0, edge_u), (1, edge_h)):
            for level in range(levels):
                index = field * levels + level
                group, at = index // per, index % per
                place = (level // slab_levels, level % slab_levels)
                before = halo[cycle, 1, group]
                after = halo[cycle, 0, group]
                if at:
                    before = pltpu.roll(before, LANES - at * HALO, 1)
                turn = (2 * LANES - HALO - at * HALO) % LANES
                if turn:
                    after = pltpu.roll(after, turn, 1)
                first = source[(field,) + place + (slice(None), slice(0, LANES))]
                last = source[(field,) + place + (slice(None), slice(width - LANES, width))]
                mixed = jnp.where(
                    lane < LANES // 2,
                    pltpu.roll(first, HALO, 1), pltpu.roll(last, LANES - HALO, 1),
                )
                mixed = jnp.where(lane < HALO, before, mixed)
                target[place] = jnp.where(lane >= LANES - HALO, after, mixed)

    def rise(field):
        return pltpu.roll(field, field.shape[-1] - 1, 1) - pltpu.roll(field, 1, 1)

    def substep(read_u, read_h, write_u, write_h, press):
        span = press.shape[-1]
        for at in range(span // LANES):
            lanes = slice(at * LANES, (at + 1) * LANES)
            high, low = split(read_h(slice(0, slab_count), lanes).reshape(rows, LANES))
            result = one(kron[0], high) + (one(kron[0], low) + one(kron[1], high))
            press[:, :, :, lanes] = result.reshape(slab_count, slab_levels, block, LANES)
        everything = slice(0, span)

        for at in range(slab_count):
            part = slice(at, at + 1)
            size = (slab_levels * block, span)
            velocity = read_u(part, everything).reshape(size)
            height = read_h(part, everything).reshape(size)
            pressure = press[part].reshape(size)
            moved = velocity - 0.5 * time_step * (velocity * rise(velocity) + rise(pressure))
            risen = height - 0.5 * time_step * rise(moved * height)
            write_u[part] = moved.reshape(1, slab_levels, block, span)
            write_h[part] = risen.reshape(1, slab_levels, block, span)

    def reader(ref):
        return lambda part, lanes: ref[part, :, :, lanes]

    def field_reader(ref, field):
        return lambda part, lanes: ref[field, part, :, :, lanes]

    def advance(source, cycle, greet):
        substep(field_reader(source, 0), field_reader(source, 1), u_ref, h_ref, p_ref)

        def again(step, carry):
            substep(reader(u_ref), reader(h_ref), u_ref, h_ref, p_ref)
            return carry

        def edge(step, carry):
            substep(reader(edge_u), reader(edge_h), edge_u, edge_h, edge_p)
            return carry

        def both(step, carry):
            return edge(step, again(step, carry))

        ahead = SUBSTEPS // 2 if cycle == 0 else 1
        if ahead > 1:
            lax.fori_loop(1, ahead, again, 0)
        copies = greet()
        lax.fori_loop(ahead, SUBSTEPS, again, 0)
        for copy in copies:
            copy.wait()
        unpack(source, cycle)
        lax.fori_loop(0, SUBSTEPS, edge, 0)
        lane = iota((block, LANES), 1)
        for strip, whole in ((edge_h, h_ref), (edge_u, u_ref)):
            for at in range(slab_count):
                for level in range(slab_levels):
                    fresh = strip[at, level]
                    first = whole[at, level, :, 0:LANES]
                    last = whole[at, level, :, width - LANES : width]
                    whole[at, level, :, 0:LANES] = jnp.where(
                        lane < HALO, pltpu.roll(fresh, LANES - HALO, 1), first
                    )
                    whole[at, level, :, width - LANES : width] = jnp.where(
                        lane >= LANES - HALO, pltpu.roll(fresh, HALO, 1), last
                    )

    def arrive(target, recv_sem, other):
        remote(
            target.at[other], target.at[other], recv_sem.at[other], recv_sem.at[other], {"hor": hor}
        ).wait_recv()

    def cube_send(source, target, send_sem, recv_sem, some=slice(None)):
        copies = []
        for device, other in cube[some]:
            copy = remote(
                source.at[other], target.at[slab], send_sem.at[other], recv_sem.at[slab], device
            )
            copy.start()
            copies.append(copy)
        return copies

    def cube_take(target, recv_sem):
        for _, other in cube:
            arrive(target, recv_sem, other)

    def relay_copy(field, source, at, other):
        return remote(
            source.at[other], relayed.at[field, at], send_r.at[field, at], recv_r.at[field, at],
            {"hor": 2 * pair + 1 - side},
        )

    def inward_relay(field, source):
        @pl.when(away == 1)
        def _():
            for at, step in enumerate(steps[: len(steps) // 2]):
                relay_copy(field, source, at, spot(half, 1, *step[1:])[1]).start()

    def inward_copies(spots, source, target, send_sem, recv_sem):
        return [
            remote(
                source.at[other], target.at[first_block],
                send_sem.at[other], recv_sem.at[first_block], device,
            )
            for device, other in spots
        ]

    straight = [there for _, there in across]

    def forward_copy(field, target, recv_sem, at, device):
        return remote(
            relayed.at[field, at], target.at[first_block],
            send_g.at[field, at], recv_sem.at[first_block], device,
        )

    def inward_send(field, source, target, send_sem, recv_sem, early=True, late=True):
        some = slice(0 if early else EARLY, None if late else EARLY)

        @pl.when(away == 1)
        def _():
            for copy in inward_copies(straight[some], source, target, send_sem, recv_sem):
                copy.start()

        @pl.when(away == 0)
        def _():
            if early:
                for copy in inward_copies(level_first, source, target, send_sem, recv_sem):
                    copy.start()
            own_copies = inward_copies(level_later[some], source, target, send_sem, recv_sem)
            for copy, (at, (device, other)) in zip(own_copies, across[some]):
                copy.start()
                relay_copy(field, source, at, other).wait_recv()
                forward_copy(field, target, recv_sem, at, device).start()

    def inward_drain(field, source, target, send_sem, recv_sem):
        @pl.when(away == 1)
        def _():
            for copy in inward_copies(straight, source, target, send_sem, recv_sem):
                copy.wait_send()
            for at, step in enumerate(steps[: len(steps) // 2]):
                relay_copy(field, source, at, spot(half, 1, *step[1:])[1]).wait_send()

        @pl.when(away == 0)
        def _():
            for copy in inward_copies(cube, source, target, send_sem, recv_sem):
                copy.wait_send()
            for at, (device, other) in across:
                forward_copy(field, target, recv_sem, at, device).wait_send()

    def inward_take(target, recv_sem):
        for step_mem in range(mem_count):
            for step_grp in range(grp_count):
                other = turned(mem, step_mem, mem_count) * grp_count + turned(grp, step_grp, grp_count)
                if step_mem + step_grp:
                    arrive(target, recv_sem, other)
                else:
                    @pl.when(away == 1)
                    def _():
                        arrive(target, recv_sem, other)

    def outward_copies(field):
        copies = []
        for step_mem in range(mem_count):
            for step_grp in range(grp_count):
                to_mem = turned(mem, step_mem, mem_count)
                to_grp = turned(grp, step_grp, grp_count)
                other = to_mem * grp_count + to_grp
                copies.append(remote(
                    updated.at[field, other], final_hbm.at[field, slab],
                    send_f.at[field, other], recv_f.at[field, slab],
                    {"mem": to_mem, "hor": 2 * pair + half, "grp": to_grp},
                ))
        return copies

    def keep_copy(field):
        return pltpu.make_async_copy(
            updated.at[field, slab], final_hbm.at[field, slab], send_f.at[field, slab]
        )

    def outward_send(field):
        copies = outward_copies(field)

        @pl.when(away == 1)
        def _():
            copies[0].start()

        for copy in copies[1:]:
            copy.start()

        @pl.when(away == 0)
        def _():
            keep_copy(field).start()

    def outward_finish(field):
        for at in range(slab_count):
            other = turned(slab, at, slab_count)
            if at:
                arrive(final_hbm.at[field], recv_f.at[field], other)
            else:
                @pl.when(away == 1)
                def _():
                    arrive(final_hbm.at[field], recv_f.at[field], other)
        copies = outward_copies(field)

        @pl.when(away == 1)
        def _():
            copies[0].wait_send()

        @pl.when(away == 0)
        def _():
            keep_copy(field).wait()

        for copy in copies[1:]:
            copy.wait_send()

    def bundle_copy():
        return remote(
            bundle, notes, send_o.at[0], recv_o.at[0],
            {"mem": turned(mem, depth, mem_count), "hor": 2 * pair + 1 - side},
        )

    def sum_cells(cycle):
        place = notes[cycle, 0:1].astype(jnp.int32)
        weight = notes[cycle, 1:2]
        pulled = notes[cycle, 2:3]
        parts = split3(weight) + split3(pulled)
        spare = jnp.zeros((16 - len(parts), weight.shape[1]), jnp.bfloat16)
        lhs = jnp.concatenate(parts + (spare,), axis=0)
        total = slab_levels * width

        def chunk(at, carry):
            numbers = iota((LANES, weight.shape[1]), 0) + at * LANES
            hits = jnp.where(numbers == place, 1.0, 0.0).astype(jnp.bfloat16)
            sums = one(lhs, hits, 1)
            cells[0, at] = sums[0:1] + (sums[1:2] + sums[2:3])
            cells[1, at] = sums[3:4] + (sums[4:5] + sums[5:6])
            return carry

        lax.fori_loop(0, total // LANES, chunk, 0)

    def gram():
        per = width // LANES
        total = None
        for level in range(slab_levels):
            flat = heights[:, level].reshape(members, width)
            average = jnp.mean(flat, axis=0, keepdims=True)
            anomalies = flat - average
            weight = jnp.concatenate(
                [cells[0, level * per + at] for at in range(per)], axis=1
            )
            pulled = jnp.concatenate(
                [cells[1, level * per + at] for at in range(per)], axis=1
            )
            pull = pulled - weight * average
            lhs = jnp.concatenate(
                [anomalies * weight, jnp.broadcast_to(pull, (8, width))], axis=0
            )
            here = product(lhs, anomalies, 1)
            total = here if total is None else total + here
        short = members // 2
        row, lane = iota((short, members), 0), iota((short, members), 1)
        upper = total[:short]
        own[:short] = jnp.where(
            lane - short > row, pltpu.roll(upper, short, 1), total[short:members]
        )
        diagonal = jnp.sum(jnp.where(lane == row, upper, 0.0), axis=0, keepdims=True)
        own[short:] = jnp.where(
            iota((8, members), 0) == 0, total[members:], jnp.broadcast_to(diagonal, (8, members))
        )

    def unfold(total):
        short = members // 2
        row, lane = iota((short, members), 0), iota((short, members), 1)
        lower = total[:short]
        turned_over = jnp.transpose(jnp.concatenate([lower, lower], axis=0))
        first, second = turned_over[:short], turned_over[short:]
        inside = jnp.where(lane < row, second, total[short + 1 : short + 2])
        inside = jnp.where(lane > row, pltpu.roll(lower, short, 1), inside)
        top = jnp.where(lane >= short, first, inside)
        bottom = jnp.where(lane - short > row, second, lower)
        return jnp.concatenate([top, bottom], axis=0), total[short : short + 1]

    lanes = iota((1, lane_count), 1)

    def share(row, step):
        place = turned(line, mem_count - step, mem_count) * grp_count + grp
        return jnp.sum(jnp.where(lanes == place, row[0:1], 0.0), axis=1, keepdims=True)

    def blended_for(row):
        total = share(row, 0) * own[...]
        for step in range(1, mem_count):
            total = total + share(row, step) * column[step - 1]
        return total

    def root(total):
        total = total / (count + 1.0)
        square = (members, members)
        identity = (iota(square, 0) == iota(square, 1)).astype(jnp.float32)
        whole, bvector = unfold(total)
        blended = (members - 1.0) * identity + whole
        bvector = jnp.broadcast_to(bvector, (8, members))
        squares = jnp.sum(
            jnp.sum(blended * blended, axis=1, keepdims=True), axis=0, keepdims=True
        )
        frobenius = jnp.sqrt(squares)
        iterate = blended / frobenius
        newton = 1.5 * identity - 0.5 * iterate
        inverse_root = newton
        for step in range(1, ROOT_STEPS):
            iterate = product(newton, iterate)
            newton = 1.5 * identity - 0.5 * product(inverse_root, iterate)
            if step == ROOT_STEPS - 1:
                inner = product(product(bvector, newton), inverse_root)
            inverse_root = product(newton, inverse_root)
        spread = inverse_root * (jnp.sqrt(members - 1.0) / jnp.sqrt(frobenius))
        mean_weight = product(inner, inverse_root) / frobenius
        return spread + mean_weight[0:1]

    def update(transposed, source, field):
        high, low = split(transposed)
        for level in range(slab_levels):
            flat = source[:, level].reshape(members, width)
            average = jnp.mean(flat, axis=0, keepdims=True)
            flat_high, flat_low = split(flat - average)
            result = average + (
                one(high, flat_high) + (one(high, flat_low) + one(low, flat_high))
            )
            updated[field, :, level] = result.reshape(slab_count, block, width)

    for copy in fetches[1:]:
        copy.wait()
    for cycle in range(cycles):
        weight = live_ref[cycle].astype(jnp.float32) / error_ref[cycle]
        place = level_ref[cycle] * width + column_ref[cycle]
        bundle[cycle, 0:1] = place.astype(jnp.float32)
        bundle[cycle, 1:2] = weight
        bundle[cycle, 2:3] = weight * value_ref[cycle]
    numbers = iota((8, lane_count), 1)
    blend = jnp.where(numbers == first_block, 1.0, 0.0)
    for at in range(count):
        blend = blend + jnp.where(numbers == chosen_ref[0, at], 1.0, 0.0)
    bundle[cycles, :, 0:lane_count] = blend
    spread_rows = jnp.where(
        iota((rows, levels), 0) // block == iota((rows, levels), 1), 1.0, 0.0
    ).astype(jnp.bfloat16)
    same = lax.rem(iota((rows, rows), 0), block) == lax.rem(iota((rows, rows), 1), block)
    for at, part in enumerate(split(coupling_ref[...])):
        tall = one(spread_rows, part).astype(jnp.bfloat16)
        kron[at] = jnp.where(same, one(tall, spread_rows, 1), 0.0).astype(jnp.bfloat16)
    fetches[0].wait()
    for field in range(2):
        for at in range(0, levels, 8):
            part = given_ref[:, field, at : at + 8]
            part = jnp.swapaxes(part, 0, 1)
            x_ref[field, at // slab_levels : (at + 8) // slab_levels] = part.reshape(
                8 // slab_levels, slab_levels, block, width
            )
    pack(x_ref)

    def meet():
        pl.semaphore_wait(barrier, 2 * slab_count - 1 + 4)
        copies = send_halo(0)

        @pl.when(away == 1)
        def _():
            bundle_copy().start()

        @pl.when(away == 0)
        def _():
            notes[...] = bundle[...]

        return copies

    blend_copies = []
    for cycle in range(cycles):
        source = x_ref if cycle == 0 else returned
        if cycle:
            pack(source)
            copies = send_halo(cycle)
            advance(source, cycle, lambda: copies)
        else:
            advance(source, cycle, meet)
        heights_now = (h_ref, heights, send_h.at[cycle], recv_h.at[cycle])
        speeds_now = (u_ref, speeds, send_u.at[cycle], recv_u.at[cycle])
        drains = []
        if cycle == 0:
            inward_relay(1, h_ref)
            inward_send(1, *heights_now)
            inward_relay(0, u_ref)
            inward_send(0, *speeds_now, late=False)

            @pl.when(away == 1)
            def _():
                bundle_copy().wait()

            @pl.when(away == 0)
            def _():
                heights[slab] = h_ref[slab]
                speeds[slab] = u_ref[slab]

            blends[0] = notes[cycles, 0:8, 0:lane_count]
            for step in range(1, grp_count):
                copy = remote(
                    blends.at[0], blends.at[step], send_b.at[step], recv_b.at[step],
                    {"grp": turned(grp, step, grp_count)},
                )
                copy.start()
                blend_copies.append(copy)
        else:
            drains = cube_send(*heights_now) + cube_send(*speeds_now, slice(0, 2 * EARLY))
            heights[slab] = h_ref[slab]
            speeds[slab] = u_ref[slab]
        sum_cells(cycle)
        if cycle == 0:
            inward_take(heights, recv_h.at[cycle])
        else:
            cube_take(heights, recv_h.at[cycle])
        gram()

        gathers = []
        for step in range(1, mem_count):
            to_line = turned(line, step, mem_count)
            copy = remote(
                own, column.at[step - 1], send_a.at[cycle, step - 1], recv_a.at[cycle, step - 1],
                {"mem": half * depth + lax.rem(to_line, depth), "hor": 2 * pair + to_line // depth},
            )
            copy.start()
            gathers.append(copy)
        if cycle == 0:
            inward_send(0, *speeds_now, early=False)
        else:
            drains = drains + cube_send(*speeds_now, slice(2 * EARLY, None))
        for copy in blend_copies:
            copy.wait()
        blend_copies = []
        for copy in gathers:
            copy.wait()
        returns = []
        for step in range(1, grp_count):
            partial[step - 1] = blended_for(blends[step])
            copy = remote(
                partial.at[step - 1], arrived.at[step - 1],
                send_c.at[cycle, step - 1], recv_c.at[cycle, step - 1],
                {"grp": turned(grp, grp_count - step, grp_count)},
            )
            copy.start()
            returns.append(copy)
        total = blended_for(blends[0])
        for copy in returns:
            copy.wait()
        for step in range(1, grp_count):
            total = total + arrived[step - 1]
        transposed = root(total)
        last = cycle == cycles - 1
        for field, patch in ((1, heights), (0, speeds)):
            if field == 0:
                if cycle == 0:
                    inward_take(speeds, recv_u.at[cycle])
                else:
                    cube_take(speeds, recv_u.at[cycle])
            update(transposed, patch, field)
            if last:
                outward_send(field)
            else:
                drains = drains + cube_send(
                    updated.at[field], returned.at[field],
                    send_e.at[cycle, field], recv_e.at[cycle, field],
                )
                returned[field, slab] = updated[field, slab]
        if not last:
            for field in (1, 0):
                cube_take(returned.at[field], recv_e.at[cycle, field])
        for copy in drains:
            copy.wait_send()
        if cycle == 0:
            inward_drain(1, *heights_now)
            inward_drain(0, *speeds_now)
    for field in (1, 0):
        outward_finish(field)


def turn(state_hbm, out_hbm, given, turned, read_sem, write_sem):
    fields, slab_count, slab_levels, block, width = given.shape
    per = 8 // slab_levels
    parts = [(field, at) for field in (1, 0) for at in range(0, slab_count, per)]
    reads, writes = [], []
    for number, (field, at) in enumerate(parts):
        copy = pltpu.make_async_copy(
            state_hbm.at[field, at : at + per], given.at[field, at : at + per],
            read_sem.at[number],
        )
        copy.start()
        reads.append(copy)
    for number, (field, at) in enumerate(parts):
        reads[number].wait()
        levels = slice(at * slab_levels, (at + per) * slab_levels)
        part = given[field, at : at + per].reshape(8, block, width)
        turned[:, field, levels] = jnp.swapaxes(part, 0, 1)
        copy = pltpu.make_async_copy(
            turned.at[:, field, levels], out_hbm.at[:, field, levels], write_sem.at[number]
        )
        copy.start()
        writes.append(copy)
    for copy in writes:
        copy.wait()


def shards(ensemble, coupling, obs_column, obs_level, obs_value, obs_error, obs_live, partners):
    mem_count = lax.axis_size("mem")
    grp_count = lax.axis_size("grp")
    hor_count = lax.axis_size("hor")
    slab_count = mem_count * grp_count
    lanes = max(LANES, -(-slab_count // LANES) * LANES)
    count = partners.shape[-1]
    block, fields, levels, width = ensemble.shape
    cycles = obs_column.shape[0]
    members = block * slab_count
    slab_levels = levels // slab_count
    state = (slab_count, slab_levels, block, width)
    strip = (slab_count, slab_levels, block, LANES)
    tall = (members // 2 + 8, members)
    rows = levels * block
    groups = 2 * levels * HALO // LANES
    noted = (cycles, 1, obs_column.shape[-1])
    slots = max(obs_column.shape[-1], lanes)
    vmem = pl.BlockSpec(memory_space=pltpu.VMEM)
    dma = pltpu.SemaphoreType.DMA
    f32 = jnp.float32
    result = pl.pallas_call(
        functools.partial(program, (mem_count, grp_count, hor_count), count, cycles),
        out_shape=jax.ShapeDtypeStruct((2,) + state, f32),
        in_specs=[pl.BlockSpec(memory_space=pltpu.HBM)] * 7 + [pl.BlockSpec(memory_space=pltpu.SMEM)],
        out_specs=pl.BlockSpec(memory_space=pl.ANY),
        scratch_shapes=[
            pltpu.VMEM(ensemble.shape, f32), pltpu.VMEM(coupling.shape, f32),
            pltpu.VMEM(noted, jnp.int32), pltpu.VMEM(noted, jnp.int32),
            pltpu.VMEM(noted, f32), pltpu.VMEM(noted, f32), pltpu.VMEM(noted, jnp.int32),
            dma((7,)),
            pltpu.VMEM((2,) + state, f32),
            pltpu.VMEM((2, rows, rows), jnp.bfloat16),
            pltpu.VMEM(state, f32), pltpu.VMEM(state, f32), pltpu.VMEM(state, f32),
            pltpu.VMEM(strip, f32), pltpu.VMEM(strip, f32), pltpu.VMEM(strip, f32),
            pltpu.VMEM((2, groups, block, LANES), f32),
            pltpu.VMEM((cycles, 2, groups, block, LANES), f32),
            pltpu.VMEM(state, f32), pltpu.VMEM(state, f32),
            pltpu.VMEM((2,) + state, f32), pltpu.VMEM((2,) + state, f32),
            pltpu.VMEM((2, slab_count // 2) + state[1:], f32),
            pltpu.VMEM((2, slab_levels * width // LANES, 1, LANES), f32),
            pltpu.VMEM((cycles + 1, 8, slots), f32), pltpu.VMEM((cycles + 1, 8, slots), f32),
            pltpu.VMEM(tall, f32),
            pltpu.VMEM((mem_count - 1,) + tall, f32),
            pltpu.VMEM((grp_count - 1,) + tall, f32),
            pltpu.VMEM((grp_count - 1,) + tall, f32),
            pltpu.VMEM((grp_count, 8, lanes), f32),
            dma((cycles, 2)), dma((cycles, 2)),
            dma((1,)), dma((1,)),
            dma((cycles, mem_count - 1)), dma((cycles, mem_count - 1)),
            dma((grp_count,)), dma((grp_count,)),
            dma((cycles, grp_count - 1)), dma((cycles, grp_count - 1)),
            dma((cycles, slab_count)), dma((cycles, slab_count)),
            dma((cycles, slab_count)), dma((cycles, slab_count)),
            dma((cycles, 2, slab_count)), dma((cycles, 2, slab_count)),
            dma((2, slab_count)), dma((2, slab_count)),
            dma((2, slab_count // 2)), dma((2, slab_count // 2)), dma((2, slab_count // 2)),
        ],
        compiler_params=pltpu.CompilerParams(collective_id=0, has_side_effects=True),
    )(
        ensemble, coupling, obs_column[:, 0], obs_level[:, 0], obs_value[:, 0], obs_error[:, 0],
        obs_live[:, 0], partners[0],
    )
    anywhere = pl.BlockSpec(memory_space=pl.ANY)
    parts = 2 * levels // 8
    return pl.pallas_call(
        turn,
        out_shape=jax.ShapeDtypeStruct(ensemble.shape, f32),
        in_specs=[anywhere], out_specs=anywhere,
        scratch_shapes=[
            pltpu.VMEM((2,) + state, f32), pltpu.VMEM(ensemble.shape, f32),
            dma((parts,)), dma((parts,)),
        ],
    )(result)


def solution(mesh):
    in_specs = (
        P(("mem", "grp"), None, None, "hor"),
        P(),
        P(None, ("mem", "grp"), "hor", None),
        P(None, ("mem", "grp"), "hor", None),
        P(None, ("mem", "grp"), "hor", None),
        P(None, ("mem", "grp"), "hor", None),
        P(None, ("mem", "grp"), "hor", None),
        P(("mem", "grp"), "hor", None),
    )
    out_specs = P(("mem", "grp"), None, None, "hor")
    return jax.shard_map(shards, mesh=mesh, in_specs=in_specs, out_specs=out_specs, check_vma=False)
```

```python
import functools

import jax
import jax.numpy as jnp
from jax import lax
from jax.experimental import pallas as pl
from jax.experimental.pallas import tpu as pltpu
from jax.sharding import PartitionSpec as P

SUBSTEPS = 4
ROOT_STEPS = 8
MESH = pl.DeviceIdType.MESH
LANES = 128
HALO = 2 * SUBSTEPS
EARLY = 1

time_step = 0.2


def split(value):
    high = value.astype(jnp.bfloat16)
    return high, (value - high.astype(jnp.float32)).astype(jnp.bfloat16)


def split3(value):
    high, rest = value.astype(jnp.bfloat16), None
    rest = value - high.astype(jnp.float32)
    middle = rest.astype(jnp.bfloat16)
    low = (rest - middle.astype(jnp.float32)).astype(jnp.bfloat16)
    return high, middle, low


def one(a, b, across=0):
    dims = (((1,), (across,)), ((), ()))
    return lax.dot_general(a, b, dims, preferred_element_type=jnp.float32)


def product(left, right, across=0):
    left_high, left_low = split(left)
    right_high, right_low = split(right)
    return one(left_high, right_high, across) + (
        one(left_high, right_low, across) + one(left_low, right_high, across)
    )


def iota(shape, axis):
    return lax.broadcasted_iota(jnp.int32, shape, axis)


def program(
    sizes, count, cycles,
    given_hbm, coupling_hbm, column_hbm, level_hbm, value_hbm, error_hbm, live_hbm, chosen_ref,
    final_hbm,
    given_ref, coupling_ref, column_ref, level_ref, value_ref, error_ref, live_ref, fetch_sem,
    x_ref, kron, u_ref, h_ref, p_ref, edge_u, edge_h, edge_p, packed, halo,
    heights, speeds, updated, returned, relayed, cells, bundle, notes,
    own, column, partial, arrived, blends,
    send_n, recv_n, send_o, recv_o, send_a, recv_a, send_b, recv_b, send_c, recv_c,
    send_h, recv_h, send_u, recv_u, send_e, recv_e, send_f, recv_f,
    send_r, recv_r, send_g,
):
    fetches = []
    for at, (source, target) in enumerate((
        (given_hbm, given_ref), (coupling_hbm, coupling_ref), (column_hbm, column_ref),
        (level_hbm, level_ref), (value_hbm, value_ref), (error_hbm, error_ref),
        (live_hbm, live_ref),
    )):
        copy = pltpu.make_async_copy(source, target, fetch_sem.at[at])
        copy.start()
        fetches.append(copy)
    mem_count, grp_count, hor_count = sizes
    mem = lax.axis_index("mem")
    grp = lax.axis_index("grp")
    hor = lax.axis_index("hor")
    slab_count = mem_count * grp_count
    slab_levels, block, width = x_ref.shape[2:]
    lane_count = blends.shape[2]
    levels = slab_count * slab_levels
    rows = levels * block
    members = slab_count * block

    depth = mem_count // 2
    pairs = hor_count // 2
    pair = hor // 2
    side = lax.rem(hor, 2)
    half = mem // depth
    deep = lax.rem(mem, depth)
    away = half + side - 2 * half * side
    line = side * depth + deep
    slab = line * grp_count + grp
    first_block = mem * grp_count + grp

    def turned(at, step, size):
        return lax.rem(at + step, size)

    def spot(in_half, step_side, step_deep, step_grp):
        to_side = turned(side, step_side, 2)
        to_deep = turned(deep, step_deep, depth)
        to_grp = turned(grp, step_grp, grp_count)
        device = {"mem": in_half * depth + to_deep, "hor": 2 * pair + to_side, "grp": to_grp}
        return device, (to_side * depth + to_deep) * grp_count + to_grp

    steps = [
        (one_side, one_deep, one_grp)
        for one_side in range(2) for one_deep in range(depth) for one_grp in range(grp_count)
    ]
    cube = [spot(half, *step) for step in steps[:0:-1]]
    level_first = [spot(half, *step) for step in steps[1:] if step[1] == 0]
    level_later = [spot(half, *step) for step in steps[1:] if step[1]]
    across = [(at, spot(1 - half, 0, *step[1:])) for at, step in enumerate(steps[: len(steps) // 2])]

    right = ({"hor": turned(hor, 1, hor_count)},
             {"mem": turned(mem, depth, mem_count),
              "hor": 2 * turned(pair, half, pairs) + side})
    left = ({"hor": turned(hor, hor_count - 1, hor_count)},
            {"mem": turned(mem, depth, mem_count),
             "hor": 2 * turned(pair, half + pairs - 1, pairs) + side})

    barrier = pltpu.get_barrier_semaphore()
    for device, _ in cube + [spot(1 - half, *step) for step in steps]:
        pl.semaphore_signal(barrier, inc=1, device_id=device, device_id_type=MESH)
    for device in left + right:
        pl.semaphore_signal(barrier, inc=1, device_id=device, device_id_type=MESH)

    def remote(source, target, send_sem, recv_sem, device):
        return pltpu.make_async_remote_copy(
            src_ref=source, dst_ref=target, send_sem=send_sem, recv_sem=recv_sem,
            device_id=device, device_id_type=MESH,
        )

    def pack(source):
        lane = iota((block, LANES), 1)
        per = LANES // HALO
        for group in range(2 * levels // per):
            low = jnp.zeros((block, LANES), jnp.float32)
            high = jnp.zeros((block, LANES), jnp.float32)
            for at in range(per):
                index = group * per + at
                field, level = index // levels, index % levels
                place = (field, level // slab_levels, level % slab_levels)
                inside = (lane >= at * HALO) & (lane < (at + 1) * HALO)
                first = source[place + (slice(None), slice(0, LANES))]
                last = source[place + (slice(None), slice(width - LANES, width))]
                if at:
                    first = pltpu.roll(first, at * HALO, 1)
                turn = (at * HALO + HALO) % LANES
                if turn:
                    last = pltpu.roll(last, turn, 1)
                low = jnp.where(inside, first, low)
                high = jnp.where(inside, last, high)
            packed[0, group] = low
            packed[1, group] = high

    def send_halo(cycle):
        copies = []
        for at, target in ((0, left[cycle > 0]), (1, right[cycle > 0])):
            copy = remote(
                packed.at[at], halo.at[cycle, at],
                send_n.at[cycle, at], recv_n.at[cycle, at], target,
            )
            copy.start()
            copies.append(copy)
        return copies

    def unpack(source, cycle):
        lane = iota((block, LANES), 1)
        per = LANES // HALO
        for field, target in ((0, edge_u), (1, edge_h)):
            for level in range(levels):
                index = field * levels + level
                group, at = index // per, index % per
                place = (level // slab_levels, level % slab_levels)
                before = halo[cycle, 1, group]
                after = halo[cycle, 0, group]
                if at:
                    before = pltpu.roll(before, LANES - at * HALO, 1)
                turn = (2 * LANES - HALO - at * HALO) % LANES
                if turn:
                    after = pltpu.roll(after, turn, 1)
                first = source[(field,) + place + (slice(None), slice(0, LANES))]
                last = source[(field,) + place + (slice(None), slice(width - LANES, width))]
                mixed = jnp.where(
                    lane < LANES // 2,
                    pltpu.roll(first, HALO, 1), pltpu.roll(last, LANES - HALO, 1),
                )
                mixed = jnp.where(lane < HALO, before, mixed)
                target[place] = jnp.where(lane >= LANES - HALO, after, mixed)

    def rise(field):
        return pltpu.roll(field, field.shape[-1] - 1, 1) - pltpu.roll(field, 1, 1)

    def substep(read_u, read_h, write_u, write_h, press):
        span = press.shape[-1]
        for at in range(span // LANES):
            lanes = slice(at * LANES, (at + 1) * LANES)
            high, low = split(read_h(slice(0, slab_count), lanes).reshape(rows, LANES))
            result = one(kron[0], high) + (one(kron[0], low) + one(kron[1], high))
            press[:, :, :, lanes] = result.reshape(slab_count, slab_levels, block, LANES)
        everything = slice(0, span)

        for at in range(slab_count):
            part = slice(at, at + 1)
            size = (slab_levels * block, span)
            velocity = read_u(part, everything).reshape(size)
            height = read_h(part, everything).reshape(size)
            pressure = press[part].reshape(size)
            moved = velocity - 0.5 * time_step * (velocity * rise(velocity) + rise(pressure))
            risen = height - 0.5 * time_step * rise(moved * height)
            write_u[part] = moved.reshape(1, slab_levels, block, span)
            write_h[part] = risen.reshape(1, slab_levels, block, span)

    def reader(ref):
        return lambda part, lanes: ref[part, :, :, lanes]

    def field_reader(ref, field):
        return lambda part, lanes: ref[field, part, :, :, lanes]

    def advance(source, cycle, greet):
        substep(field_reader(source, 0), field_reader(source, 1), u_ref, h_ref, p_ref)

        def again(step, carry):
            substep(reader(u_ref), reader(h_ref), u_ref, h_ref, p_ref)
            return carry

        def edge(step, carry):
            substep(reader(edge_u), reader(edge_h), edge_u, edge_h, edge_p)
            return carry

        def both(step, carry):
            return edge(step, again(step, carry))

        ahead = 1
        if ahead > 1:
            lax.fori_loop(1, ahead, again, 0)
        copies = greet()
        lax.fori_loop(ahead, SUBSTEPS, again, 0)
        for copy in copies:
            copy.wait()
        unpack(source, cycle)
        lax.fori_loop(0, SUBSTEPS, edge, 0)
        lane = iota((block, LANES), 1)
        for strip, whole in ((edge_h, h_ref), (edge_u, u_ref)):
            for at in range(slab_count):
                for level in range(slab_levels):
                    fresh = strip[at, level]
                    first = whole[at, level, :, 0:LANES]
                    last = whole[at, level, :, width - LANES : width]
                    whole[at, level, :, 0:LANES] = jnp.where(
                        lane < HALO, pltpu.roll(fresh, LANES - HALO, 1), first
                    )
                    whole[at, level, :, width - LANES : width] = jnp.where(
                        lane >= LANES - HALO, pltpu.roll(fresh, HALO, 1), last
                    )

    def arrive(target, recv_sem, other):
        remote(
            target.at[other], target.at[other], recv_sem.at[other], recv_sem.at[other], {"hor": hor}
        ).wait_recv()

    def cube_send(source, target, send_sem, recv_sem, some=slice(None)):
        copies = []
        for device, other in cube[some]:
            copy = remote(
                source.at[other], target.at[slab], send_sem.at[other], recv_sem.at[slab], device
            )
            copy.start()
            copies.append(copy)
        return copies

    def cube_take(target, recv_sem):
        for _, other in cube:
            arrive(target, recv_sem, other)

    def relay_copy(field, source, at, other):
        return remote(
            source.at[other], relayed.at[field, at], send_r.at[field, at], recv_r.at[field, at],
            {"hor": 2 * pair + 1 - side},
        )

    def inward_relay(field, source):
        @pl.when(away == 1)
        def _():
            for at, step in enumerate(steps[: len(steps) // 2]):
                relay_copy(field, source, at, spot(half, 1, *step[1:])[1]).start()

    def inward_copies(spots, source, target, send_sem, recv_sem):
        return [
            remote(
                source.at[other], target.at[first_block],
                send_sem.at[other], recv_sem.at[first_block], device,
            )
            for device, other in spots
        ]

    straight = [there for _, there in across]

    def forward_copy(field, target, recv_sem, at, device):
        return remote(
            relayed.at[field, at], target.at[first_block],
            send_g.at[field, at], recv_sem.at[first_block], device,
        )

    def inward_send(field, source, target, send_sem, recv_sem, early=True, late=True):
        some = slice(0 if early else EARLY, None if late else EARLY)

        @pl.when(away == 1)
        def _():
            for copy in inward_copies(straight[some], source, target, send_sem, recv_sem):
                copy.start()

        @pl.when(away == 0)
        def _():
            if early:
                for copy in inward_copies(level_first, source, target, send_sem, recv_sem):
                    copy.start()
            own_copies = inward_copies(level_later[some], source, target, send_sem, recv_sem)
            for copy, (at, (device, other)) in zip(own_copies, across[some]):
                copy.start()
                relay_copy(field, source, at, other).wait_recv()
                forward_copy(field, target, recv_sem, at, device).start()

    def inward_drain(field, source, target, send_sem, recv_sem):
        @pl.when(away == 1)
        def _():
            for copy in inward_copies(straight, source, target, send_sem, recv_sem):
                copy.wait_send()
            for at, step in enumerate(steps[: len(steps) // 2]):
                relay_copy(field, source, at, spot(half, 1, *step[1:])[1]).wait_send()

        @pl.when(away == 0)
        def _():
            for copy in inward_copies(cube, source, target, send_sem, recv_sem):
                copy.wait_send()
            for at, (device, other) in across:
                forward_copy(field, target, recv_sem, at, device).wait_send()

    def inward_take(target, recv_sem):
        for step_mem in range(mem_count):
            for step_grp in range(grp_count):
                other = turned(mem, step_mem, mem_count) * grp_count + turned(grp, step_grp, grp_count)
                if step_mem + step_grp:
                    arrive(target, recv_sem, other)
                else:
                    @pl.when(away == 1)
                    def _():
                        arrive(target, recv_sem, other)

    crossing = [(at + depth) % mem_count for at in range(mem_count) if at != depth]

    def outward_copies(field):
        copies = []
        for step_mem in [0] + crossing:
            for step_grp in range(grp_count):
                to_mem = turned(mem, step_mem, mem_count)
                to_grp = turned(grp, step_grp, grp_count)
                other = to_mem * grp_count + to_grp
                copies.append(remote(
                    updated.at[field, other], final_hbm.at[field, slab],
                    send_f.at[field, other], recv_f.at[field, slab],
                    {"mem": to_mem, "hor": 2 * pair + half, "grp": to_grp},
                ))
        return copies

    def keep_copy(field):
        return pltpu.make_async_copy(
            updated.at[field, slab], final_hbm.at[field, slab], send_f.at[field, slab]
        )

    def outward_send(field):
        copies = outward_copies(field)

        @pl.when(away == 1)
        def _():
            copies[0].start()

        for copy in copies[1:]:
            copy.start()

        @pl.when(away == 0)
        def _():
            keep_copy(field).start()

    def outward_finish(field):
        for at in range(slab_count):
            other = turned(slab, at, slab_count)
            if at:
                arrive(final_hbm.at[field], recv_f.at[field], other)
            else:
                @pl.when(away == 1)
                def _():
                    arrive(final_hbm.at[field], recv_f.at[field], other)
        copies = outward_copies(field)

        @pl.when(away == 1)
        def _():
            copies[0].wait_send()

        @pl.when(away == 0)
        def _():
            keep_copy(field).wait()

        for copy in copies[1:]:
            copy.wait_send()

    def bundle_copy():
        return remote(
            bundle, notes, send_o.at[0], recv_o.at[0],
            {"mem": turned(mem, depth, mem_count), "hor": 2 * pair + 1 - side},
        )

    def sum_cells(cycle):
        place = notes[cycle, 0:1].astype(jnp.int32)
        weight = notes[cycle, 1:2]
        pulled = notes[cycle, 2:3]
        parts = split3(weight) + split3(pulled)
        spare = jnp.zeros((16 - len(parts), weight.shape[1]), jnp.bfloat16)
        lhs = jnp.concatenate(parts + (spare,), axis=0)
        total = slab_levels * width

        def chunk(at, carry):
            numbers = iota((LANES, weight.shape[1]), 0) + at * LANES
            hits = jnp.where(numbers == place, 1.0, 0.0).astype(jnp.bfloat16)
            sums = one(lhs, hits, 1)
            cells[0, at] = sums[0:1] + (sums[1:2] + sums[2:3])
            cells[1, at] = sums[3:4] + (sums[4:5] + sums[5:6])
            return carry

        lax.fori_loop(0, total // LANES, chunk, 0)

    def gram():
        per = width // LANES
        total = None
        for level in range(slab_levels):
            flat = heights[:, level].reshape(members, width)
            average = jnp.mean(flat, axis=0, keepdims=True)
            anomalies = flat - average
            weight = jnp.concatenate(
                [cells[0, level * per + at] for at in range(per)], axis=1
            )
            pulled = jnp.concatenate(
                [cells[1, level * per + at] for at in range(per)], axis=1
            )
            pull = pulled - weight * average
            lhs = jnp.concatenate(
                [anomalies * weight, jnp.broadcast_to(pull, (8, width))], axis=0
            )
            here = product(lhs, anomalies, 1)
            total = here if total is None else total + here
        short = members // 2
        row, lane = iota((short, members), 0), iota((short, members), 1)
        upper = total[:short]
        own[:short] = jnp.where(
            lane - short > row, pltpu.roll(upper, short, 1), total[short:members]
        )
        diagonal = jnp.sum(jnp.where(lane == row, upper, 0.0), axis=0, keepdims=True)
        own[short:] = jnp.where(
            iota((8, members), 0) == 0, total[members:], jnp.broadcast_to(diagonal, (8, members))
        )

    def unfold(total):
        short = members // 2
        row, lane = iota((short, members), 0), iota((short, members), 1)
        lower = total[:short]
        turned_over = jnp.transpose(jnp.concatenate([lower, lower], axis=0))
        first, second = turned_over[:short], turned_over[short:]
        inside = jnp.where(lane < row, second, total[short + 1 : short + 2])
        inside = jnp.where(lane > row, pltpu.roll(lower, short, 1), inside)
        top = jnp.where(lane >= short, first, inside)
        bottom = jnp.where(lane - short > row, second, lower)
        return jnp.concatenate([top, bottom], axis=0), total[short : short + 1]

    lanes = iota((1, lane_count), 1)

    def share(row, step):
        place = turned(line, mem_count - step, mem_count) * grp_count + grp
        return jnp.sum(jnp.where(lanes == place, row[0:1], 0.0), axis=1, keepdims=True)

    def blended_for(row):
        total = share(row, 0) * own[...]
        for step in range(1, mem_count):
            total = total + share(row, step) * column[step - 1]
        return total

    def root(total):
        total = total / (count + 1.0)
        square = (members, members)
        identity = (iota(square, 0) == iota(square, 1)).astype(jnp.float32)
        whole, bvector = unfold(total)
        blended = (members - 1.0) * identity + whole
        bvector = jnp.broadcast_to(bvector, (8, members))
        squares = jnp.sum(
            jnp.sum(blended * blended, axis=1, keepdims=True), axis=0, keepdims=True
        )
        frobenius = jnp.sqrt(squares)
        iterate = blended / frobenius
        newton = 1.5 * identity - 0.5 * iterate
        inverse_root = newton
        for step in range(1, ROOT_STEPS):
            iterate = product(newton, iterate)
            newton = 1.5 * identity - 0.5 * product(inverse_root, iterate)
            if step == ROOT_STEPS - 1:
                inner = product(product(bvector, newton), inverse_root)
            inverse_root = product(newton, inverse_root)
        spread = inverse_root * (jnp.sqrt(members - 1.0) / jnp.sqrt(frobenius))
        mean_weight = product(inner, inverse_root) / frobenius
        return spread + mean_weight[0:1]

    def update(transposed, source, field):
        high, low = split(transposed)
        for level in range(slab_levels):
            flat = source[:, level].reshape(members, width)
            average = jnp.mean(flat, axis=0, keepdims=True)
            flat_high, flat_low = split(flat - average)
            result = average + (
                one(high, flat_high) + (one(high, flat_low) + one(low, flat_high))
            )
            updated[field, :, level] = result.reshape(slab_count, block, width)

    for copy in fetches[1:]:
        copy.wait()
    for cycle in range(cycles):
        weight = live_ref[cycle].astype(jnp.float32) / error_ref[cycle]
        place = level_ref[cycle] * width + column_ref[cycle]
        bundle[cycle, 0:1] = place.astype(jnp.float32)
        bundle[cycle, 1:2] = weight
        bundle[cycle, 2:3] = weight * value_ref[cycle]
    numbers = iota((8, lane_count), 1)
    blend = jnp.where(numbers == first_block, 1.0, 0.0)
    for at in range(count):
        blend = blend + jnp.where(numbers == chosen_ref[0, at], 1.0, 0.0)
    bundle[cycles, :, 0:lane_count] = blend
    spread_rows = jnp.where(
        iota((rows, levels), 0) // block == iota((rows, levels), 1), 1.0, 0.0
    ).astype(jnp.bfloat16)
    same = lax.rem(iota((rows, rows), 0), block) == lax.rem(iota((rows, rows), 1), block)
    for at, part in enumerate(split(coupling_ref[...])):
        tall = one(spread_rows, part).astype(jnp.bfloat16)
        kron[at] = jnp.where(same, one(tall, spread_rows, 1), 0.0).astype(jnp.bfloat16)
    fetches[0].wait()
    for field in range(2):
        for at in range(0, levels, 8):
            part = given_ref[:, field, at : at + 8]
            part = jnp.swapaxes(part, 0, 1)
            x_ref[field, at // slab_levels : (at + 8) // slab_levels] = part.reshape(
                8 // slab_levels, slab_levels, block, width
            )
    pack(x_ref)

    def meet():
        pl.semaphore_wait(barrier, 2 * slab_count - 1 + 4)
        copies = send_halo(0)

        @pl.when(away == 1)
        def _():
            bundle_copy().start()

        @pl.when(away == 0)
        def _():
            notes[...] = bundle[...]

        return copies

    blend_copies = []
    for cycle in range(cycles):
        source = x_ref if cycle == 0 else returned
        if cycle:
            pack(source)
            copies = send_halo(cycle)
            advance(source, cycle, lambda: copies)
        else:
            advance(source, cycle, meet)
        heights_now = (h_ref, heights, send_h.at[cycle], recv_h.at[cycle])
        speeds_now = (u_ref, speeds, send_u.at[cycle], recv_u.at[cycle])
        drains = []
        if cycle == 0:
            inward_relay(1, h_ref)
            inward_send(1, *heights_now)
            inward_relay(0, u_ref)
            inward_send(0, *speeds_now, late=False)

            @pl.when(away == 1)
            def _():
                bundle_copy().wait()

            @pl.when(away == 0)
            def _():
                heights[slab] = h_ref[slab]
                speeds[slab] = u_ref[slab]

            blends[0] = notes[cycles, 0:8, 0:lane_count]
            for step in range(1, grp_count):
                copy = remote(
                    blends.at[0], blends.at[step], send_b.at[step], recv_b.at[step],
                    {"grp": turned(grp, step, grp_count)},
                )
                copy.start()
                blend_copies.append(copy)
        else:
            drains = cube_send(*heights_now) + cube_send(*speeds_now, slice(0, 2 * EARLY))
            heights[slab] = h_ref[slab]
            speeds[slab] = u_ref[slab]
        sum_cells(cycle)
        if cycle == 0:
            inward_take(heights, recv_h.at[cycle])
        else:
            cube_take(heights, recv_h.at[cycle])
        gram()

        gathers = []
        for step in range(1, mem_count):
            to_line = turned(line, step, mem_count)
            copy = remote(
                own, column.at[step - 1], send_a.at[cycle, step - 1], recv_a.at[cycle, step - 1],
                {"mem": half * depth + lax.rem(to_line, depth), "hor": 2 * pair + to_line // depth},
            )
            copy.start()
            gathers.append(copy)
        if cycle == 0:
            inward_send(0, *speeds_now, early=False)
        else:
            drains = drains + cube_send(*speeds_now, slice(2 * EARLY, None))
        for copy in blend_copies:
            copy.wait()
        blend_copies = []
        for copy in gathers:
            copy.wait()
        returns = []
        for step in range(1, grp_count):
            partial[step - 1] = blended_for(blends[step])
            copy = remote(
                partial.at[step - 1], arrived.at[step - 1],
                send_c.at[cycle, step - 1], recv_c.at[cycle, step - 1],
                {"grp": turned(grp, grp_count - step, grp_count)},
            )
            copy.start()
            returns.append(copy)
        total = blended_for(blends[0])
        for copy in returns:
            copy.wait()
        for step in range(1, grp_count):
            total = total + arrived[step - 1]
        transposed = root(total)
        last = cycle == cycles - 1
        for field, patch in ((1, heights), (0, speeds)):
            if field == 0:
                if cycle == 0:
                    inward_take(speeds, recv_u.at[cycle])
                else:
                    cube_take(speeds, recv_u.at[cycle])
            update(transposed, patch, field)
            if last:
                outward_send(field)
            else:
                drains = drains + cube_send(
                    updated.at[field], returned.at[field],
                    send_e.at[cycle, field], recv_e.at[cycle, field],
                )
                returned[field, slab] = updated[field, slab]
        if not last:
            for field in (1, 0):
                cube_take(returned.at[field], recv_e.at[cycle, field])
        for copy in drains:
            copy.wait_send()
        if cycle == 0:
            inward_drain(1, *heights_now)
            inward_drain(0, *speeds_now)
    for field in (1, 0):
        outward_finish(field)


def turn(state_hbm, out_hbm, given, turned, read_sem, write_sem):
    fields, slab_count, slab_levels, block, width = given.shape
    per = 8 // slab_levels
    parts = [(field, at) for field in (1, 0) for at in range(0, slab_count, per)]
    reads, writes = [], []
    for number, (field, at) in enumerate(parts):
        copy = pltpu.make_async_copy(
            state_hbm.at[field, at : at + per], given.at[field, at : at + per],
            read_sem.at[number],
        )
        copy.start()
        reads.append(copy)
    for number, (field, at) in enumerate(parts):
        reads[number].wait()
        levels = slice(at * slab_levels, (at + per) * slab_levels)
        part = given[field, at : at + per].reshape(8, block, width)
        turned[:, field, levels] = jnp.swapaxes(part, 0, 1)
        copy = pltpu.make_async_copy(
            turned.at[:, field, levels], out_hbm.at[:, field, levels], write_sem.at[number]
        )
        copy.start()
        writes.append(copy)
    for copy in writes:
        copy.wait()


def shards(ensemble, coupling, obs_column, obs_level, obs_value, obs_error, obs_live, partners):
    mem_count = lax.axis_size("mem")
    grp_count = lax.axis_size("grp")
    hor_count = lax.axis_size("hor")
    slab_count = mem_count * grp_count
    lanes = max(LANES, -(-slab_count // LANES) * LANES)
    count = partners.shape[-1]
    block, fields, levels, width = ensemble.shape
    cycles = obs_column.shape[0]
    members = block * slab_count
    slab_levels = levels // slab_count
    state = (slab_count, slab_levels, block, width)
    strip = (slab_count, slab_levels, block, LANES)
    tall = (members // 2 + 8, members)
    rows = levels * block
    groups = 2 * levels * HALO // LANES
    noted = (cycles, 1, obs_column.shape[-1])
    slots = max(obs_column.shape[-1], lanes)
    vmem = pl.BlockSpec(memory_space=pltpu.VMEM)
    dma = pltpu.SemaphoreType.DMA
    f32 = jnp.float32
    result = pl.pallas_call(
        functools.partial(program, (mem_count, grp_count, hor_count), count, cycles),
        out_shape=jax.ShapeDtypeStruct((2,) + state, f32),
        in_specs=[pl.BlockSpec(memory_space=pltpu.HBM)] * 7 + [pl.BlockSpec(memory_space=pltpu.SMEM)],
        out_specs=pl.BlockSpec(memory_space=pl.ANY),
        scratch_shapes=[
            pltpu.VMEM(ensemble.shape, f32), pltpu.VMEM(coupling.shape, f32),
            pltpu.VMEM(noted, jnp.int32), pltpu.VMEM(noted, jnp.int32),
            pltpu.VMEM(noted, f32), pltpu.VMEM(noted, f32), pltpu.VMEM(noted, jnp.int32),
            dma((7,)),
            pltpu.VMEM((2,) + state, f32),
            pltpu.VMEM((2, rows, rows), jnp.bfloat16),
            pltpu.VMEM(state, f32), pltpu.VMEM(state, f32), pltpu.VMEM(state, f32),
            pltpu.VMEM(strip, f32), pltpu.VMEM(strip, f32), pltpu.VMEM(strip, f32),
            pltpu.VMEM((2, groups, block, LANES), f32),
            pltpu.VMEM((cycles, 2, groups, block, LANES), f32),
            pltpu.VMEM(state, f32), pltpu.VMEM(state, f32),
            pltpu.VMEM((2,) + state, f32), pltpu.VMEM((2,) + state, f32),
            pltpu.VMEM((2, slab_count // 2) + state[1:], f32),
            pltpu.VMEM((2, slab_levels * width // LANES, 1, LANES), f32),
            pltpu.VMEM((cycles + 1, 8, slots), f32), pltpu.VMEM((cycles + 1, 8, slots), f32),
            pltpu.VMEM(tall, f32),
            pltpu.VMEM((mem_count - 1,) + tall, f32),
            pltpu.VMEM((grp_count - 1,) + tall, f32),
            pltpu.VMEM((grp_count - 1,) + tall, f32),
            pltpu.VMEM((grp_count, 8, lanes), f32),
            dma((cycles, 2)), dma((cycles, 2)),
            dma((1,)), dma((1,)),
            dma((cycles, mem_count - 1)), dma((cycles, mem_count - 1)),
            dma((grp_count,)), dma((grp_count,)),
            dma((cycles, grp_count - 1)), dma((cycles, grp_count - 1)),
            dma((cycles, slab_count)), dma((cycles, slab_count)),
            dma((cycles, slab_count)), dma((cycles, slab_count)),
            dma((cycles, 2, slab_count)), dma((cycles, 2, slab_count)),
            dma((2, slab_count)), dma((2, slab_count)),
            dma((2, slab_count // 2)), dma((2, slab_count // 2)), dma((2, slab_count // 2)),
        ],
        compiler_params=pltpu.CompilerParams(collective_id=0, has_side_effects=True),
    )(
        ensemble, coupling, obs_column[:, 0], obs_level[:, 0], obs_value[:, 0], obs_error[:, 0],
        obs_live[:, 0], partners[0],
    )
    anywhere = pl.BlockSpec(memory_space=pl.ANY)
    parts = 2 * levels // 8
    return pl.pallas_call(
        turn,
        out_shape=jax.ShapeDtypeStruct(ensemble.shape, f32),
        in_specs=[anywhere], out_specs=anywhere,
        scratch_shapes=[
            pltpu.VMEM((2,) + state, f32), pltpu.VMEM(ensemble.shape, f32),
            dma((parts,)), dma((parts,)),
        ],
    )(result)


def solution(mesh):
    in_specs = (
        P(("mem", "grp"), None, None, "hor"),
        P(),
        P(None, ("mem", "grp"), "hor", None),
        P(None, ("mem", "grp"), "hor", None),
        P(None, ("mem", "grp"), "hor", None),
        P(None, ("mem", "grp"), "hor", None),
        P(None, ("mem", "grp"), "hor", None),
        P(("mem", "grp"), "hor", None),
    )
    out_specs = P(("mem", "grp"), None, None, "hor")
    return jax.shard_map(shards, mesh=mesh, in_specs=in_specs, out_specs=out_specs, check_vma=False)
```

```python
import functools

import jax
import jax.numpy as jnp
from jax import lax
from jax.experimental import pallas as pl
from jax.experimental.pallas import tpu as pltpu
from jax.sharding import PartitionSpec as P

SUBSTEPS = 4
ROOT_STEPS = 8
MESH = pl.DeviceIdType.MESH
LANES = 128
HALO = 2 * SUBSTEPS
EARLY = 1

time_step = 0.2


def split(value):
    high = value.astype(jnp.bfloat16)
    return high, (value - high.astype(jnp.float32)).astype(jnp.bfloat16)


def split3(value):
    high, rest = value.astype(jnp.bfloat16), None
    rest = value - high.astype(jnp.float32)
    middle = rest.astype(jnp.bfloat16)
    low = (rest - middle.astype(jnp.float32)).astype(jnp.bfloat16)
    return high, middle, low


def one(a, b, across=0):
    dims = (((1,), (across,)), ((), ()))
    return lax.dot_general(a, b, dims, preferred_element_type=jnp.float32)


def product(left, right, across=0):
    left_high, left_low = split(left)
    right_high, right_low = split(right)
    return one(left_high, right_high, across) + (
        one(left_high, right_low, across) + one(left_low, right_high, across)
    )


def iota(shape, axis):
    return lax.broadcasted_iota(jnp.int32, shape, axis)


def program(
    sizes, count, cycles,
    given_hbm, coupling_hbm, column_hbm, level_hbm, value_hbm, error_hbm, live_hbm, chosen_ref,
    final_hbm,
    given_ref, coupling_ref, column_ref, level_ref, value_ref, error_ref, live_ref, fetch_sem,
    x_ref, kron, u_ref, h_ref, p_ref, edge_u, edge_h, edge_p, packed, halo,
    heights, speeds, updated, returned, relayed, cells, bundle, notes,
    own, column, partial, arrived, blends,
    send_n, recv_n, send_o, recv_o, send_a, recv_a, send_b, recv_b, send_c, recv_c,
    send_h, recv_h, send_u, recv_u, send_e, recv_e, send_f, recv_f,
    send_r, recv_r, send_g,
):
    fetches = []
    for at, (source, target) in enumerate((
        (given_hbm, given_ref), (coupling_hbm, coupling_ref), (column_hbm, column_ref),
        (level_hbm, level_ref), (value_hbm, value_ref), (error_hbm, error_ref),
        (live_hbm, live_ref),
    )):
        copy = pltpu.make_async_copy(source, target, fetch_sem.at[at])
        copy.start()
        fetches.append(copy)
    mem_count, grp_count, hor_count = sizes
    mem = lax.axis_index("mem")
    grp = lax.axis_index("grp")
    hor = lax.axis_index("hor")
    slab_count = mem_count * grp_count
    slab_levels, block, width = x_ref.shape[2:]
    lane_count = blends.shape[2]
    levels = slab_count * slab_levels
    rows = levels * block
    members = slab_count * block

    depth = mem_count // 2
    pairs = hor_count // 2
    pair = hor // 2
    side = lax.rem(hor, 2)
    half = mem // depth
    deep = lax.rem(mem, depth)
    away = half + side - 2 * half * side
    line = side * depth + deep
    slab = line * grp_count + grp
    first_block = mem * grp_count + grp

    def turned(at, step, size):
        return lax.rem(at + step, size)

    def spot(in_half, step_side, step_deep, step_grp):
        to_side = turned(side, step_side, 2)
        to_deep = turned(deep, step_deep, depth)
        to_grp = turned(grp, step_grp, grp_count)
        device = {"mem": in_half * depth + to_deep, "hor": 2 * pair + to_side, "grp": to_grp}
        return device, (to_side * depth + to_deep) * grp_count + to_grp

    steps = [
        (one_side, one_deep, one_grp)
        for one_side in range(2) for one_deep in range(depth) for one_grp in range(grp_count)
    ]
    cube = [spot(half, *step) for step in steps[:0:-1]]
    level_first = [spot(half, *step) for step in steps[1:] if step[1] == 0]
    level_later = [spot(half, *step) for step in steps[1:] if step[1]]
    across = [(at, spot(1 - half, 0, *step[1:])) for at, step in enumerate(steps[: len(steps) // 2])]

    right = ({"hor": turned(hor, 1, hor_count)},
             {"mem": turned(mem, depth, mem_count),
              "hor": 2 * turned(pair, half, pairs) + side})
    left = ({"hor": turned(hor, hor_count - 1, hor_count)},
            {"mem": turned(mem, depth, mem_count),
             "hor": 2 * turned(pair, half + pairs - 1, pairs) + side})

    barrier = pltpu.get_barrier_semaphore()
    for device, _ in cube + [spot(1 - half, *step) for step in steps]:
        pl.semaphore_signal(barrier, inc=1, device_id=device, device_id_type=MESH)
    for device in left + right:
        pl.semaphore_signal(barrier, inc=1, device_id=device, device_id_type=MESH)

    def remote(source, target, send_sem, recv_sem, device):
        return pltpu.make_async_remote_copy(
            src_ref=source, dst_ref=target, send_sem=send_sem, recv_sem=recv_sem,
            device_id=device, device_id_type=MESH,
        )

    def pack(source):
        lane = iota((block, LANES), 1)
        per = LANES // HALO
        for group in range(2 * levels // per):
            low = jnp.zeros((block, LANES), jnp.float32)
            high = jnp.zeros((block, LANES), jnp.float32)
            for at in range(per):
                index = group * per + at
                field, level = index // levels, index % levels
                place = (field, level // slab_levels, level % slab_levels)
                inside = (lane >= at * HALO) & (lane < (at + 1) * HALO)
                first = source[place + (slice(None), slice(0, LANES))]
                last = source[place + (slice(None), slice(width - LANES, width))]
                if at:
                    first = pltpu.roll(first, at * HALO, 1)
                turn = (at * HALO + HALO) % LANES
                if turn:
                    last = pltpu.roll(last, turn, 1)
                low = jnp.where(inside, first, low)
                high = jnp.where(inside, last, high)
            packed[0, group] = low
            packed[1, group] = high

    def send_halo(cycle):
        copies = []
        for at, target in ((0, left[cycle > 0]), (1, right[cycle > 0])):
            copy = remote(
                packed.at[at], halo.at[cycle, at],
                send_n.at[cycle, at], recv_n.at[cycle, at], target,
            )
            copy.start()
            copies.append(copy)
        return copies

    def unpack(source, cycle):
        lane = iota((block, LANES), 1)
        per = LANES // HALO
        for field, target in ((0, edge_u), (1, edge_h)):
            for level in range(levels):
                index = field * levels + level
                group, at = index // per, index % per
                place = (level // slab_levels, level % slab_levels)
                before = halo[cycle, 1, group]
                after = halo[cycle, 0, group]
                if at:
                    before = pltpu.roll(before, LANES - at * HALO, 1)
                turn = (2 * LANES - HALO - at * HALO) % LANES
                if turn:
                    after = pltpu.roll(after, turn, 1)
                first = source[(field,) + place + (slice(None), slice(0, LANES))]
                last = source[(field,) + place + (slice(None), slice(width - LANES, width))]
                mixed = jnp.where(
                    lane < LANES // 2,
                    pltpu.roll(first, HALO, 1), pltpu.roll(last, LANES - HALO, 1),
                )
                mixed = jnp.where(lane < HALO, before, mixed)
                target[place] = jnp.where(lane >= LANES - HALO, after, mixed)

    def rise(field):
        return pltpu.roll(field, field.shape[-1] - 1, 1) - pltpu.roll(field, 1, 1)

    def substep(read_u, read_h, write_u, write_h, press):
        span = press.shape[-1]
        for at in range(span // LANES):
            lanes = slice(at * LANES, (at + 1) * LANES)
            high, low = split(read_h(slice(0, slab_count), lanes).reshape(rows, LANES))
            result = one(kron[0], high) + (one(kron[0], low) + one(kron[1], high))
            press[:, :, :, lanes] = result.reshape(slab_count, slab_levels, block, LANES)
        everything = slice(0, span)

        for at in range(slab_count):
            part = slice(at, at + 1)
            size = (slab_levels * block, span)
            velocity = read_u(part, everything).reshape(size)
            height = read_h(part, everything).reshape(size)
            pressure = press[part].reshape(size)
            moved = velocity - 0.5 * time_step * (velocity * rise(velocity) + rise(pressure))
            risen = height - 0.5 * time_step * rise(moved * height)
            write_u[part] = moved.reshape(1, slab_levels, block, span)
            write_h[part] = risen.reshape(1, slab_levels, block, span)

    def reader(ref):
        return lambda part, lanes: ref[part, :, :, lanes]

    def field_reader(ref, field):
        return lambda part, lanes: ref[field, part, :, :, lanes]

    def advance(source, cycle, greet):
        substep(field_reader(source, 0), field_reader(source, 1), u_ref, h_ref, p_ref)

        def again(step, carry):
            substep(reader(u_ref), reader(h_ref), u_ref, h_ref, p_ref)
            return carry

        def edge(step, carry):
            substep(reader(edge_u), reader(edge_h), edge_u, edge_h, edge_p)
            return carry

        def both(step, carry):
            return edge(step, again(step, carry))

        ahead = 1
        if ahead > 1:
            lax.fori_loop(1, ahead, again, 0)
        copies = greet()
        lax.fori_loop(ahead, SUBSTEPS, again, 0)
        for copy in copies:
            copy.wait()
        unpack(source, cycle)
        lax.fori_loop(0, SUBSTEPS, edge, 0)
        mend(edge_h, h_ref)

    def mend(strip, whole):
        lane = iota((block, LANES), 1)
        for at in range(slab_count):
            for level in range(slab_levels):
                fresh = strip[at, level]
                first = whole[at, level, :, 0:LANES]
                last = whole[at, level, :, width - LANES : width]
                whole[at, level, :, 0:LANES] = jnp.where(
                    lane < HALO, pltpu.roll(fresh, LANES - HALO, 1), first
                )
                whole[at, level, :, width - LANES : width] = jnp.where(
                    lane >= LANES - HALO, pltpu.roll(fresh, HALO, 1), last
                )

    def arrive(target, recv_sem, other):
        remote(
            target.at[other], target.at[other], recv_sem.at[other], recv_sem.at[other], {"hor": hor}
        ).wait_recv()

    def cube_send(source, target, send_sem, recv_sem, some=slice(None)):
        copies = []
        for device, other in cube[some]:
            copy = remote(
                source.at[other], target.at[slab], send_sem.at[other], recv_sem.at[slab], device
            )
            copy.start()
            copies.append(copy)
        return copies

    def cube_take(target, recv_sem):
        for _, other in cube:
            arrive(target, recv_sem, other)

    def relay_copy(field, source, at, other):
        return remote(
            source.at[other], relayed.at[field, at], send_r.at[field, at], recv_r.at[field, at],
            {"hor": 2 * pair + 1 - side},
        )

    def inward_relay(field, source):
        @pl.when(away == 1)
        def _():
            for at, step in enumerate(steps[: len(steps) // 2]):
                relay_copy(field, source, at, spot(half, 1, *step[1:])[1]).start()

    def inward_copies(spots, source, target, send_sem, recv_sem):
        return [
            remote(
                source.at[other], target.at[first_block],
                send_sem.at[other], recv_sem.at[first_block], device,
            )
            for device, other in spots
        ]

    straight = [there for _, there in across]

    def forward_copy(field, target, recv_sem, at, device):
        return remote(
            relayed.at[field, at], target.at[first_block],
            send_g.at[field, at], recv_sem.at[first_block], device,
        )

    def inward_send(field, source, target, send_sem, recv_sem, early=True, late=True):
        some = slice(0 if early else EARLY, None if late else EARLY)

        @pl.when(away == 1)
        def _():
            for copy in inward_copies(straight[some], source, target, send_sem, recv_sem):
                copy.start()

        @pl.when(away == 0)
        def _():
            if early:
                for copy in inward_copies(level_first, source, target, send_sem, recv_sem):
                    copy.start()
            own_copies = inward_copies(level_later[some], source, target, send_sem, recv_sem)
            for copy, (at, (device, other)) in zip(own_copies, across[some]):
                copy.start()
                relay_copy(field, source, at, other).wait_recv()
                forward_copy(field, target, recv_sem, at, device).start()

    def inward_drain(field, source, target, send_sem, recv_sem):
        @pl.when(away == 1)
        def _():
            for copy in inward_copies(straight, source, target, send_sem, recv_sem):
                copy.wait_send()
            for at, step in enumerate(steps[: len(steps) // 2]):
                relay_copy(field, source, at, spot(half, 1, *step[1:])[1]).wait_send()

        @pl.when(away == 0)
        def _():
            for copy in inward_copies(cube, source, target, send_sem, recv_sem):
                copy.wait_send()
            for at, (device, other) in across:
                forward_copy(field, target, recv_sem, at, device).wait_send()

    def inward_take(target, recv_sem):
        for step_mem in range(mem_count):
            for step_grp in range(grp_count):
                other = turned(mem, step_mem, mem_count) * grp_count + turned(grp, step_grp, grp_count)
                if step_mem + step_grp:
                    arrive(target, recv_sem, other)
                else:
                    @pl.when(away == 1)
                    def _():
                        arrive(target, recv_sem, other)

    crossing = [(at + depth) % mem_count for at in range(mem_count) if at != depth]

    def outward_copies(field):
        copies = []
        for step_mem in [0] + crossing:
            for step_grp in range(grp_count):
                to_mem = turned(mem, step_mem, mem_count)
                to_grp = turned(grp, step_grp, grp_count)
                other = to_mem * grp_count + to_grp
                copies.append(remote(
                    updated.at[field, other], final_hbm.at[field, slab],
                    send_f.at[field, other], recv_f.at[field, slab],
                    {"mem": to_mem, "hor": 2 * pair + half, "grp": to_grp},
                ))
        return copies

    def keep_copy(field):
        return pltpu.make_async_copy(
            updated.at[field, slab], final_hbm.at[field, slab], send_f.at[field, slab]
        )

    def outward_send(field):
        copies = outward_copies(field)

        @pl.when(away == 1)
        def _():
            copies[0].start()

        for copy in copies[1:]:
            copy.start()

        @pl.when(away == 0)
        def _():
            keep_copy(field).start()

    def outward_finish(field):
        for at in range(slab_count):
            other = turned(slab, at, slab_count)
            if at:
                arrive(final_hbm.at[field], recv_f.at[field], other)
            else:
                @pl.when(away == 1)
                def _():
                    arrive(final_hbm.at[field], recv_f.at[field], other)
        copies = outward_copies(field)

        @pl.when(away == 1)
        def _():
            copies[0].wait_send()

        @pl.when(away == 0)
        def _():
            keep_copy(field).wait()

        for copy in copies[1:]:
            copy.wait_send()

    def bundle_copy():
        return remote(
            bundle, notes, send_o.at[0], recv_o.at[0],
            {"mem": turned(mem, depth, mem_count), "hor": 2 * pair + 1 - side},
        )

    def sum_cells(cycle):
        place = notes[cycle, 0:1].astype(jnp.int32)
        weight = notes[cycle, 1:2]
        pulled = notes[cycle, 2:3]
        parts = split3(weight) + split3(pulled)
        spare = jnp.zeros((16 - len(parts), weight.shape[1]), jnp.bfloat16)
        lhs = jnp.concatenate(parts + (spare,), axis=0)
        total = slab_levels * width

        def chunk(at, carry):
            numbers = iota((LANES, weight.shape[1]), 0) + at * LANES
            hits = jnp.where(numbers == place, 1.0, 0.0).astype(jnp.bfloat16)
            sums = one(lhs, hits, 1)
            cells[0, at] = sums[0:1] + (sums[1:2] + sums[2:3])
            cells[1, at] = sums[3:4] + (sums[4:5] + sums[5:6])
            return carry

        lax.fori_loop(0, total // LANES, chunk, 0)

    def gram():
        per = width // LANES
        total = None
        for level in range(slab_levels):
            flat = heights[:, level].reshape(members, width)
            average = jnp.mean(flat, axis=0, keepdims=True)
            anomalies = flat - average
            weight = jnp.concatenate(
                [cells[0, level * per + at] for at in range(per)], axis=1
            )
            pulled = jnp.concatenate(
                [cells[1, level * per + at] for at in range(per)], axis=1
            )
            pull = pulled - weight * average
            lhs = jnp.concatenate(
                [anomalies * weight, jnp.broadcast_to(pull, (8, width))], axis=0
            )
            here = product(lhs, anomalies, 1)
            total = here if total is None else total + here
        short = members // 2
        row, lane = iota((short, members), 0), iota((short, members), 1)
        upper = total[:short]
        own[:short] = jnp.where(
            lane - short > row, pltpu.roll(upper, short, 1), total[short:members]
        )
        diagonal = jnp.sum(jnp.where(lane == row, upper, 0.0), axis=0, keepdims=True)
        own[short:] = jnp.where(
            iota((8, members), 0) == 0, total[members:], jnp.broadcast_to(diagonal, (8, members))
        )

    def unfold(total):
        short = members // 2
        row, lane = iota((short, members), 0), iota((short, members), 1)
        lower = total[:short]
        turned_over = jnp.transpose(jnp.concatenate([lower, lower], axis=0))
        first, second = turned_over[:short], turned_over[short:]
        inside = jnp.where(lane < row, second, total[short + 1 : short + 2])
        inside = jnp.where(lane > row, pltpu.roll(lower, short, 1), inside)
        top = jnp.where(lane >= short, first, inside)
        bottom = jnp.where(lane - short > row, second, lower)
        return jnp.concatenate([top, bottom], axis=0), total[short : short + 1]

    lanes = iota((1, lane_count), 1)

    def share(row, step):
        place = turned(line, mem_count - step, mem_count) * grp_count + grp
        return jnp.sum(jnp.where(lanes == place, row[0:1], 0.0), axis=1, keepdims=True)

    def blended_for(row):
        total = share(row, 0) * own[...]
        for step in range(1, mem_count):
            total = total + share(row, step) * column[step - 1]
        return total

    def root(total):
        total = total / (count + 1.0)
        square = (members, members)
        identity = (iota(square, 0) == iota(square, 1)).astype(jnp.float32)
        whole, bvector = unfold(total)
        blended = (members - 1.0) * identity + whole
        bvector = jnp.broadcast_to(bvector, (8, members))
        squares = jnp.sum(
            jnp.sum(blended * blended, axis=1, keepdims=True), axis=0, keepdims=True
        )
        frobenius = jnp.sqrt(squares)
        iterate = blended / frobenius
        newton = 1.5 * identity - 0.5 * iterate
        inverse_root = newton
        for step in range(1, ROOT_STEPS):
            iterate = product(newton, iterate)
            newton = 1.5 * identity - 0.5 * product(inverse_root, iterate)
            if step == ROOT_STEPS - 1:
                inner = product(product(bvector, newton), inverse_root)
            inverse_root = product(newton, inverse_root)
        spread = inverse_root * (jnp.sqrt(members - 1.0) / jnp.sqrt(frobenius))
        mean_weight = product(inner, inverse_root) / frobenius
        return spread + mean_weight[0:1]

    def update(transposed, source, field):
        high, low = split(transposed)
        for level in range(slab_levels):
            flat = source[:, level].reshape(members, width)
            average = jnp.mean(flat, axis=0, keepdims=True)
            flat_high, flat_low = split(flat - average)
            result = average + (
                one(high, flat_high) + (one(high, flat_low) + one(low, flat_high))
            )
            updated[field, :, level] = result.reshape(slab_count, block, width)

    for copy in fetches[1:]:
        copy.wait()
    for cycle in range(cycles):
        weight = live_ref[cycle].astype(jnp.float32) / error_ref[cycle]
        place = level_ref[cycle] * width + column_ref[cycle]
        bundle[cycle, 0:1] = place.astype(jnp.float32)
        bundle[cycle, 1:2] = weight
        bundle[cycle, 2:3] = weight * value_ref[cycle]
    numbers = iota((8, lane_count), 1)
    blend = jnp.where(numbers == first_block, 1.0, 0.0)
    for at in range(count):
        blend = blend + jnp.where(numbers == chosen_ref[0, at], 1.0, 0.0)
    bundle[cycles, :, 0:lane_count] = blend
    spread_rows = jnp.where(
        iota((rows, levels), 0) // block == iota((rows, levels), 1), 1.0, 0.0
    ).astype(jnp.bfloat16)
    same = lax.rem(iota((rows, rows), 0), block) == lax.rem(iota((rows, rows), 1), block)
    for at, part in enumerate(split(coupling_ref[...])):
        tall = one(spread_rows, part).astype(jnp.bfloat16)
        kron[at] = jnp.where(same, one(tall, spread_rows, 1), 0.0).astype(jnp.bfloat16)
    fetches[0].wait()
    for field in range(2):
        for at in range(0, levels, 8):
            part = given_ref[:, field, at : at + 8]
            part = jnp.swapaxes(part, 0, 1)
            x_ref[field, at // slab_levels : (at + 8) // slab_levels] = part.reshape(
                8 // slab_levels, slab_levels, block, width
            )
    pack(x_ref)

    def meet():
        pl.semaphore_wait(barrier, 2 * slab_count - 1 + 4)
        copies = send_halo(0)

        @pl.when(away == 1)
        def _():
            bundle_copy().start()

        @pl.when(away == 0)
        def _():
            notes[...] = bundle[...]

        return copies

    blend_copies = []
    for cycle in range(cycles):
        source = x_ref if cycle == 0 else returned
        if cycle:
            pack(source)
            copies = send_halo(cycle)
            advance(source, cycle, lambda: copies)
        else:
            advance(source, cycle, meet)
        heights_now = (h_ref, heights, send_h.at[cycle], recv_h.at[cycle])
        speeds_now = (u_ref, speeds, send_u.at[cycle], recv_u.at[cycle])
        drains = []
        if cycle == 0:
            inward_relay(1, h_ref)
            inward_send(1, *heights_now)
            mend(edge_u, u_ref)
            inward_relay(0, u_ref)
            inward_send(0, *speeds_now, late=False)

            @pl.when(away == 1)
            def _():
                bundle_copy().wait()

            @pl.when(away == 0)
            def _():
                heights[slab] = h_ref[slab]
                speeds[slab] = u_ref[slab]

            blends[0] = notes[cycles, 0:8, 0:lane_count]
            for step in range(1, grp_count):
                copy = remote(
                    blends.at[0], blends.at[step], send_b.at[step], recv_b.at[step],
                    {"grp": turned(grp, step, grp_count)},
                )
                copy.start()
                blend_copies.append(copy)
        else:
            drains = cube_send(*heights_now)
            mend(edge_u, u_ref)
            drains = drains + cube_send(*speeds_now, slice(0, 2 * EARLY))
            heights[slab] = h_ref[slab]
            speeds[slab] = u_ref[slab]
        sum_cells(cycle)
        if cycle == 0:
            inward_take(heights, recv_h.at[cycle])
        else:
            cube_take(heights, recv_h.at[cycle])
        gram()

        gathers = []
        for step in range(1, mem_count):
            to_line = turned(line, step, mem_count)
            copy = remote(
                own, column.at[step - 1], send_a.at[cycle, step - 1], recv_a.at[cycle, step - 1],
                {"mem": half * depth + lax.rem(to_line, depth), "hor": 2 * pair + to_line // depth},
            )
            copy.start()
            gathers.append(copy)
        if cycle == 0:
            inward_send(0, *speeds_now, early=False)
        else:
            drains = drains + cube_send(*speeds_now, slice(2 * EARLY, None))
        for copy in blend_copies:
            copy.wait()
        blend_copies = []
        for copy in gathers:
            copy.wait()
        returns = []
        for step in range(1, grp_count):
            partial[step - 1] = blended_for(blends[step])
            copy = remote(
                partial.at[step - 1], arrived.at[step - 1],
                send_c.at[cycle, step - 1], recv_c.at[cycle, step - 1],
                {"grp": turned(grp, grp_count - step, grp_count)},
            )
            copy.start()
            returns.append(copy)
        total = blended_for(blends[0])
        for copy in returns:
            copy.wait()
        for step in range(1, grp_count):
            total = total + arrived[step - 1]
        transposed = root(total)
        last = cycle == cycles - 1
        for field, patch in ((1, heights), (0, speeds)):
            if field == 0:
                if cycle == 0:
                    inward_take(speeds, recv_u.at[cycle])
                else:
                    cube_take(speeds, recv_u.at[cycle])
            update(transposed, patch, field)
            if last:
                outward_send(field)
            else:
                drains = drains + cube_send(
                    updated.at[field], returned.at[field],
                    send_e.at[cycle, field], recv_e.at[cycle, field],
                )
                returned[field, slab] = updated[field, slab]
        if not last:
            for field in (1, 0):
                cube_take(returned.at[field], recv_e.at[cycle, field])
        for copy in drains:
            copy.wait_send()
        if cycle == 0:
            inward_drain(1, *heights_now)
            inward_drain(0, *speeds_now)
    for field in (1, 0):
        outward_finish(field)


def turn(state_hbm, out_hbm, given, turned, read_sem, write_sem):
    fields, slab_count, slab_levels, block, width = given.shape
    per = 8 // slab_levels
    parts = [(field, at) for field in (1, 0) for at in range(0, slab_count, per)]
    reads, writes = [], []
    for number, (field, at) in enumerate(parts):
        copy = pltpu.make_async_copy(
            state_hbm.at[field, at : at + per], given.at[field, at : at + per],
            read_sem.at[number],
        )
        copy.start()
        reads.append(copy)
    for number, (field, at) in enumerate(parts):
        reads[number].wait()
        levels = slice(at * slab_levels, (at + per) * slab_levels)
        part = given[field, at : at + per].reshape(8, block, width)
        turned[:, field, levels] = jnp.swapaxes(part, 0, 1)
        copy = pltpu.make_async_copy(
            turned.at[:, field, levels], out_hbm.at[:, field, levels], write_sem.at[number]
        )
        copy.start()
        writes.append(copy)
    for copy in writes:
        copy.wait()


def shards(ensemble, coupling, obs_column, obs_level, obs_value, obs_error, obs_live, partners):
    mem_count = lax.axis_size("mem")
    grp_count = lax.axis_size("grp")
    hor_count = lax.axis_size("hor")
    slab_count = mem_count * grp_count
    lanes = max(LANES, -(-slab_count // LANES) * LANES)
    count = partners.shape[-1]
    block, fields, levels, width = ensemble.shape
    cycles = obs_column.shape[0]
    members = block * slab_count
    slab_levels = levels // slab_count
    state = (slab_count, slab_levels, block, width)
    strip = (slab_count, slab_levels, block, LANES)
    tall = (members // 2 + 8, members)
    rows = levels * block
    groups = 2 * levels * HALO // LANES
    noted = (cycles, 1, obs_column.shape[-1])
    slots = max(obs_column.shape[-1], lanes)
    vmem = pl.BlockSpec(memory_space=pltpu.VMEM)
    dma = pltpu.SemaphoreType.DMA
    f32 = jnp.float32
    result = pl.pallas_call(
        functools.partial(program, (mem_count, grp_count, hor_count), count, cycles),
        out_shape=jax.ShapeDtypeStruct((2,) + state, f32),
        in_specs=[pl.BlockSpec(memory_space=pltpu.HBM)] * 7 + [pl.BlockSpec(memory_space=pltpu.SMEM)],
        out_specs=pl.BlockSpec(memory_space=pl.ANY),
        scratch_shapes=[
            pltpu.VMEM(ensemble.shape, f32), pltpu.VMEM(coupling.shape, f32),
            pltpu.VMEM(noted, jnp.int32), pltpu.VMEM(noted, jnp.int32),
            pltpu.VMEM(noted, f32), pltpu.VMEM(noted, f32), pltpu.VMEM(noted, jnp.int32),
            dma((7,)),
            pltpu.VMEM((2,) + state, f32),
            pltpu.VMEM((2, rows, rows), jnp.bfloat16),
            pltpu.VMEM(state, f32), pltpu.VMEM(state, f32), pltpu.VMEM(state, f32),
            pltpu.VMEM(strip, f32), pltpu.VMEM(strip, f32), pltpu.VMEM(strip, f32),
            pltpu.VMEM((2, groups, block, LANES), f32),
            pltpu.VMEM((cycles, 2, groups, block, LANES), f32),
            pltpu.VMEM(state, f32), pltpu.VMEM(state, f32),
            pltpu.VMEM((2,) + state, f32), pltpu.VMEM((2,) + state, f32),
            pltpu.VMEM((2, slab_count // 2) + state[1:], f32),
            pltpu.VMEM((2, slab_levels * width // LANES, 1, LANES), f32),
            pltpu.VMEM((cycles + 1, 8, slots), f32), pltpu.VMEM((cycles + 1, 8, slots), f32),
            pltpu.VMEM(tall, f32),
            pltpu.VMEM((mem_count - 1,) + tall, f32),
            pltpu.VMEM((grp_count - 1,) + tall, f32),
            pltpu.VMEM((grp_count - 1,) + tall, f32),
            pltpu.VMEM((grp_count, 8, lanes), f32),
            dma((cycles, 2)), dma((cycles, 2)),
            dma((1,)), dma((1,)),
            dma((cycles, mem_count - 1)), dma((cycles, mem_count - 1)),
            dma((grp_count,)), dma((grp_count,)),
            dma((cycles, grp_count - 1)), dma((cycles, grp_count - 1)),
            dma((cycles, slab_count)), dma((cycles, slab_count)),
            dma((cycles, slab_count)), dma((cycles, slab_count)),
            dma((cycles, 2, slab_count)), dma((cycles, 2, slab_count)),
            dma((2, slab_count)), dma((2, slab_count)),
            dma((2, slab_count // 2)), dma((2, slab_count // 2)), dma((2, slab_count // 2)),
        ],
        compiler_params=pltpu.CompilerParams(collective_id=0, has_side_effects=True),
    )(
        ensemble, coupling, obs_column[:, 0], obs_level[:, 0], obs_value[:, 0], obs_error[:, 0],
        obs_live[:, 0], partners[0],
    )
    anywhere = pl.BlockSpec(memory_space=pl.ANY)
    parts = 2 * levels // 8
    return pl.pallas_call(
        turn,
        out_shape=jax.ShapeDtypeStruct(ensemble.shape, f32),
        in_specs=[anywhere], out_specs=anywhere,
        scratch_shapes=[
            pltpu.VMEM((2,) + state, f32), pltpu.VMEM(ensemble.shape, f32),
            dma((parts,)), dma((parts,)),
        ],
    )(result)


def solution(mesh):
    in_specs = (
        P(("mem", "grp"), None, None, "hor"),
        P(),
        P(None, ("mem", "grp"), "hor", None),
        P(None, ("mem", "grp"), "hor", None),
        P(None, ("mem", "grp"), "hor", None),
        P(None, ("mem", "grp"), "hor", None),
        P(None, ("mem", "grp"), "hor", None),
        P(("mem", "grp"), "hor", None),
    )
    out_specs = P(("mem", "grp"), None, None, "hor")
    return jax.shard_map(shards, mesh=mesh, in_specs=in_specs, out_specs=out_specs, check_vma=False)
```
